8 devices in a mesh: dp: 2 (over y, z), tp: 4 (over x, core).
Axes of the slice: x: 2, y: 2, z: 1, core: 2. Of those that a mesh axis runs over, the one named last changes fastest.
Arguments:
- x: bfloat16 [2, 1024, 4096], P('dp', 'tp'), parts along dimension 0
- dy: bfloat16 [2, 1024, 4096], P('dp', 'tp'), parts along dimension 0
- wq: bfloat16 [4096, 4096], P(None, 'tp')
- wk: bfloat16 [4096, 1024], P(None, 'tp')
- wv: bfloat16 [4096, 1024], P(None, 'tp')
- wo: bfloat16 [4096, 4096], P('tp')
- w_gate: bfloat16 [4096, 12800], P(None, 'tp')
- w_up: bfloat16 [4096, 12800], P(None, 'tp')
- w_down: bfloat16 [12800, 4096], P('tp')
Outputs:
- output 1: bfloat16 [2, 1024, 4096], P('dp', 'tp'), parts along dimension 0
- output 2: bfloat16 [8192, 4096], P('dp', 'tp'), parts along dimension 0
- output 3: bfloat16 [8192, 1024], P('dp', 'tp'), parts along dimension 0
- output 4: bfloat16 [8192, 1024], P('dp', 'tp'), parts along dimension 0
- output 5: bfloat16 [8192, 4096], P(('dp', 'tp')), parts along dimension 0
- output 6: bfloat16 [8192, 12800], P('dp', 'tp'), parts along dimension 0
- output 7: bfloat16 [8192, 12800], P('dp', 'tp'), parts along dimension 0
- output 8: bfloat16 [25600, 4096], P(('dp', 'tp')), parts along dimension 0
There are 2 independent parts. The reference program is written for one: setup_inputs(seed, part) draws one part's arguments, and reference() takes and returns one part's arrays. A program takes and returns all parts, laid end to end along the dimension named above; an argument that names none is the same for every part.
All inputs are finite; a program needn't handle non-finite values.
Results may differ from the reference program's by a relative error of at most 0.024.
Values are sent between devices in bfloat16 or wider.
A program may use at most 2 GiB of HBM per device.

```python
import jax
import jax.numpy as jnp
from jax import lax

SEQUENCES = 1
TOKENS = 1024
D = 4096
HEADS = 32
KV_HEADS = 8
HEAD = 128
FF = 12800
THETA = 10000
NAMES = ("wq", "wk", "wv", "wo", "w_gate", "w_up", "w_down")
SHAPES = {
    "wq": (D, HEADS * HEAD),
    "wk": (D, KV_HEADS * HEAD),
    "wv": (D, KV_HEADS * HEAD),
    "wo": (HEADS * HEAD, D),
    "w_gate": (D, FF),
    "w_up": (D, FF),
    "w_down": (FF, D),
}


def bump(key, n, height):
    away = (jnp.arange(n, dtype=jnp.int32) - jax.random.randint(key, (), 0, n, jnp.int32)) % n
    return jnp.where(away < n // 8, height, 1.0)


def together(key, own, strength):
    shared = jax.random.normal(key, own.shape[1:], jnp.float32)
    return (own + strength * shared) * lax.rsqrt(1 + strength * strength)


def setup_inputs(seed: int = 0, part: int = 0) -> dict:
    kx, kdy, ka, kb, kz, kf, kh, kl, *kw = jax.random.split(jax.random.key(seed), 8 + len(NAMES))
    kx, kdy, ka, kb = (jax.random.fold_in(k, part) for k in (kx, kdy, ka, kb))
    shape = (SEQUENCES, TOKENS, D)
    much_x, much_dy = jax.random.uniform(kz, (2,), jnp.float32, 0.0, 1.0)
    loud = 2.0 ** jax.random.uniform(jax.random.fold_in(kz, 1), (), jnp.float32, -1.0, 2.0)
    halves = 2.0 ** jax.random.uniform(kl, (2,), jnp.float32, -1.0, 1.0)
    times = {"wq": 1.0, "wk": 1.0, "wv": 2.0, "wo": halves[0], "w_gate": 1.0, "w_up": bump(kh, FF, 4.0), "w_down": halves[1]}
    x = together(ka, jax.random.normal(kx, shape, jnp.float32), much_x) * bump(kf, D, 4.0)
    dy = together(kb, jax.random.normal(kdy, shape, jnp.float32), much_dy)
    drawn = {"x": x.astype(jnp.bfloat16), "dy": (loud * dy * (SEQUENCES * TOKENS) ** -0.5).astype(jnp.bfloat16)}
    for key, name in zip(kw, NAMES, strict=True):
        drawn[name] = (jax.random.normal(key, SHAPES[name], jnp.float32) * SHAPES[name][0] ** -0.5 * times[name]).astype(jnp.bfloat16)
    return drawn


def matmul(a, w):
    return jnp.dot(a, w, preferred_element_type=jnp.float32).astype(jnp.bfloat16)


def normed(h):
    wide = h.astype(jnp.float32)
    scale = lax.rsqrt(jnp.mean(wide**2, -1, keepdims=True) + 1e-6)
    return (wide * scale).astype(jnp.bfloat16)


def turned(t, theta):
    half = t.shape[-1] // 2
    angle = jnp.arange(t.shape[0], dtype=jnp.float32)[:, None] * theta ** (-jnp.arange(half, dtype=jnp.float32) / half)
    cos, sin = jnp.cos(angle)[:, None], jnp.sin(angle)[:, None]
    a, b = t[..., :half].astype(jnp.float32), t[..., half:].astype(jnp.float32)
    return jnp.concatenate([a * cos - b * sin, b * cos + a * sin], -1).astype(jnp.bfloat16)


def seen_by(q, k, v):
    tokens, kv = q.shape[0], k.shape[1]
    q = q.reshape(tokens, kv, -1, q.shape[-1])
    scores = jnp.einsum("tgsd,ugd->gstu", q.astype(jnp.float32), k.astype(jnp.float32)) * q.shape[-1] ** -0.5
    place = jnp.arange(tokens)
    weights = jax.nn.softmax(jnp.where(place[:, None] >= place, scores, -jnp.inf), -1).astype(jnp.bfloat16)
    return jnp.einsum("gstu,ugd->tgsd", weights.astype(jnp.float32), v.astype(jnp.float32)).astype(jnp.bfloat16).reshape(tokens, -1)


def layer(h, w):
    a = normed(h)
    q, k = (turned(matmul(a, w[name]).reshape(h.shape[0], -1, HEAD), THETA) for name in ("wq", "wk"))
    h = h + matmul(seen_by(q, k, matmul(a, w["wv"]).reshape(h.shape[0], -1, HEAD)), w["wo"])
    b = normed(h)
    gate = jnp.dot(b, w["w_gate"], preferred_element_type=jnp.float32)
    up = jnp.dot(b, w["w_up"], preferred_element_type=jnp.float32)
    return h + matmul((jax.nn.silu(gate) * up).astype(jnp.bfloat16), w["w_down"])


def reference(x, dy, wq, wk, wv, wo, w_gate, w_up, w_down):
    weights = dict(zip(NAMES, (wq, wk, wv, wo, w_gate, w_up, w_down), strict=True))

    def take(so_far, sequence):
        h, by_y = sequence
        _, back = jax.vjp(lambda w, h: layer(h, w), weights, h)
        by_weights, by_h = back(by_y)
        return jax.tree.map(lambda total, term: total + term.astype(jnp.float32), so_far, by_weights), by_h

    none_yet = {name: jnp.zeros(w.shape, jnp.float32) for name, w in weights.items()}
    by_weights, by_x = lax.scan(take, none_yet, (x, dy))
    return (by_x, *(by_weights[name].astype(jnp.bfloat16) for name in NAMES))
```

```python
import functools

import jax
import jax.numpy as jnp
from jax import lax
from jax.experimental import pallas as pl
from jax.experimental.pallas import tpu as pltpu
from jax.sharding import PartitionSpec as P

HEAD = 128
THETA = 10000
LOG2E = 1.4426950408889634
NEG = -1e30
HIDDEN = 2 * NEG
SCALE = HEAD**-0.5
BF, F32 = jnp.bfloat16, jnp.float32
VMEM = 56 * 2**20
BLOCK = 256
STRIP = 512


def _dot(a, b, ca, cb):
    return lax.dot_general(a, b, (((ca,), (cb,)), ((), ())), preferred_element_type=F32)


def _rope(x, cos, sin):
    x = x.astype(F32)
    return x * cos + pltpu.roll(x, HEAD // 2, 1) * sin


def _unrope(x, cos, sin):
    return x * cos - pltpu.roll(x, HEAD // 2, 1) * sin


def _hidden(cols):
    key = lax.broadcasted_iota(jnp.int32, (BLOCK, cols), 0)
    return key > lax.rem(lax.broadcasted_iota(jnp.int32, (BLOCK, cols), 1), BLOCK)


def _attend(me_ref, q_ref, k_ref, v_ref, cos_ref, sin_ref, o_ref, lse_ref, qr_ref, kr_ref, vt_s, q_s, top_s, mix_s):
    iq = pl.program_id(1)
    me = me_ref[0]
    n = k_ref.shape[0] // BLOCK
    g = q_ref.shape[1] // HEAD
    cols = g * BLOCK
    e = SCALE * LOG2E

    @pl.when(iq == 0)
    def _():
        for s in range(n):
            here = pl.ds((s ^ me) * BLOCK, BLOCK)
            rows = slice(s * BLOCK, (s + 1) * BLOCK)
            kr_ref[rows, :] = _rope(k_ref[rows, :], cos_ref[here, :], sin_ref[here, :]).astype(BF)
            vt_s[s, :HEAD, :] = v_ref[rows, :].T
            vt_s[s, HEAD:, :] = jnp.ones((8, BLOCK), BF)

    here = pl.ds(iq * BLOCK, BLOCK)
    cos, sin = cos_ref[here, :], sin_ref[here, :]
    for h in range(g):
        turned = _rope(q_ref[:, h * HEAD : (h + 1) * HEAD], cos, sin).astype(BF)
        qr_ref[:, h * HEAD : (h + 1) * HEAD] = turned
        q_s[h * BLOCK : (h + 1) * BLOCK, :] = turned
    top_s[...] = jnp.full((1, cols), NEG, F32)
    mix_s[...] = jnp.zeros((HEAD + 8, cols), F32)

    def block(j, masked):
        slot = j ^ me
        keys = kr_ref[pl.ds(slot * BLOCK, BLOCK), :]
        strips = range(0, cols, STRIP)
        scores = [_dot(keys, q_s[at : at + STRIP, :], 1, 1) for at in strips]
        weights, keeps = [], []
        for at, s in zip(strips, scores):
            if masked:
                s = jnp.where(_hidden(STRIP), HIDDEN, s)
            old = top_s[:, at : at + STRIP]
            top = jnp.maximum(old, s.max(axis=0, keepdims=True))
            top_s[:, at : at + STRIP] = top
            weights.append(jnp.exp2((s - top) * e).astype(BF))
            keeps.append(jnp.exp2((old - top) * e))
        for at, p, keep in zip(strips, weights, keeps):
            mix_s[:, at : at + STRIP] = mix_s[:, at : at + STRIP] * keep + _dot(vt_s[slot], p, 1, 0)

    lax.fori_loop(0, iq, lambda j, _: block(j, False), None)
    block(iq, True)
    total = mix_s[HEAD : HEAD + 1, :]
    out = (mix_s[:HEAD, :] * (1 / total)).T.astype(BF)
    for h in range(g):
        o_ref[:, h * HEAD : (h + 1) * HEAD] = out[h * BLOCK : (h + 1) * BLOCK, :]
    lse_ref[0] = top_s[...] * e + jnp.log2(total)


def _attend_bwd(me_ref, q_ref, k_ref, v_ref, do_ref, o_ref, lse_ref, cos_ref, sin_ref, dq_ref, dk_ref, dv_ref,
                q_s, do_s, dq_s, dk_s, dv_s, kt_s, delta_s):
    iq = pl.program_id(1)
    me = me_ref[0]
    n = k_ref.shape[0] // BLOCK
    g = q_ref.shape[1] // HEAD
    cols = g * BLOCK
    e = SCALE * LOG2E

    @pl.when(iq == 0)
    def _():
        dk_s[...] = jnp.zeros_like(dk_s)
        dv_s[...] = jnp.zeros_like(dv_s)
        for s in range(n):
            kt_s[s] = k_ref[s * BLOCK : (s + 1) * BLOCK, :].T

    dq_s[...] = jnp.zeros_like(dq_s)
    for h in range(g):
        lanes, rows = slice(h * HEAD, (h + 1) * HEAD), slice(h * BLOCK, (h + 1) * BLOCK)
        q_s[rows, :] = q_ref[:, lanes]
        do_s[rows, :] = do_ref[:, lanes]
        prod = do_ref[:, lanes].astype(F32) * o_ref[:, lanes].astype(F32)
        delta_s[:, rows] = prod.T.sum(axis=0, keepdims=True)

    def block(j, masked):
        slot = j ^ me
        here = pl.ds(slot * BLOCK, BLOCK)
        keys, values = k_ref[here, :], v_ref[here, :]
        strips = range(0, cols, STRIP)
        scores = [_dot(keys, q_s[at : at + STRIP, :], 1, 1) for at in strips]
        dps = [_dot(values, do_s[at : at + STRIP, :], 1, 1) for at in strips]
        for at, s, dp in zip(strips, scores, dps):
            p = jnp.exp2(s * e - lse_ref[0, :, at : at + STRIP])
            if masked:
                p = jnp.where(_hidden(STRIP), 0.0, p)
            ds = (p * (dp - delta_s[:, at : at + STRIP])).astype(BF)
            dv_s[here, :] += _dot(p.astype(BF), do_s[at : at + STRIP, :], 1, 0)
            dk_s[here, :] += _dot(ds, q_s[at : at + STRIP, :], 1, 0)
            dq_s[:, at : at + STRIP] += _dot(kt_s[slot], ds, 1, 0)

    lax.fori_loop(0, iq, lambda j, _: block(j, False), None)
    block(iq, True)
    here = pl.ds(iq * BLOCK, BLOCK)
    cos, sin = cos_ref[here, :], sin_ref[here, :]
    dq = (dq_s[...] * SCALE).T
    for h in range(g):
        dq_ref[:, h * HEAD : (h + 1) * HEAD] = _unrope(dq[h * BLOCK : (h + 1) * BLOCK, :], cos, sin).astype(BF)

    @pl.when(iq == n - 1)
    def _():
        for s in range(n):
            here = pl.ds((s ^ me) * BLOCK, BLOCK)
            rows = slice(s * BLOCK, (s + 1) * BLOCK)
            dk_ref[rows, :] = _unrope(dk_s[rows, :] * SCALE, cos_ref[here, :], sin_ref[here, :]).astype(BF)
            dv_ref[rows, :] = dv_s[rows, :].astype(BF)


def _attn_specs(tokens, g):
    queries = pl.BlockSpec((BLOCK, g * HEAD), lambda h, i, me: (i ^ me[0], h))
    keys = pl.BlockSpec((tokens, HEAD), lambda h, i, me: (0, h))
    table = pl.BlockSpec((tokens, HEAD), lambda h, i, me: (0, 0))
    stats = pl.BlockSpec((1, 1, g * BLOCK), lambda h, i, me: (h * (tokens // BLOCK) + i, 0, 0))
    return queries, keys, table, stats


def attend(me, q, k, v, cos, sin):
    tokens, kv = k.shape[0], k.shape[1] // HEAD
    g = q.shape[1] // k.shape[1]
    queries, keys, table, stats = _attn_specs(tokens, g)
    n = tokens // BLOCK
    return pl.pallas_call(
        _attend,
        grid_spec=pltpu.PrefetchScalarGridSpec(
            num_scalar_prefetch=1, grid=(kv, n), in_specs=[queries, keys, keys, table, table], out_specs=[queries, stats, queries, keys],
            scratch_shapes=[pltpu.VMEM((n, HEAD + 8, BLOCK), BF), pltpu.VMEM((g * BLOCK, HEAD), BF), pltpu.VMEM((1, g * BLOCK), F32),
                            pltpu.VMEM((HEAD + 8, g * BLOCK), F32)]),
        out_shape=[jax.ShapeDtypeStruct(q.shape, BF), jax.ShapeDtypeStruct((kv * n, 1, g * BLOCK), F32), jax.ShapeDtypeStruct(q.shape, BF),
                   jax.ShapeDtypeStruct(k.shape, BF)],
        compiler_params=pltpu.CompilerParams(dimension_semantics=("arbitrary", "arbitrary"), vmem_limit_bytes=24 * 2**20),
        cost_estimate=pl.CostEstimate(flops=12 * 10**9, transcendentals=0, bytes_accessed=8 * 2**20),
        name="attend",
    )(me, q, k, v, cos, sin)


def attend_bwd(me, q, k, v, do, o, lse, cos, sin):
    tokens, kv = k.shape[0], k.shape[1] // HEAD
    g = q.shape[1] // k.shape[1]
    queries, keys, table, stats = _attn_specs(tokens, g)
    n = tokens // BLOCK
    return pl.pallas_call(
        _attend_bwd,
        grid_spec=pltpu.PrefetchScalarGridSpec(
            num_scalar_prefetch=1, grid=(kv, n), in_specs=[queries, keys, keys, queries, queries, stats, table, table],
            out_specs=[queries, keys, keys],
            scratch_shapes=[pltpu.VMEM((g * BLOCK, HEAD), BF), pltpu.VMEM((g * BLOCK, HEAD), BF), pltpu.VMEM((HEAD, g * BLOCK), F32),
                            pltpu.VMEM((tokens, HEAD), F32), pltpu.VMEM((tokens, HEAD), F32), pltpu.VMEM((n, HEAD, BLOCK), BF),
                            pltpu.VMEM((1, g * BLOCK), F32)]),
        out_shape=[jax.ShapeDtypeStruct(q.shape, BF), jax.ShapeDtypeStruct(k.shape, BF), jax.ShapeDtypeStruct(k.shape, BF)],
        compiler_params=pltpu.CompilerParams(dimension_semantics=("arbitrary", "arbitrary"), vmem_limit_bytes=24 * 2**20),
        cost_estimate=pl.CostEstimate(flops=18 * 10**9, transcendentals=0, bytes_accessed=12 * 2**20),
        name="attend_bwd",
    )(me, q, k, v, do, o, lse, cos, sin)


CORE = [(0, 1), (1, 0), (2, 3), (3, 2)]
CROSS = [(0, 2), (2, 0), (1, 3), (3, 1)]


def core(v):
    return lax.ppermute(v, "tp", CORE)


def cross(v):
    return lax.ppermute(v, "tp", CROSS)


def gather(v):
    near = core(v)
    parts = [cross(t) for t in jnp.split(v, 2)]
    return jnp.concatenate([v, near]), jnp.concatenate([*parts, *(core(t) for t in parts)])


def scatter(near, far):
    far = far
    mine, other = far[:BLOCK], far[BLOCK:]
    both = (mine.astype(F32) + core(other).astype(F32)).astype(BF)
    across = cross(both)
    return near[:BLOCK].astype(F32) + core(near[BLOCK:]).astype(F32) + across.astype(F32)


def mm(a, b, ca, cb):
    return _dot(a, b, ca, cb).astype(BF)


def norm(h):
    wide = h.astype(F32)
    scale = lax.rsqrt(jnp.mean(wide**2, -1, keepdims=True) + 1e-6)
    return (wide * scale).astype(BF), scale


def norm_bwd(h, scale, g):
    wide = h.astype(F32)
    g = g.astype(BF).astype(F32)
    return scale * g - wide * (scale**3 * jnp.mean(g * wide, -1, keepdims=True))


def both(f, near, far):
    return jnp.concatenate([f(near), f(far)])


def step(x, dy, wq, wk, wv, wo, wg, wu, wd):
    x, dy = x[0], dy[0]
    me = lax.axis_index("tp").astype(jnp.int32).reshape(1)
    tokens = 4 * x.shape[0]
    half = HEAD // 2
    angle = jnp.arange(tokens, dtype=F32)[:, None] * THETA ** (-jnp.arange(half, dtype=F32) / half)
    cos, sin = jnp.cos(angle), jnp.sin(angle)
    cos, sin = jnp.concatenate([cos, cos], 1), jnp.concatenate([-sin, sin], 1)

    a, a_scale = norm(x)
    a_near, a_far = gather(a)
    dy_near, dy_far = gather(dy)
    q, k, v = (both(lambda t: mm(t, w, 1, 0), a_near, a_far) for w in (wq, wk, wv))
    heads, lse, q, k = attend(me, q, k, v, cos, sin)
    cut = tokens // 2
    h = x.astype(F32) + scatter(mm(heads[:cut], wo, 1, 0), mm(heads[cut:], wo, 1, 0))
    h = h.astype(BF)
    b, b_scale = norm(h)
    b_near, b_far = gather(b)

    def mlp(b, dy):
        gate, up = _dot(b, wg, 1, 0), _dot(b, wu, 1, 0)
        dhid = mm(dy, wd, 1, 1).astype(F32)
        sig = jax.nn.sigmoid(gate)
        silu = gate * sig
        hid = (silu * up).astype(BF)
        dup = (dhid * silu).astype(BF)
        dgate = (dhid * up * (sig + silu * (1 - sig))).astype(BF)
        return hid, dgate, dup

    def by_b(dgate, dup):
        return (_dot(dgate, wg, 1, 1) + _dot(dup, wu, 1, 1)).astype(BF)

    hid_near, dgate_near, dup_near = mlp(b_near, dy_near)
    hid_far, dgate_far, dup_far = mlp(b_far, dy_far)
    db = scatter(by_b(dgate_near, dup_near), by_b(dgate_far, dup_far))
    dh = (dy.astype(F32) + norm_bwd(h, b_scale, db)).astype(BF)
    dh_near, dh_far = gather(dh)
    cat = lambda *t: jnp.concatenate(t)
    b_all, dy_all = cat(b_near, b_far), cat(dy_near, dy_far)
    d_wd = mm(cat(hid_near, hid_far), dy_all, 0, 0)
    d_wg = mm(b_all, cat(dgate_near, dgate_far), 0, 0)
    d_wu = mm(b_all, cat(dup_near, dup_far), 0, 0)
    dheads = both(lambda t: mm(t, wo, 1, 1), dh_near, dh_far)
    d_wo = mm(heads, cat(dh_near, dh_far), 0, 0)
    dq, dk, dv = attend_bwd(me, q, k, v, dheads, heads, lse, cos, sin)

    def by_a(s):
        return (_dot(dq[s], wq, 1, 1) + _dot(dk[s], wk, 1, 1) + _dot(dv[s], wv, 1, 1)).astype(BF)

    da = scatter(by_a(slice(0, cut)), by_a(slice(cut, None)))
    a_all = cat(a_near, a_far)
    d_wq, d_wk, d_wv = (mm(a_all, t, 0, 0) for t in (dq, dk, dv))
    dx = (dh.astype(F32) + norm_bwd(x, a_scale, da)).astype(BF)
    return (dx[None], d_wq, d_wk, d_wv, d_wo, d_wg, d_wu, d_wd)


def solution(mesh):
    states, by_columns, by_rows = P("dp", "tp", None), P(None, "tp"), P("tp", None)
    weights = (by_columns, by_columns, by_columns, by_rows, by_columns, by_columns, by_rows)
    own = tuple(P("dp", "tp") if spec == by_columns else P(("dp", "tp"), None) for spec in weights)
    return jax.shard_map(step, mesh=mesh, in_specs=(states, states, *weights), out_specs=(states, *own), check_vma=False)
```

```python
import functools

import jax
import jax.numpy as jnp
from jax import lax
from jax.experimental import pallas as pl
from jax.experimental.pallas import tpu as pltpu
from jax.sharding import PartitionSpec as P

HEAD = 128
THETA = 10000
LOG2E = 1.4426950408889634
NEG = -1e30
HIDDEN = 2 * NEG
SCALE = HEAD**-0.5
BF, F32 = jnp.bfloat16, jnp.float32
VMEM = 56 * 2**20
BLOCK = 256
STRIP = 512


def _dot(a, b, ca, cb):
    return lax.dot_general(a, b, (((ca,), (cb,)), ((), ())), preferred_element_type=F32)


def _rope(x, cos, sin):
    x = x.astype(F32)
    return x * cos + pltpu.roll(x, HEAD // 2, 1) * sin


def _unrope(x, cos, sin):
    return x * cos - pltpu.roll(x, HEAD // 2, 1) * sin


def _hidden(cols):
    key = lax.broadcasted_iota(jnp.int32, (BLOCK, cols), 0)
    return key > lax.rem(lax.broadcasted_iota(jnp.int32, (BLOCK, cols), 1), BLOCK)


def _attend(me_ref, q_ref, k_ref, v_ref, cos_ref, sin_ref, o_ref, lse_ref, qr_ref, kr_ref, vt_s, q_s, top_s, mix_s):
    iq = pl.program_id(1)
    me = me_ref[0]
    n = k_ref.shape[0] // BLOCK
    g = q_ref.shape[1] // HEAD
    cols = g * BLOCK
    e = SCALE * LOG2E

    @pl.when(iq == 0)
    def _():
        for s in range(n):
            here = pl.ds((s ^ me) * BLOCK, BLOCK)
            rows = slice(s * BLOCK, (s + 1) * BLOCK)
            kr_ref[rows, :] = _rope(k_ref[rows, :], cos_ref[here, :], sin_ref[here, :]).astype(BF)
            vt_s[s, :HEAD, :] = v_ref[rows, :].T
            vt_s[s, HEAD:, :] = jnp.ones((8, BLOCK), BF)

    here = pl.ds(iq * BLOCK, BLOCK)
    cos, sin = cos_ref[here, :], sin_ref[here, :]
    for h in range(g):
        turned = _rope(q_ref[:, h * HEAD : (h + 1) * HEAD], cos, sin).astype(BF)
        qr_ref[:, h * HEAD : (h + 1) * HEAD] = turned
        q_s[h * BLOCK : (h + 1) * BLOCK, :] = turned
    top_s[...] = jnp.full((1, cols), NEG, F32)
    mix_s[...] = jnp.zeros((HEAD + 8, cols), F32)

    def block(j, masked):
        slot = j ^ me
        keys = kr_ref[pl.ds(slot * BLOCK, BLOCK), :]
        strips = range(0, cols, STRIP)
        scores = [_dot(keys, q_s[at : at + STRIP, :], 1, 1) for at in strips]
        weights, keeps = [], []
        for at, s in zip(strips, scores):
            if masked:
                s = jnp.where(_hidden(STRIP), HIDDEN, s)
            old = top_s[:, at : at + STRIP]
            top = jnp.maximum(old, s.max(axis=0, keepdims=True))
            top_s[:, at : at + STRIP] = top
            weights.append(jnp.exp2((s - top) * e).astype(BF))
            keeps.append(jnp.exp2((old - top) * e))
        for at, p, keep in zip(strips, weights, keeps):
            mix_s[:, at : at + STRIP] = mix_s[:, at : at + STRIP] * keep + _dot(vt_s[slot], p, 1, 0)

    lax.fori_loop(0, iq, lambda j, _: block(j, False), None)
    block(iq, True)
    total = mix_s[HEAD : HEAD + 1, :]
    out = (mix_s[:HEAD, :] * (1 / total)).T.astype(BF)
    for h in range(g):
        o_ref[:, h * HEAD : (h + 1) * HEAD] = out[h * BLOCK : (h + 1) * BLOCK, :]
    lse_ref[0] = top_s[...] * e + jnp.log2(total)


def _attend_bwd(me_ref, q_ref, k_ref, v_ref, do_ref, o_ref, lse_ref, cos_ref, sin_ref, dq_ref, dk_ref, dv_ref,
                q_s, do_s, dq_s, dk_s, dv_s, kt_s, delta_s):
    iq = pl.program_id(1)
    me = me_ref[0]
    n = k_ref.shape[0] // BLOCK
    g = q_ref.shape[1] // HEAD
    cols = g * BLOCK
    e = SCALE * LOG2E

    @pl.when(iq == 0)
    def _():
        dk_s[...] = jnp.zeros_like(dk_s)
        dv_s[...] = jnp.zeros_like(dv_s)
        for s in range(n):
            kt_s[s] = k_ref[s * BLOCK : (s + 1) * BLOCK, :].T

    dq_s[...] = jnp.zeros_like(dq_s)
    for h in range(g):
        lanes, rows = slice(h * HEAD, (h + 1) * HEAD), slice(h * BLOCK, (h + 1) * BLOCK)
        q_s[rows, :] = q_ref[:, lanes]
        do_s[rows, :] = do_ref[:, lanes]
        prod = do_ref[:, lanes].astype(F32) * o_ref[:, lanes].astype(F32)
        delta_s[:, rows] = prod.T.sum(axis=0, keepdims=True)

    def block(j, masked):
        slot = j ^ me
        here = pl.ds(slot * BLOCK, BLOCK)
        keys, values = k_ref[here, :], v_ref[here, :]
        strips = range(0, cols, STRIP)
        scores = [_dot(keys, q_s[at : at + STRIP, :], 1, 1) for at in strips]
        dps = [_dot(values, do_s[at : at + STRIP, :], 1, 1) for at in strips]
        for at, s, dp in zip(strips, scores, dps):
            p = jnp.exp2(s * e - lse_ref[0, :, at : at + STRIP])
            if masked:
                p = jnp.where(_hidden(STRIP), 0.0, p)
            ds = (p * (dp - delta_s[:, at : at + STRIP])).astype(BF)
            dv_s[here, :] += _dot(p.astype(BF), do_s[at : at + STRIP, :], 1, 0)
            dk_s[here, :] += _dot(ds, q_s[at : at + STRIP, :], 1, 0)
            dq_s[:, at : at + STRIP] += _dot(kt_s[slot], ds, 1, 0)

    lax.fori_loop(0, iq, lambda j, _: block(j, False), None)
    block(iq, True)
    here = pl.ds(iq * BLOCK, BLOCK)
    cos, sin = cos_ref[here, :], sin_ref[here, :]
    dq = (dq_s[...] * SCALE).T
    for h in range(g):
        dq_ref[:, h * HEAD : (h + 1) * HEAD] = _unrope(dq[h * BLOCK : (h + 1) * BLOCK, :], cos, sin).astype(BF)

    @pl.when(iq == n - 1)
    def _():
        for s in range(n):
            here = pl.ds((s ^ me) * BLOCK, BLOCK)
            rows = slice(s * BLOCK, (s + 1) * BLOCK)
            dk_ref[rows, :] = _unrope(dk_s[rows, :] * SCALE, cos_ref[here, :], sin_ref[here, :]).astype(BF)
            dv_ref[rows, :] = dv_s[rows, :].astype(BF)


def _attn_specs(tokens, g):
    queries = pl.BlockSpec((BLOCK, g * HEAD), lambda h, i, me: (i ^ me[0], h))
    keys = pl.BlockSpec((tokens, HEAD), lambda h, i, me: (0, h))
    table = pl.BlockSpec((tokens, HEAD), lambda h, i, me: (0, 0))
    stats = pl.BlockSpec((1, 1, g * BLOCK), lambda h, i, me: (h * (tokens // BLOCK) + i, 0, 0))
    return queries, keys, table, stats


def attend(me, q, k, v, cos, sin):
    tokens, kv = k.shape[0], k.shape[1] // HEAD
    g = q.shape[1] // k.shape[1]
    queries, keys, table, stats = _attn_specs(tokens, g)
    n = tokens // BLOCK
    return pl.pallas_call(
        _attend,
        grid_spec=pltpu.PrefetchScalarGridSpec(
            num_scalar_prefetch=1, grid=(kv, n), in_specs=[queries, keys, keys, table, table], out_specs=[queries, stats, queries, keys],
            scratch_shapes=[pltpu.VMEM((n, HEAD + 8, BLOCK), BF), pltpu.VMEM((g * BLOCK, HEAD), BF), pltpu.VMEM((1, g * BLOCK), F32),
                            pltpu.VMEM((HEAD + 8, g * BLOCK), F32)]),
        out_shape=[jax.ShapeDtypeStruct(q.shape, BF), jax.ShapeDtypeStruct((kv * n, 1, g * BLOCK), F32), jax.ShapeDtypeStruct(q.shape, BF),
                   jax.ShapeDtypeStruct(k.shape, BF)],
        compiler_params=pltpu.CompilerParams(dimension_semantics=("arbitrary", "arbitrary"), vmem_limit_bytes=24 * 2**20),
        cost_estimate=pl.CostEstimate(flops=12 * 10**9, transcendentals=0, bytes_accessed=8 * 2**20),
        name="attend",
    )(me, q, k, v, cos, sin)


def attend_bwd(me, q, k, v, do, o, lse, cos, sin):
    tokens, kv = k.shape[0], k.shape[1] // HEAD
    g = q.shape[1] // k.shape[1]
    queries, keys, table, stats = _attn_specs(tokens, g)
    n = tokens // BLOCK
    return pl.pallas_call(
        _attend_bwd,
        grid_spec=pltpu.PrefetchScalarGridSpec(
            num_scalar_prefetch=1, grid=(kv, n), in_specs=[queries, keys, keys, queries, queries, stats, table, table],
            out_specs=[queries, keys, keys],
            scratch_shapes=[pltpu.VMEM((g * BLOCK, HEAD), BF), pltpu.VMEM((g * BLOCK, HEAD), BF), pltpu.VMEM((HEAD, g * BLOCK), F32),
                            pltpu.VMEM((tokens, HEAD), F32), pltpu.VMEM((tokens, HEAD), F32), pltpu.VMEM((n, HEAD, BLOCK), BF),
                            pltpu.VMEM((1, g * BLOCK), F32)]),
        out_shape=[jax.ShapeDtypeStruct(q.shape, BF), jax.ShapeDtypeStruct(k.shape, BF), jax.ShapeDtypeStruct(k.shape, BF)],
        compiler_params=pltpu.CompilerParams(dimension_semantics=("arbitrary", "arbitrary"), vmem_limit_bytes=24 * 2**20),
        cost_estimate=pl.CostEstimate(flops=18 * 10**9, transcendentals=0, bytes_accessed=12 * 2**20),
        name="attend_bwd",
    )(me, q, k, v, do, o, lse, cos, sin)


ANY = pl.BlockSpec(memory_space=pltpu.HBM)


def _load(pieces, whole, sems):
    copies, at = [], 0
    for i, piece in enumerate(pieces):
        n = piece.shape[0]
        copies.append(pltpu.make_async_copy(piece, whole.at[pl.ds(at, n), :], sems.at[i]))
        at += n
    for c in copies:
        c.start()
    return copies


def _params(mib, steps=1):
    return pltpu.CompilerParams(dimension_semantics=("arbitrary",) * steps, vmem_limit_bytes=mib * 2**20)


def _price(flops, arrays):
    return pl.CostEstimate(flops=flops, transcendentals=0, bytes_accessed=sum(a.size * 2 for a in arrays))


def _rows(pieces):
    return sum(p.shape[0] for p in pieces)


def qkv(pieces, wq, wk, wv):
    n, (d, nq), nk = len(pieces), wq.shape, wk.shape[1]
    rows, cut = _rows(pieces), 512

    def kernel(*refs):
        xs, (wq_ref, wk_ref, wv_ref), (q_ref, k_ref, v_ref) = refs[:n], refs[n : n + 3], refs[n + 3 : n + 6]
        x_s, q_s, k_s, v_s, sems, wsems = refs[n + 6 :]
        copies = _load(xs, x_s, sems)
        todo = []
        for i, at in enumerate(range(0, nq, cut)):
            here = slice(at, at + cut)
            todo.append((pltpu.make_async_copy(wq_ref.at[:, here], q_s.at[:, here], wsems.at[i]), q_s.at[:, here], q_ref, here))
        for i, (w, w_s, o) in enumerate(((wk_ref, k_s, k_ref), (wv_ref, v_s, v_ref))):
            todo.append((pltpu.make_async_copy(w, w_s, wsems.at[nq // cut + i]), w_s, o, slice(0, nk)))
        for t in todo:
            t[0].start()
        for c in copies:
            c.wait()
        for c, w_s, o, here in todo:
            c.wait()
            o[:, here] = _dot(x_s[...], w_s[...], 1, 0).astype(BF)

    return pl.pallas_call(
        kernel, in_specs=[ANY] * (n + 3), out_specs=[pl.BlockSpec(memory_space=pltpu.VMEM)] * 3,
        out_shape=[jax.ShapeDtypeStruct((rows, m), BF) for m in (nq, nk, nk)],
        scratch_shapes=[pltpu.VMEM((rows, d), BF), pltpu.VMEM((d, nq), BF), pltpu.VMEM((d, nk), BF), pltpu.VMEM((d, nk), BF),
                        pltpu.SemaphoreType.DMA((n,)), pltpu.SemaphoreType.DMA((nq // cut + 2,))],
        compiler_params=pltpu.CompilerParams(vmem_limit_bytes=30 * 2**20),
        cost_estimate=_price(2 * rows * d * (nq + 2 * nk), [*pieces, wq, wk, wv]), name="qkv",
    )(*pieces, wq, wk, wv)


def by_rows_of(pieces, w, bn, name):
    n, (cols, d) = len(pieces), w.shape
    rows = _rows(pieces)
    steps, rest = -(-cols // bn), cols % bn
    small = -(-rest // 256) * 256

    def kernel(*refs):
        xs, w_ref, o_ref, x_s, sems = refs[:n], refs[n], refs[n + 1], refs[n + 2], refs[n + 3]
        i = pl.program_id(0)

        @pl.when(i == 0)
        def _():
            for c in _load(xs, x_s, sems):
                c.wait()

        if rest == 0 or small == bn:
            o_ref[...] = _dot(x_s[...], w_ref[...], 1, 1).astype(BF)
            return

        @pl.when(i < steps - 1)
        def _():
            o_ref[...] = _dot(x_s[...], w_ref[...], 1, 1).astype(BF)

        @pl.when(i == steps - 1)
        def _():
            o_ref[:, :small] = _dot(x_s[...], w_ref[:small, :], 1, 1).astype(BF)

    return pl.pallas_call(
        kernel, grid=(steps,), in_specs=[ANY] * n + [pl.BlockSpec((bn, d), lambda i: (i, 0))],
        out_specs=pl.BlockSpec((rows, bn), lambda i: (0, i)), out_shape=jax.ShapeDtypeStruct((rows, cols), BF),
        scratch_shapes=[pltpu.VMEM((rows, d), BF), pltpu.SemaphoreType.DMA((n,))], compiler_params=_params(40),
        cost_estimate=_price(2 * rows * d * cols, [*pieces, w]), name=name,
    )(*pieces, w)


def mlp(pieces, dhid, wg, wu, bn=256):
    n, (d, cols) = len(pieces), wg.shape
    rows = _rows(pieces)

    def kernel(*refs):
        xs, (dhid_ref, g_ref, u_ref), (hid_ref, dg_ref, du_ref), (x_s, sems) = refs[:n], refs[n : n + 3], refs[n + 3 : n + 6], refs[n + 6 :]

        @pl.when(pl.program_id(0) == 0)
        def _():
            for c in _load(xs, x_s, sems):
                c.wait()

        gate, up = _dot(x_s[...], g_ref[...], 1, 0), _dot(x_s[...], u_ref[...], 1, 0)
        dhid = dhid_ref[...].astype(F32)
        sig = jax.nn.sigmoid(gate)
        silu = gate * sig
        hid_ref[...] = (silu * up).astype(BF)
        du_ref[...] = (dhid * silu).astype(BF)
        dg_ref[...] = (dhid * up * (sig + silu * (1 - sig))).astype(BF)

    w, o = pl.BlockSpec((d, bn), lambda i: (0, i)), pl.BlockSpec((rows, bn), lambda i: (0, i))
    return pl.pallas_call(
        kernel, grid=(-(-cols // bn),), in_specs=[ANY] * n + [o, w, w], out_specs=[o, o, o],
        out_shape=[jax.ShapeDtypeStruct((rows, cols), BF)] * 3,
        scratch_shapes=[pltpu.VMEM((rows, d), BF), pltpu.SemaphoreType.DMA((n,))], compiler_params=_params(40),
        cost_estimate=_price(4 * rows * d * cols, [*pieces, wg, wu, dhid, dhid, dhid]), name="mlp",
    )(*pieces, dhid, wg, wu)


def back(xs, ws, bn, name):
    n, d = len(xs), ws[0].shape[0]
    rows = xs[0][0].shape[0] if isinstance(xs[0], tuple) else xs[0].shape[0]

    def kernel(*refs):
        x, w, (a_ref, b_ref) = refs[:n], refs[n : 2 * n], refs[2 * n :]
        total = _dot(x[0][...], w[0][...], 1, 1)
        for i in range(1, n):
            total += _dot(x[i][...], w[i][...], 1, 1)
        total = total.astype(BF)
        a_ref[...], b_ref[...] = total[:BLOCK], total[BLOCK:]

    o = pl.BlockSpec((BLOCK, bn), lambda i: (0, i))
    return pl.pallas_call(
        kernel, grid=(d // bn,),
        in_specs=[pl.BlockSpec(x.shape, lambda i: (0, 0)) for x in xs] + [pl.BlockSpec((bn, w.shape[1]), lambda i: (i, 0)) for w in ws],
        out_specs=[o, o], out_shape=[jax.ShapeDtypeStruct((BLOCK, d), BF)] * 2, compiler_params=_params(48),
        cost_estimate=_price(sum(2 * rows * d * w.shape[1] for w in ws), [*xs, *ws]), name=name,
    )(*xs, *ws)


def weight_grads(lefts, rights, bm, name):
    n, m, rows = len(lefts), lefts[0].shape[1], _rows(lefts)
    counts = [len(r) for r in rights]
    widths = [r[0].shape[1] for r in rights]

    def kernel(*refs):
        ls, refs = refs[:n], refs[n:]
        rs = []
        for c in counts:
            rs.append(refs[:c])
            refs = refs[c:]
        outs, wholes, sems = refs[: len(rights)], refs[len(rights) : 2 * len(rights)], refs[2 * len(rights) :]

        @pl.when(pl.program_id(0) == 0)
        def _():
            for c in [c for r, w, s in zip(rs, wholes, sems) for c in _load(r, w, s)]:
                c.wait()

        left = jnp.concatenate([l[...] for l in ls], axis=0).T
        for o, w in zip(outs, wholes):
            o[...] = _dot(left, w[...], 1, 0).astype(BF)

    return pl.pallas_call(
        kernel, grid=(m // bm,),
        in_specs=[pl.BlockSpec((l.shape[0], bm), lambda i: (0, i)) for l in lefts] + [ANY] * sum(counts),
        out_specs=[pl.BlockSpec((bm, w), lambda i: (i, 0)) for w in widths],
        out_shape=[jax.ShapeDtypeStruct((m, w), BF) for w in widths],
        scratch_shapes=[pltpu.VMEM((rows, w), BF) for w in widths] + [pltpu.SemaphoreType.DMA((c,)) for c in counts],
        compiler_params=_params(48), cost_estimate=_price(2 * rows * m * sum(widths), [*lefts, *(p for r in rights for p in r)]), name=name,
    )(*lefts, *(p for r in rights for p in r))


CORE = [(0, 1), (1, 0), (2, 3), (3, 2)]
CROSS = [(0, 2), (2, 0), (1, 3), (3, 1)]


def core(v):
    return lax.ppermute(v, "tp", CORE)


def cross(v):
    return lax.ppermute(v, "tp", CROSS)


def after(v, *others):
    return lax.optimization_barrier((v, *others))[0]


def later(pieces, *others):
    return [after(pieces[0], *others), *pieces[1:]]


def gather(v):
    near = core(v)
    first, second = jnp.split(v, 2)
    first = cross(first)
    second = cross(second)
    return [v, near], [first, second, core(first), core(second)]


def scatter_far(mine, other):
    both = (mine.astype(F32) + core(other).astype(F32)).astype(BF)
    return both, cross(both)


def scatter_near(mine, other, far):
    return mine.astype(F32) + core(other).astype(F32) + far.astype(F32)


def mm(a, b, ca, cb):
    return _dot(a, b, ca, cb).astype(BF)


def norm(h):
    wide = h.astype(F32)
    scale = lax.rsqrt(jnp.mean(wide**2, -1, keepdims=True) + 1e-6)
    return (wide * scale).astype(BF), scale


def norm_bwd(h, scale, g):
    wide = h.astype(F32)
    g = g.astype(BF).astype(F32)
    return scale * g - wide * (scale**3 * jnp.mean(g * wide, -1, keepdims=True))


def step(x, dy, wq, wk, wv, wo, wg, wu, wd):
    x, dy = x[0], dy[0]
    me = lax.axis_index("tp").astype(jnp.int32).reshape(1)
    tokens = 4 * x.shape[0]
    half = HEAD // 2
    angle = jnp.arange(tokens, dtype=F32)[:, None] * THETA ** (-jnp.arange(half, dtype=F32) / half)
    cos, sin = jnp.cos(angle), jnp.sin(angle)
    cos, sin = jnp.concatenate([cos, cos], 1), jnp.concatenate([-sin, sin], 1)
    cut = tokens // 2

    a, a_scale = norm(x)
    a_near, a_far = gather(a)
    dy_near = [dy, core(dy)]
    near_qkv = qkv(a_near, wq, wk, wv)
    dhid_near = by_rows_of(later(dy_near, near_qkv[0]), wd, 512, "dhid")
    dy_far = gather(after(dy, a_far[1]))[1]
    far_qkv = qkv(later(a_far, dhid_near), wq, wk, wv)
    q, k, v = (jnp.concatenate(t) for t in zip(near_qkv, far_qkv))
    heads, lse, q, k = attend(me, q, k, v, cos, sin)
    cuts = [heads[at : at + BLOCK] for at in range(0, tokens, BLOCK)]
    other = mm(cuts[3], wo, 1, 0)
    mine = mm(after(cuts[2], other), wo, 1, 0)
    near_other = mm(after(cuts[1], mine), wo, 1, 0)
    near_mine = mm(after(cuts[0], near_other), wo, 1, 0)
    both, far = scatter_far(mine, other)
    dhid_far = by_rows_of(later(dy_far, both, near_mine), wd, 512, "dhid")
    h = (x.astype(F32) + scatter_near(near_mine, near_other, after(far, dhid_far))).astype(BF)
    b, b_scale = norm(h)
    b_near, b_far = gather(b)
    hid_near, dgate_near, dup_near = mlp(b_near, dhid_near, wg, wu)
    hid_far, dgate_far, dup_far = mlp(later(b_far, hid_near), dhid_far, wg, wu)
    both, far = scatter_far(*back([dgate_far, dup_far], [wg, wu], 512, "by_b"))
    near = back(later([dgate_near, dup_near], both), [wg, wu], 512, "by_b")
    (d_wd,) = weight_grads(later([hid_near, hid_far], near[0]), [[*dy_near, *dy_far]], 640, "by_wd")
    db = scatter_near(*near, after(far, d_wd))
    dh = (dy.astype(F32) + norm_bwd(h, b_scale, db)).astype(BF)
    dh_near, dh_far = gather(dh)
    dheads_near = by_rows_of(dh_near, wo, 512, "by_heads")
    (d_wg,) = weight_grads(later([*b_near, *b_far], dheads_near), [[dgate_near, dgate_far]], 512, "by_wg")
    dheads_far = by_rows_of(later(dh_far, d_wg), wo, 512, "by_heads")
    dq, dk, dv = attend_bwd(me, q, k, v, jnp.concatenate([dheads_near, dheads_far]), heads, lse, cos, sin)
    both, far = scatter_far(*back([t[cut:] for t in (dq, dk, dv)], [wq, wk, wv], 512, "by_a"))
    near = back(later([t[:cut] for t in (dq, dk, dv)], both), [wq, wk, wv], 512, "by_a")
    d_wq, d_wk, d_wv = weight_grads(later([*a_near, *a_far], near[0]), [[dq], [dk], [dv]], 512, "by_wqkv")
    (d_wo,) = weight_grads(later([heads], d_wq), [[*dh_near, *dh_far]], 512, "by_wo")
    (d_wu,) = weight_grads(later([*b_near, *b_far], d_wo), [[dup_near, dup_far]], 512, "by_wu")
    da = scatter_near(*near, after(far, d_wu))
    dx = (dh.astype(F32) + norm_bwd(x, a_scale, da)).astype(BF)
    return (dx[None], d_wq, d_wk, d_wv, d_wo, d_wg, d_wu, d_wd)


def solution(mesh):
    states, by_columns, by_rows = P("dp", "tp", None), P(None, "tp"), P("tp", None)
    weights = (by_columns, by_columns, by_columns, by_rows, by_columns, by_columns, by_rows)
    own = tuple(P("dp", "tp") if spec == by_columns else P(("dp", "tp"), None) for spec in weights)
    return jax.shard_map(step, mesh=mesh, in_specs=(states, states, *weights), out_specs=(states, *own), check_vma=False)
```

```python
import functools

import jax
import jax.numpy as jnp
from jax import lax
from jax.experimental import pallas as pl
from jax.experimental.pallas import tpu as pltpu
from jax.sharding import PartitionSpec as P

HEAD = 128
THETA = 10000
LOG2E = 1.4426950408889634
NEG = -1e30
HIDDEN = 2 * NEG
SCALE = HEAD**-0.5
BF, F32 = jnp.bfloat16, jnp.float32
VMEM = 56 * 2**20
BLOCK = 256
STRIP = 512


def _dot(a, b, ca, cb):
    return lax.dot_general(a, b, (((ca,), (cb,)), ((), ())), preferred_element_type=F32)


def _rope(x, cos, sin):
    x = x.astype(F32)
    return x * cos + pltpu.roll(x, HEAD // 2, 1) * sin


def _unrope(x, cos, sin):
    return x * cos - pltpu.roll(x, HEAD // 2, 1) * sin


def _hidden(cols):
    key = lax.broadcasted_iota(jnp.int32, (BLOCK, cols), 0)
    return key > lax.rem(lax.broadcasted_iota(jnp.int32, (BLOCK, cols), 1), BLOCK)


def _attend(me_ref, q_ref, k_ref, v_ref, cos_ref, sin_ref, o_ref, lse_ref, qr_ref, kr_ref, vt_s, q_s, top_s, mix_s):
    iq = pl.program_id(1)
    me = me_ref[0]
    n = k_ref.shape[0] // BLOCK
    g = q_ref.shape[1] // HEAD
    cols = g * BLOCK
    e = SCALE * LOG2E

    @pl.when(iq == 0)
    def _():
        for s in range(n):
            here = pl.ds((s ^ me) * BLOCK, BLOCK)
            rows = slice(s * BLOCK, (s + 1) * BLOCK)
            kr_ref[rows, :] = _rope(k_ref[rows, :], cos_ref[here, :], sin_ref[here, :]).astype(BF)
            vt_s[s, :HEAD, :] = v_ref[rows, :].T
            vt_s[s, HEAD:, :] = jnp.ones((8, BLOCK), BF)

    here = pl.ds(iq * BLOCK, BLOCK)
    cos, sin = cos_ref[here, :], sin_ref[here, :]
    for h in range(g):
        turned = _rope(q_ref[:, h * HEAD : (h + 1) * HEAD], cos, sin).astype(BF)
        qr_ref[:, h * HEAD : (h + 1) * HEAD] = turned
        q_s[h * BLOCK : (h + 1) * BLOCK, :] = turned
    top_s[...] = jnp.full((1, cols), NEG, F32)
    mix_s[...] = jnp.zeros((HEAD + 8, cols), F32)

    def block(j, masked):
        slot = j ^ me
        keys = kr_ref[pl.ds(slot * BLOCK, BLOCK), :]
        strips = range(0, cols, STRIP)
        scores = [_dot(keys, q_s[at : at + STRIP, :], 1, 1) for at in strips]
        weights, keeps = [], []
        for at, s in zip(strips, scores):
            if masked:
                s = jnp.where(_hidden(STRIP), HIDDEN, s)
            old = top_s[:, at : at + STRIP]
            top = jnp.maximum(old, s.max(axis=0, keepdims=True))
            top_s[:, at : at + STRIP] = top
            weights.append(jnp.exp2((s - top) * e).astype(BF))
            keeps.append(jnp.exp2((old - top) * e))
        for at, p, keep in zip(strips, weights, keeps):
            mix_s[:, at : at + STRIP] = mix_s[:, at : at + STRIP] * keep + _dot(vt_s[slot], p, 1, 0)

    lax.fori_loop(0, iq, lambda j, _: block(j, False), None)
    block(iq, True)
    total = mix_s[HEAD : HEAD + 1, :]
    out = (mix_s[:HEAD, :] * (1 / total)).T.astype(BF)
    for h in range(g):
        o_ref[:, h * HEAD : (h + 1) * HEAD] = out[h * BLOCK : (h + 1) * BLOCK, :]
    lse_ref[0] = top_s[...] * e + jnp.log2(total)


def _attend_bwd(me_ref, q_ref, k_ref, v_ref, do_ref, o_ref, lse_ref, cos_ref, sin_ref, dq_ref, dk_ref, dv_ref,
                q_s, do_s, dq_s, dk_s, dv_s, kt_s, delta_s):
    iq = pl.program_id(1)
    me = me_ref[0]
    n = k_ref.shape[0] // BLOCK
    g = q_ref.shape[1] // HEAD
    cols = g * BLOCK
    e = SCALE * LOG2E

    @pl.when(iq == 0)
    def _():
        dk_s[...] = jnp.zeros_like(dk_s)
        dv_s[...] = jnp.zeros_like(dv_s)
        for s in range(n):
            kt_s[s] = k_ref[s * BLOCK : (s + 1) * BLOCK, :].T

    dq_s[...] = jnp.zeros_like(dq_s)
    for h in range(g):
        lanes, rows = slice(h * HEAD, (h + 1) * HEAD), slice(h * BLOCK, (h + 1) * BLOCK)
        q_s[rows, :] = q_ref[:, lanes]
        do_s[rows, :] = do_ref[:, lanes]
        prod = do_ref[:, lanes].astype(F32) * o_ref[:, lanes].astype(F32)
        delta_s[:, rows] = prod.T.sum(axis=0, keepdims=True)

    def block(j, masked):
        slot = j ^ me
        here = pl.ds(slot * BLOCK, BLOCK)
        keys, values = k_ref[here, :], v_ref[here, :]
        strips = range(0, cols, STRIP)
        scores = [_dot(keys, q_s[at : at + STRIP, :], 1, 1) for at in strips]
        dps = [_dot(values, do_s[at : at + STRIP, :], 1, 1) for at in strips]
        for at, s, dp in zip(strips, scores, dps):
            p = jnp.exp2(s * e - lse_ref[0, :, at : at + STRIP])
            if masked:
                p = jnp.where(_hidden(STRIP), 0.0, p)
            ds = (p * (dp - delta_s[:, at : at + STRIP])).astype(BF)
            dv_s[here, :] += _dot(p.astype(BF), do_s[at : at + STRIP, :], 1, 0)
            dk_s[here, :] += _dot(ds, q_s[at : at + STRIP, :], 1, 0)
            dq_s[:, at : at + STRIP] += _dot(kt_s[slot], ds, 1, 0)

    lax.fori_loop(0, iq, lambda j, _: block(j, False), None)
    block(iq, True)
    here = pl.ds(iq * BLOCK, BLOCK)
    cos, sin = cos_ref[here, :], sin_ref[here, :]
    dq = (dq_s[...] * SCALE).T
    for h in range(g):
        dq_ref[:, h * HEAD : (h + 1) * HEAD] = _unrope(dq[h * BLOCK : (h + 1) * BLOCK, :], cos, sin).astype(BF)

    @pl.when(iq == n - 1)
    def _():
        for s in range(n):
            here = pl.ds((s ^ me) * BLOCK, BLOCK)
            rows = slice(s * BLOCK, (s + 1) * BLOCK)
            dk_ref[rows, :] = _unrope(dk_s[rows, :] * SCALE, cos_ref[here, :], sin_ref[here, :]).astype(BF)
            dv_ref[rows, :] = dv_s[rows, :].astype(BF)


def _attn_specs(tokens, g):
    queries = pl.BlockSpec((BLOCK, g * HEAD), lambda h, i, me: (i ^ me[0], h))
    keys = pl.BlockSpec((tokens, HEAD), lambda h, i, me: (0, h))
    table = pl.BlockSpec((tokens, HEAD), lambda h, i, me: (0, 0))
    stats = pl.BlockSpec((1, 1, g * BLOCK), lambda h, i, me: (h * (tokens // BLOCK) + i, 0, 0))
    return queries, keys, table, stats


def attend(me, q, k, v, cos, sin):
    tokens, kv = k.shape[0], k.shape[1] // HEAD
    g = q.shape[1] // k.shape[1]
    queries, keys, table, stats = _attn_specs(tokens, g)
    n = tokens // BLOCK
    return pl.pallas_call(
        _attend,
        grid_spec=pltpu.PrefetchScalarGridSpec(
            num_scalar_prefetch=1, grid=(kv, n), in_specs=[queries, keys, keys, table, table], out_specs=[queries, stats, queries, keys],
            scratch_shapes=[pltpu.VMEM((n, HEAD + 8, BLOCK), BF), pltpu.VMEM((g * BLOCK, HEAD), BF), pltpu.VMEM((1, g * BLOCK), F32),
                            pltpu.VMEM((HEAD + 8, g * BLOCK), F32)]),
        out_shape=[jax.ShapeDtypeStruct(q.shape, BF), jax.ShapeDtypeStruct((kv * n, 1, g * BLOCK), F32), jax.ShapeDtypeStruct(q.shape, BF),
                   jax.ShapeDtypeStruct(k.shape, BF)],
        compiler_params=pltpu.CompilerParams(dimension_semantics=("arbitrary", "arbitrary"), vmem_limit_bytes=24 * 2**20),
        cost_estimate=pl.CostEstimate(flops=12 * 10**9, transcendentals=0, bytes_accessed=8 * 2**20),
        name="attend",
    )(me, q, k, v, cos, sin)


def attend_bwd(me, q, k, v, do, o, lse, cos, sin):
    tokens, kv = k.shape[0], k.shape[1] // HEAD
    g = q.shape[1] // k.shape[1]
    queries, keys, table, stats = _attn_specs(tokens, g)
    n = tokens // BLOCK
    return pl.pallas_call(
        _attend_bwd,
        grid_spec=pltpu.PrefetchScalarGridSpec(
            num_scalar_prefetch=1, grid=(kv, n), in_specs=[queries, keys, keys, queries, queries, stats, table, table],
            out_specs=[queries, keys, keys],
            scratch_shapes=[pltpu.VMEM((g * BLOCK, HEAD), BF), pltpu.VMEM((g * BLOCK, HEAD), BF), pltpu.VMEM((HEAD, g * BLOCK), F32),
                            pltpu.VMEM((tokens, HEAD), F32), pltpu.VMEM((tokens, HEAD), F32), pltpu.VMEM((n, HEAD, BLOCK), BF),
                            pltpu.VMEM((1, g * BLOCK), F32)]),
        out_shape=[jax.ShapeDtypeStruct(q.shape, BF), jax.ShapeDtypeStruct(k.shape, BF), jax.ShapeDtypeStruct(k.shape, BF)],
        compiler_params=pltpu.CompilerParams(dimension_semantics=("arbitrary", "arbitrary"), vmem_limit_bytes=24 * 2**20),
        cost_estimate=pl.CostEstimate(flops=18 * 10**9, transcendentals=0, bytes_accessed=12 * 2**20),
        name="attend_bwd",
    )(me, q, k, v, do, o, lse, cos, sin)


ANY = pl.BlockSpec(memory_space=pltpu.HBM)


def _load(pieces, whole, sems):
    copies, at = [], 0
    for i, piece in enumerate(pieces):
        n = piece.shape[0]
        copies.append(pltpu.make_async_copy(piece, whole.at[pl.ds(at, n), :], sems.at[i]))
        at += n
    for c in copies:
        c.start()
    return copies


def _params(mib, steps=1):
    return pltpu.CompilerParams(dimension_semantics=("arbitrary",) * steps, vmem_limit_bytes=mib * 2**20)


def _price(flops, arrays):
    return pl.CostEstimate(flops=flops, transcendentals=0, bytes_accessed=sum(a.size * 2 for a in arrays))


def _rows(pieces):
    return sum(p.shape[0] for p in pieces)


def qkv(pieces, wq, wk, wv):
    n, (d, nq), nk = len(pieces), wq.shape, wk.shape[1]
    rows, cut = _rows(pieces), 512

    def kernel(*refs):
        xs, (wq_ref, wk_ref, wv_ref), (q_ref, k_ref, v_ref) = refs[:n], refs[n : n + 3], refs[n + 3 : n + 6]
        x_s, q_s, k_s, v_s, sems, wsems = refs[n + 6 :]
        copies = _load(xs, x_s, sems)
        todo = []
        for i, at in enumerate(range(0, nq, cut)):
            here = slice(at, at + cut)
            todo.append((pltpu.make_async_copy(wq_ref.at[:, here], q_s.at[:, here], wsems.at[i]), q_s.at[:, here], q_ref, here))
        for i, (w, w_s, o) in enumerate(((wk_ref, k_s, k_ref), (wv_ref, v_s, v_ref))):
            todo.append((pltpu.make_async_copy(w, w_s, wsems.at[nq // cut + i]), w_s, o, slice(0, nk)))
        for t in todo:
            t[0].start()
        for c in copies:
            c.wait()
        for c, w_s, o, here in todo:
            c.wait()
            o[:, here] = _dot(x_s[...], w_s[...], 1, 0).astype(BF)

    return pl.pallas_call(
        kernel, in_specs=[ANY] * (n + 3), out_specs=[pl.BlockSpec(memory_space=pltpu.VMEM)] * 3,
        out_shape=[jax.ShapeDtypeStruct((rows, m), BF) for m in (nq, nk, nk)],
        scratch_shapes=[pltpu.VMEM((rows, d), BF), pltpu.VMEM((d, nq), BF), pltpu.VMEM((d, nk), BF), pltpu.VMEM((d, nk), BF),
                        pltpu.SemaphoreType.DMA((n,)), pltpu.SemaphoreType.DMA((nq // cut + 2,))],
        compiler_params=pltpu.CompilerParams(vmem_limit_bytes=30 * 2**20),
        cost_estimate=_price(2 * rows * d * (nq + 2 * nk), [*pieces, wq, wk, wv]), name="qkv",
    )(*pieces, wq, wk, wv)


def by_rows_of(pieces, w, bn, name):
    n, (cols, d) = len(pieces), w.shape
    rows = _rows(pieces)
    steps, rest = -(-cols // bn), cols % bn
    small = -(-rest // 256) * 256

    def kernel(*refs):
        xs, w_ref, o_ref, x_s, sems = refs[:n], refs[n], refs[n + 1], refs[n + 2], refs[n + 3]
        i = pl.program_id(0)

        @pl.when(i == 0)
        def _():
            for c in _load(xs, x_s, sems):
                c.wait()

        if rest == 0 or small == bn:
            o_ref[...] = _dot(x_s[...], w_ref[...], 1, 1).astype(BF)
            return

        @pl.when(i < steps - 1)
        def _():
            o_ref[...] = _dot(x_s[...], w_ref[...], 1, 1).astype(BF)

        @pl.when(i == steps - 1)
        def _():
            o_ref[:, :small] = _dot(x_s[...], w_ref[:small, :], 1, 1).astype(BF)

    return pl.pallas_call(
        kernel, grid=(steps,), in_specs=[ANY] * n + [pl.BlockSpec((bn, d), lambda i: (i, 0))],
        out_specs=pl.BlockSpec((rows, bn), lambda i: (0, i)), out_shape=jax.ShapeDtypeStruct((rows, cols), BF),
        scratch_shapes=[pltpu.VMEM((rows, d), BF), pltpu.SemaphoreType.DMA((n,))], compiler_params=_params(40),
        cost_estimate=_price(2 * rows * d * cols, [*pieces, w]), name=name,
    )(*pieces, w)


def mlp(pieces, dhid, wg, wu, bn=256):
    n, (d, cols) = len(pieces), wg.shape
    rows = _rows(pieces)

    def kernel(*refs):
        xs, (dhid_ref, g_ref, u_ref), (hid_ref, dg_ref, du_ref), (x_s, sems) = refs[:n], refs[n : n + 3], refs[n + 3 : n + 6], refs[n + 6 :]

        @pl.when(pl.program_id(0) == 0)
        def _():
            for c in _load(xs, x_s, sems):
                c.wait()

        gate, up = _dot(x_s[...], g_ref[...], 1, 0), _dot(x_s[...], u_ref[...], 1, 0)
        dhid = dhid_ref[...].astype(F32)
        sig = jax.nn.sigmoid(gate)
        silu = gate * sig
        hid_ref[...] = (silu * up).astype(BF)
        du_ref[...] = (dhid * silu).astype(BF)
        dg_ref[...] = (dhid * up * (sig + silu * (1 - sig))).astype(BF)

    w, o = pl.BlockSpec((d, bn), lambda i: (0, i)), pl.BlockSpec((rows, bn), lambda i: (0, i))
    return pl.pallas_call(
        kernel, grid=(-(-cols // bn),), in_specs=[ANY] * n + [o, w, w], out_specs=[o, o, o],
        out_shape=[jax.ShapeDtypeStruct((rows, cols), BF)] * 3,
        scratch_shapes=[pltpu.VMEM((rows, d), BF), pltpu.SemaphoreType.DMA((n,))], compiler_params=_params(56),
        cost_estimate=_price(4 * rows * d * cols, [*pieces, wg, wu, dhid, dhid, dhid]), name="mlp",
    )(*pieces, dhid, wg, wu)


def back(xs, ws, bn, name):
    n, d = len(xs), ws[0].shape[0]
    rows = xs[0][0].shape[0] if isinstance(xs[0], tuple) else xs[0].shape[0]

    def kernel(*refs):
        x, w, (a_ref, b_ref) = refs[:n], refs[n : 2 * n], refs[2 * n :]
        total = _dot(x[0][...], w[0][...], 1, 1)
        for i in range(1, n):
            total += _dot(x[i][...], w[i][...], 1, 1)
        total = total.astype(BF)
        a_ref[...], b_ref[...] = total[:BLOCK], total[BLOCK:]

    o = pl.BlockSpec((BLOCK, bn), lambda i: (0, i))
    return pl.pallas_call(
        kernel, grid=(d // bn,),
        in_specs=[pl.BlockSpec(x.shape, lambda i: (0, 0)) for x in xs] + [pl.BlockSpec((bn, w.shape[1]), lambda i: (i, 0)) for w in ws],
        out_specs=[o, o], out_shape=[jax.ShapeDtypeStruct((BLOCK, d), BF)] * 2, compiler_params=_params(48),
        cost_estimate=_price(sum(2 * rows * d * w.shape[1] for w in ws), [*xs, *ws]), name=name,
    )(*xs, *ws)


def weight_grads(lefts, rights, bm, name):
    n, m, rows = len(lefts), lefts[0].shape[1], _rows(lefts)
    counts = [len(r) for r in rights]
    widths = [r[0].shape[1] for r in rights]

    def kernel(*refs):
        ls, refs = refs[:n], refs[n:]
        rs = []
        for c in counts:
            rs.append(refs[:c])
            refs = refs[c:]
        outs, wholes, sems = refs[: len(rights)], refs[len(rights) : 2 * len(rights)], refs[2 * len(rights) :]

        @pl.when(pl.program_id(0) == 0)
        def _():
            for c in [c for r, w, s in zip(rs, wholes, sems) for c in _load(r, w, s)]:
                c.wait()

        left = jnp.concatenate([l[...] for l in ls], axis=0).T
        for o, w in zip(outs, wholes):
            o[...] = _dot(left, w[...], 1, 0).astype(BF)

    return pl.pallas_call(
        kernel, grid=(m // bm,),
        in_specs=[pl.BlockSpec((l.shape[0], bm), lambda i: (0, i)) for l in lefts] + [ANY] * sum(counts),
        out_specs=[pl.BlockSpec((bm, w), lambda i: (i, 0)) for w in widths],
        out_shape=[jax.ShapeDtypeStruct((m, w), BF) for w in widths],
        scratch_shapes=[pltpu.VMEM((rows, w), BF) for w in widths] + [pltpu.SemaphoreType.DMA((c,)) for c in counts],
        compiler_params=_params(48), cost_estimate=_price(2 * rows * m * sum(widths), [*lefts, *(p for r in rights for p in r)]), name=name,
    )(*lefts, *(p for r in rights for p in r))


CORE = [(0, 1), (1, 0), (2, 3), (3, 2)]
CROSS = [(0, 2), (2, 0), (1, 3), (3, 1)]


def core(v):
    return lax.ppermute(v, "tp", CORE)


def cross(v):
    return lax.ppermute(v, "tp", CROSS)


def after(v, *others):
    return lax.optimization_barrier((v, *others))[0]


def later(pieces, *others):
    return [after(pieces[0], *others), *pieces[1:]]


def gather(v):
    return [v, core(v)], cross(v)


def far_of(first, *others):
    first = after(first, *others)
    return [first, core(first)]


def scatter_far(mine, other):
    both = (mine.astype(F32) + core(other).astype(F32)).astype(BF)
    return both, cross(both)


def scatter_near(mine, other, far):
    return mine.astype(F32) + core(other).astype(F32) + far.astype(F32)


def mm(a, b, ca, cb):
    return _dot(a, b, ca, cb).astype(BF)


def norm(h):
    wide = h.astype(F32)
    scale = lax.rsqrt(jnp.mean(wide**2, -1, keepdims=True) + 1e-6)
    return (wide * scale).astype(BF), scale


def norm_bwd(h, scale, g):
    wide = h.astype(F32)
    g = g.astype(BF).astype(F32)
    return scale * g - wide * (scale**3 * jnp.mean(g * wide, -1, keepdims=True))


def step(x, dy, wq, wk, wv, wo, wg, wu, wd):
    x, dy = x[0], dy[0]
    me = lax.axis_index("tp").astype(jnp.int32).reshape(1)
    tokens = 4 * x.shape[0]
    half = HEAD // 2
    angle = jnp.arange(tokens, dtype=F32)[:, None] * THETA ** (-jnp.arange(half, dtype=F32) / half)
    cos, sin = jnp.cos(angle), jnp.sin(angle)
    cos, sin = jnp.concatenate([cos, cos], 1), jnp.concatenate([-sin, sin], 1)
    cut = tokens // 2

    a, a_scale = norm(x)
    a_near, a_far = gather(a)
    dy_near = [dy, core(dy)]
    near_qkv = qkv(a_near, wq, wk, wv)
    dhid_near = by_rows_of(later(dy_near, near_qkv[0]), wd, 512, "dhid")
    a_far = far_of(a_far, dhid_near)
    dy_far = cross(after(dy, a_far[0]))
    far_qkv = qkv(a_far, wq, wk, wv)
    q, k, v = (jnp.concatenate(t) for t in zip(near_qkv, far_qkv))
    heads, lse, q, k = attend(me, q, k, v, cos, sin)
    cuts = [heads[at : at + BLOCK] for at in range(0, tokens, BLOCK)]
    other = mm(cuts[3], wo, 1, 0)
    mine = mm(after(cuts[2], other), wo, 1, 0)
    near_other = mm(after(cuts[1], mine), wo, 1, 0)
    near_mine = mm(after(cuts[0], near_other), wo, 1, 0)
    both, far = scatter_far(mine, other)
    dy_far = far_of(dy_far, both, near_mine)
    dhid_far = by_rows_of(dy_far, wd, 512, "dhid")
    h = (x.astype(F32) + scatter_near(near_mine, near_other, after(far, dhid_far))).astype(BF)
    b, b_scale = norm(h)
    b_near, b_far = gather(b)
    hid_near, dgate_near, dup_near = mlp(b_near, dhid_near, wg, wu)
    b_far = far_of(b_far, hid_near)
    hid_far, dgate_far, dup_far = mlp(b_far, dhid_far, wg, wu)
    both, far = scatter_far(*back([dgate_far, dup_far], [wg, wu], 512, "by_b"))
    near = back(later([dgate_near, dup_near], both), [wg, wu], 512, "by_b")
    (d_wd,) = weight_grads(later([hid_near, hid_far], near[0]), [[*dy_near, *dy_far]], 640, "by_wd")
    db = scatter_near(*near, after(far, d_wd))
    dh = (dy.astype(F32) + norm_bwd(h, b_scale, db)).astype(BF)
    dh_near, dh_far = gather(dh)
    dheads_near = by_rows_of(dh_near, wo, 512, "by_heads")
    (d_wg,) = weight_grads(later([*b_near, *b_far], dheads_near), [[dgate_near, dgate_far]], 512, "by_wg")
    dh_far = far_of(dh_far, d_wg)
    dheads_far = by_rows_of(dh_far, wo, 512, "by_heads")
    dq, dk, dv = attend_bwd(me, q, k, v, jnp.concatenate([dheads_near, dheads_far]), heads, lse, cos, sin)
    both, far = scatter_far(*back([t[cut:] for t in (dq, dk, dv)], [wq, wk, wv], 512, "by_a"))
    near = back(later([t[:cut] for t in (dq, dk, dv)], both), [wq, wk, wv], 512, "by_a")
    d_wq, d_wk, d_wv = weight_grads(later([*a_near, *a_far], near[0]), [[dq], [dk], [dv]], 512, "by_wqkv")
    (d_wo,) = weight_grads(later([heads], d_wq), [[*dh_near, *dh_far]], 512, "by_wo")
    (d_wu,) = weight_grads(later([*b_near, *b_far], d_wo), [[dup_near, dup_far]], 512, "by_wu")
    da = scatter_near(*near, after(far, d_wu))
    dx = (dh.astype(F32) + norm_bwd(x, a_scale, da)).astype(BF)
    return (dx[None], d_wq, d_wk, d_wv, d_wo, d_wg, d_wu, d_wd)


def solution(mesh):
    states, by_columns, by_rows = P("dp", "tp", None), P(None, "tp"), P("tp", None)
    weights = (by_columns, by_columns, by_columns, by_rows, by_columns, by_columns, by_rows)
    own = tuple(P("dp", "tp") if spec == by_columns else P(("dp", "tp"), None) for spec in weights)
    return jax.shard_map(step, mesh=mesh, in_specs=(states, states, *weights), out_specs=(states, *own), check_vma=False)
```

```python
import jax
import jax.numpy as jnp
from jax import lax
from jax.experimental import pallas as pl
from jax.experimental.pallas import tpu as pltpu
from jax.sharding import PartitionSpec as P


HEAD = 128
THETA = 10000
LOG2E = 1.4426950408889634
NEG = -1e30
HIDDEN = 2 * NEG
SCALE = HEAD**-0.5
BF, F32 = jnp.bfloat16, jnp.float32
BLOCK = 256
STRIP = 512


def _dot(a, b, ca, cb):
    return lax.dot_general(a, b, (((ca,), (cb,)), ((), ())), preferred_element_type=F32)


def _rope(x, cos, sin):
    x = x.astype(F32)
    return x * cos + pltpu.roll(x, HEAD // 2, 1) * sin


def _unrope(x, cos, sin):
    return x * cos - pltpu.roll(x, HEAD // 2, 1) * sin


def _hidden(cols):
    key = lax.broadcasted_iota(jnp.int32, (BLOCK, cols), 0)
    return key > lax.rem(lax.broadcasted_iota(jnp.int32, (BLOCK, cols), 1), BLOCK)


def _attend(me_ref, q_ref, k_ref, v_ref, cos_ref, sin_ref, o_ref, lse_ref, qr_ref, kr_ref, vt_s, q_s, top_s, mix_s):
    iq = pl.program_id(1)
    me = me_ref[0]
    n = k_ref.shape[0] // BLOCK
    g = q_ref.shape[1] // HEAD
    cols = g * BLOCK
    e = SCALE * LOG2E

    @pl.when(iq == 0)
    def _():
        for s in range(n):
            here = pl.ds((s ^ me) * BLOCK, BLOCK)
            rows = slice(s * BLOCK, (s + 1) * BLOCK)
            kr_ref[rows, :] = _rope(k_ref[rows, :], cos_ref[here, :], sin_ref[here, :]).astype(BF)
            vt_s[s, :HEAD, :] = v_ref[rows, :].T
            vt_s[s, HEAD:, :] = jnp.ones((8, BLOCK), BF)

    here = pl.ds(iq * BLOCK, BLOCK)
    cos, sin = cos_ref[here, :], sin_ref[here, :]
    for h in range(g):
        turned = _rope(q_ref[:, h * HEAD : (h + 1) * HEAD], cos, sin).astype(BF)
        qr_ref[:, h * HEAD : (h + 1) * HEAD] = turned
        q_s[h * BLOCK : (h + 1) * BLOCK, :] = turned
    top_s[...] = jnp.full((1, cols), NEG, F32)
    mix_s[...] = jnp.zeros((HEAD + 8, cols), F32)

    def block(j, masked):
        slot = j ^ me
        keys = kr_ref[pl.ds(slot * BLOCK, BLOCK), :]
        strips = range(0, cols, STRIP)
        scores = [_dot(keys, q_s[at : at + STRIP, :], 1, 1) for at in strips]
        weights, keeps = [], []
        for at, s in zip(strips, scores):
            if masked:
                s = jnp.where(_hidden(STRIP), HIDDEN, s)
            old = top_s[:, at : at + STRIP]
            top = jnp.maximum(old, s.max(axis=0, keepdims=True))
            top_s[:, at : at + STRIP] = top
            weights.append(jnp.exp2((s - top) * e).astype(BF))
            keeps.append(jnp.exp2((old - top) * e))
        for at, p, keep in zip(strips, weights, keeps):
            mix_s[:, at : at + STRIP] = mix_s[:, at : at + STRIP] * keep + _dot(vt_s[slot], p, 1, 0)

    lax.fori_loop(0, iq, lambda j, _: block(j, False), None)
    block(iq, True)
    total = mix_s[HEAD : HEAD + 1, :]
    out = (mix_s[:HEAD, :] * (1 / total)).T.astype(BF)
    for h in range(g):
        o_ref[:, h * HEAD : (h + 1) * HEAD] = out[h * BLOCK : (h + 1) * BLOCK, :]
    lse_ref[0] = top_s[...] * e + jnp.log2(total)


def _attend_bwd(me_ref, q_ref, k_ref, v_ref, do_ref, o_ref, lse_ref, cos_ref, sin_ref, dq_ref, dk_ref, dv_ref,
                q_s, do_s, dq_s, dk_s, dv_s, kt_s, delta_s):
    iq = pl.program_id(1)
    me = me_ref[0]
    n = k_ref.shape[0] // BLOCK
    g = q_ref.shape[1] // HEAD
    cols = g * BLOCK
    e = SCALE * LOG2E

    @pl.when(iq == 0)
    def _():
        dk_s[...] = jnp.zeros_like(dk_s)
        dv_s[...] = jnp.zeros_like(dv_s)
        for s in range(n):
            kt_s[s] = k_ref[s * BLOCK : (s + 1) * BLOCK, :].T

    dq_s[...] = jnp.zeros_like(dq_s)
    for h in range(g):
        lanes, rows = slice(h * HEAD, (h + 1) * HEAD), slice(h * BLOCK, (h + 1) * BLOCK)
        q_s[rows, :] = q_ref[:, lanes]
        do_s[rows, :] = do_ref[:, lanes]
        prod = do_ref[:, lanes].astype(F32) * o_ref[:, lanes].astype(F32)
        delta_s[:, rows] = prod.T.sum(axis=0, keepdims=True)

    def block(j, masked):
        slot = j ^ me
        here = pl.ds(slot * BLOCK, BLOCK)
        keys, values = k_ref[here, :], v_ref[here, :]
        strips = range(0, cols, STRIP)
        scores = [_dot(keys, q_s[at : at + STRIP, :], 1, 1) for at in strips]
        dps = [_dot(values, do_s[at : at + STRIP, :], 1, 1) for at in strips]
        for at, s, dp in zip(strips, scores, dps):
            p = jnp.exp2(s * e - lse_ref[0, :, at : at + STRIP])
            if masked:
                p = jnp.where(_hidden(STRIP), 0.0, p)
            ds = (p * (dp - delta_s[:, at : at + STRIP])).astype(BF)
            dv_s[here, :] += _dot(p.astype(BF), do_s[at : at + STRIP, :], 1, 0)
            dk_s[here, :] += _dot(ds, q_s[at : at + STRIP, :], 1, 0)
            dq_s[:, at : at + STRIP] += _dot(kt_s[slot], ds, 1, 0)

    lax.fori_loop(0, iq, lambda j, _: block(j, False), None)
    block(iq, True)
    here = pl.ds(iq * BLOCK, BLOCK)
    cos, sin = cos_ref[here, :], sin_ref[here, :]
    dq = (dq_s[...] * SCALE).T
    for h in range(g):
        dq_ref[:, h * HEAD : (h + 1) * HEAD] = _unrope(dq[h * BLOCK : (h + 1) * BLOCK, :], cos, sin).astype(BF)

    @pl.when(iq == n - 1)
    def _():
        for s in range(n):
            here = pl.ds((s ^ me) * BLOCK, BLOCK)
            rows = slice(s * BLOCK, (s + 1) * BLOCK)
            dk_ref[rows, :] = _unrope(dk_s[rows, :] * SCALE, cos_ref[here, :], sin_ref[here, :]).astype(BF)
            dv_ref[rows, :] = dv_s[rows, :].astype(BF)


def _attn_specs(tokens, g):
    queries = pl.BlockSpec((BLOCK, g * HEAD), lambda h, i, me: (i ^ me[0], h))
    keys = pl.BlockSpec((tokens, HEAD), lambda h, i, me: (0, h))
    table = pl.BlockSpec((tokens, HEAD), lambda h, i, me: (0, 0))
    stats = pl.BlockSpec((1, 1, g * BLOCK), lambda h, i, me: (h * (tokens // BLOCK) + i, 0, 0))
    return queries, keys, table, stats


def attend(me, q, k, v, cos, sin):
    tokens, kv = k.shape[0], k.shape[1] // HEAD
    g = q.shape[1] // k.shape[1]
    queries, keys, table, stats = _attn_specs(tokens, g)
    n = tokens // BLOCK
    return pl.pallas_call(
        _attend,
        grid_spec=pltpu.PrefetchScalarGridSpec(
            num_scalar_prefetch=1, grid=(kv, n), in_specs=[queries, keys, keys, table, table], out_specs=[queries, stats, queries, keys],
            scratch_shapes=[pltpu.VMEM((n, HEAD + 8, BLOCK), BF), pltpu.VMEM((g * BLOCK, HEAD), BF), pltpu.VMEM((1, g * BLOCK), F32),
                            pltpu.VMEM((HEAD + 8, g * BLOCK), F32)]),
        out_shape=[jax.ShapeDtypeStruct(q.shape, BF), jax.ShapeDtypeStruct((kv * n, 1, g * BLOCK), F32), jax.ShapeDtypeStruct(q.shape, BF),
                   jax.ShapeDtypeStruct(k.shape, BF)],
        compiler_params=pltpu.CompilerParams(dimension_semantics=("arbitrary", "arbitrary"), vmem_limit_bytes=24 * 2**20),
        cost_estimate=pl.CostEstimate(flops=12 * 10**9, transcendentals=0, bytes_accessed=8 * 2**20),
        name="attend",
    )(me, q, k, v, cos, sin)


def attend_bwd(me, q, k, v, do, o, lse, cos, sin):
    tokens, kv = k.shape[0], k.shape[1] // HEAD
    g = q.shape[1] // k.shape[1]
    queries, keys, table, stats = _attn_specs(tokens, g)
    n = tokens // BLOCK
    return pl.pallas_call(
        _attend_bwd,
        grid_spec=pltpu.PrefetchScalarGridSpec(
            num_scalar_prefetch=1, grid=(kv, n), in_specs=[queries, keys, keys, queries, queries, stats, table, table],
            out_specs=[queries, keys, keys],
            scratch_shapes=[pltpu.VMEM((g * BLOCK, HEAD), BF), pltpu.VMEM((g * BLOCK, HEAD), BF), pltpu.VMEM((HEAD, g * BLOCK), F32),
                            pltpu.VMEM((tokens, HEAD), F32), pltpu.VMEM((tokens, HEAD), F32), pltpu.VMEM((n, HEAD, BLOCK), BF),
                            pltpu.VMEM((1, g * BLOCK), F32)]),
        out_shape=[jax.ShapeDtypeStruct(q.shape, BF), jax.ShapeDtypeStruct(k.shape, BF), jax.ShapeDtypeStruct(k.shape, BF)],
        compiler_params=pltpu.CompilerParams(dimension_semantics=("arbitrary", "arbitrary"), vmem_limit_bytes=24 * 2**20),
        cost_estimate=pl.CostEstimate(flops=18 * 10**9, transcendentals=0, bytes_accessed=12 * 2**20),
        name="attend_bwd",
    )(me, q, k, v, do, o, lse, cos, sin)


ANY = pl.BlockSpec(memory_space=pltpu.HBM)


def _load(pieces, whole, sems):
    copies, at = [], 0
    for i, piece in enumerate(pieces):
        n = piece.shape[0]
        copies.append(pltpu.make_async_copy(piece, whole.at[pl.ds(at, n), :], sems.at[i]))
        at += n
    for c in copies:
        c.start()
    return copies


def _params(mib, steps=1):
    return pltpu.CompilerParams(dimension_semantics=("arbitrary",) * steps, vmem_limit_bytes=mib * 2**20)


def _price(flops, arrays):
    return pl.CostEstimate(flops=flops, transcendentals=0, bytes_accessed=sum(a.size * 2 for a in arrays))


def _rows(pieces):
    return sum(p.shape[0] for p in pieces)


def qkv(pieces, wq, wk, wv):
    n, (d, nq), nk = len(pieces), wq.shape, wk.shape[1]
    rows, cut = _rows(pieces), 512

    def kernel(*refs):
        xs, (wq_ref, wk_ref, wv_ref), (q_ref, k_ref, v_ref) = refs[:n], refs[n : n + 3], refs[n + 3 : n + 6]
        x_s, q_s, k_s, v_s, sems, wsems = refs[n + 6 :]
        copies = _load(xs, x_s, sems)
        todo = []
        for i, at in enumerate(range(0, nq, cut)):
            here = slice(at, at + cut)
            todo.append((pltpu.make_async_copy(wq_ref.at[:, here], q_s.at[:, here], wsems.at[i]), q_s.at[:, here], q_ref, here))
        for i, (w, w_s, o) in enumerate(((wk_ref, k_s, k_ref), (wv_ref, v_s, v_ref))):
            todo.append((pltpu.make_async_copy(w, w_s, wsems.at[nq // cut + i]), w_s, o, slice(0, nk)))
        for t in todo:
            t[0].start()
        for c in copies:
            c.wait()
        for c, w_s, o, here in todo:
            c.wait()
            o[:, here] = _dot(x_s[...], w_s[...], 1, 0).astype(BF)

    return pl.pallas_call(
        kernel, in_specs=[ANY] * (n + 3), out_specs=[pl.BlockSpec(memory_space=pltpu.VMEM)] * 3,
        out_shape=[jax.ShapeDtypeStruct((rows, m), BF) for m in (nq, nk, nk)],
        scratch_shapes=[pltpu.VMEM((rows, d), BF), pltpu.VMEM((d, nq), BF), pltpu.VMEM((d, nk), BF), pltpu.VMEM((d, nk), BF),
                        pltpu.SemaphoreType.DMA((n,)), pltpu.SemaphoreType.DMA((nq // cut + 2,))],
        compiler_params=pltpu.CompilerParams(vmem_limit_bytes=60 * 2**20),
        cost_estimate=_price(2 * rows * d * (nq + 2 * nk), [*pieces, wq, wk, wv]), name="qkv",
    )(*pieces, wq, wk, wv)


def by_rows_of(pieces, w, bn):
    n, (cols, d) = len(pieces), w.shape
    rows = _rows(pieces)
    steps, rest = -(-cols // bn), cols % bn
    small = -(-rest // 256) * 256

    def kernel(*refs):
        xs, w_ref, o_ref, x_s, sems = refs[:n], refs[n], refs[n + 1], refs[n + 2], refs[n + 3]
        i = pl.program_id(0)

        @pl.when(i == 0)
        def _():
            for c in _load(xs, x_s, sems):
                c.wait()

        if rest == 0 or small == bn:
            o_ref[...] = _dot(x_s[...], w_ref[...], 1, 1).astype(BF)
            return

        @pl.when(i < steps - 1)
        def _():
            o_ref[...] = _dot(x_s[...], w_ref[...], 1, 1).astype(BF)

        @pl.when(i == steps - 1)
        def _():
            o_ref[:, :small] = _dot(x_s[...], w_ref[:small, :], 1, 1).astype(BF)

    return pl.pallas_call(
        kernel, grid=(steps,), in_specs=[ANY] * n + [pl.BlockSpec((bn, d), lambda i: (i, 0))],
        out_specs=pl.BlockSpec((rows, bn), lambda i: (0, i)), out_shape=jax.ShapeDtypeStruct((rows, cols), BF),
        scratch_shapes=[pltpu.VMEM((rows, d), BF), pltpu.SemaphoreType.DMA((n,))], compiler_params=_params(60),
        cost_estimate=_price(2 * rows * d * cols, [*pieces, w]),
    )(*pieces, w)


def mlp(pieces, dhid, wg, wu, bn=256):
    n, (d, cols) = len(pieces), wg.shape
    rows = _rows(pieces)

    def kernel(*refs):
        xs, (dhid_ref, g_ref, u_ref), (hid_ref, dg_ref, du_ref), (x_s, sems) = refs[:n], refs[n : n + 3], refs[n + 3 : n + 6], refs[n + 6 :]

        @pl.when(pl.program_id(0) == 0)
        def _():
            for c in _load(xs, x_s, sems):
                c.wait()

        gate, up = _dot(x_s[...], g_ref[...], 1, 0), _dot(x_s[...], u_ref[...], 1, 0)
        dhid = dhid_ref[...].astype(F32)
        sig = jax.nn.sigmoid(gate)
        silu = gate * sig
        hid_ref[...] = (silu * up).astype(BF)
        du_ref[...] = (dhid * silu).astype(BF)
        dg_ref[...] = (dhid * up * (sig + silu * (1 - sig))).astype(BF)

    w, o = pl.BlockSpec((d, bn), lambda i: (0, i)), pl.BlockSpec((rows, bn), lambda i: (0, i))
    return pl.pallas_call(
        kernel, grid=(-(-cols // bn),), in_specs=[ANY] * n + [o, w, w], out_specs=[o, o, o],
        out_shape=[jax.ShapeDtypeStruct((rows, cols), BF)] * 3,
        scratch_shapes=[pltpu.VMEM((rows, d), BF), pltpu.SemaphoreType.DMA((n,))], compiler_params=_params(60),
        cost_estimate=_price(4 * rows * d * cols, [*pieces, wg, wu, dhid, dhid, dhid]), name="mlp",
    )(*pieces, dhid, wg, wu)


def back(xs, ws, bn):
    n, d = len(xs), ws[0].shape[0]
    rows = xs[0][0].shape[0] if isinstance(xs[0], tuple) else xs[0].shape[0]

    def kernel(*refs):
        x, w, (a_ref, b_ref) = refs[:n], refs[n : 2 * n], refs[2 * n :]
        total = _dot(x[0][...], w[0][...], 1, 1)
        for i in range(1, n):
            total += _dot(x[i][...], w[i][...], 1, 1)
        total = total.astype(BF)
        a_ref[...], b_ref[...] = total[:BLOCK], total[BLOCK:]

    o = pl.BlockSpec((BLOCK, bn), lambda i: (0, i))
    return pl.pallas_call(
        kernel, grid=(d // bn,),
        in_specs=[pl.BlockSpec(x.shape, lambda i: (0, 0)) for x in xs] + [pl.BlockSpec((bn, w.shape[1]), lambda i: (i, 0)) for w in ws],
        out_specs=[o, o], out_shape=[jax.ShapeDtypeStruct((BLOCK, d), BF)] * 2, compiler_params=_params(60),
        cost_estimate=_price(sum(2 * rows * d * w.shape[1] for w in ws), [*xs, *ws]),
    )(*xs, *ws)


def weight_grads(lefts, rights, bm):
    n, m, rows = len(lefts), lefts[0].shape[1], _rows(lefts)
    counts = [len(r) for r in rights]
    widths = [r[0].shape[1] for r in rights]

    def kernel(*refs):
        ls, refs = refs[:n], refs[n:]
        rs = []
        for c in counts:
            rs.append(refs[:c])
            refs = refs[c:]
        outs, wholes, sems = refs[: len(rights)], refs[len(rights) : 2 * len(rights)], refs[2 * len(rights) :]

        @pl.when(pl.program_id(0) == 0)
        def _():
            for c in [c for r, w, s in zip(rs, wholes, sems) for c in _load(r, w, s)]:
                c.wait()

        left = jnp.concatenate([l[...] for l in ls], axis=0).T
        for o, w in zip(outs, wholes):
            o[...] = _dot(left, w[...], 1, 0).astype(BF)

    return pl.pallas_call(
        kernel, grid=(m // bm,),
        in_specs=[pl.BlockSpec((l.shape[0], bm), lambda i: (0, i)) for l in lefts] + [ANY] * sum(counts),
        out_specs=[pl.BlockSpec((bm, w), lambda i: (i, 0)) for w in widths],
        out_shape=[jax.ShapeDtypeStruct((m, w), BF) for w in widths],
        scratch_shapes=[pltpu.VMEM((rows, w), BF) for w in widths] + [pltpu.SemaphoreType.DMA((c,)) for c in counts],
        compiler_params=_params(60), cost_estimate=_price(2 * rows * m * sum(widths), [*lefts, *(p for r in rights for p in r)]),
    )(*lefts, *(p for r in rights for p in r))


CORE = [(0, 1), (1, 0), (2, 3), (3, 2)]
CROSS = [(0, 2), (2, 0), (1, 3), (3, 1)]


def core(v):
    return lax.ppermute(v, "tp", CORE)


def cross(v):
    return lax.ppermute(v, "tp", CROSS)


def after(v, *others):
    return lax.optimization_barrier((v, *others))[0]


def later(pieces, *others):
    return [after(pieces[0], *others), *pieces[1:]]


def gather(v):
    return [v, core(v)], cross(v)


def far_of(first, *others):
    first = after(first, *others)
    return [first, core(first)]


def scatter_far(mine, other):
    both = (mine.astype(F32) + core(other).astype(F32)).astype(BF)
    return both, cross(both)


def scatter_near(mine, other, far):
    return mine.astype(F32) + core(other).astype(F32) + far.astype(F32)


def mm(a, b, ca, cb):
    return _dot(a, b, ca, cb).astype(BF)


def norm(h):
    wide = h.astype(F32)
    scale = lax.rsqrt(jnp.mean(wide**2, -1, keepdims=True) + 1e-6)
    return (wide * scale).astype(BF), scale


def norm_bwd(h, scale, g):
    wide = h.astype(F32)
    g = g.astype(BF).astype(F32)
    return scale * g - wide * (scale**3 * jnp.mean(g * wide, -1, keepdims=True))


def layer(x, dy, wq, wk, wv, wo, wg, wu, wd):
    x, dy = x[0], dy[0]
    me = lax.axis_index("tp").astype(jnp.int32).reshape(1)
    tokens = 4 * x.shape[0]
    half = HEAD // 2
    angle = jnp.arange(tokens, dtype=F32)[:, None] * THETA ** (-jnp.arange(half, dtype=F32) / half)
    cos, sin = jnp.cos(angle), jnp.sin(angle)
    cos, sin = jnp.concatenate([cos, cos], 1), jnp.concatenate([-sin, sin], 1)
    cut = tokens // 2

    a, a_scale = norm(x)
    a_near, a_far = gather(a)
    dy_near = [dy, core(dy)]
    near_qkv = qkv(a_near, wq, wk, wv)
    dhid_near = by_rows_of(later(dy_near, near_qkv[0]), wd, 512)
    a_far = far_of(a_far, dhid_near)
    dy_far = cross(after(dy, a_far[0]))
    far_qkv = qkv(a_far, wq, wk, wv)
    q, k, v = (jnp.concatenate(t) for t in zip(near_qkv, far_qkv))
    heads, lse, q, k = attend(me, q, k, v, cos, sin)
    cuts = [heads[at : at + BLOCK] for at in range(0, tokens, BLOCK)]
    other = mm(cuts[3], wo, 1, 0)
    mine = mm(after(cuts[2], other), wo, 1, 0)
    near_other = mm(after(cuts[1], mine), wo, 1, 0)
    near_mine = mm(after(cuts[0], near_other), wo, 1, 0)
    both, far = scatter_far(mine, other)
    dy_far = far_of(dy_far, both, near_mine)
    dhid_far = by_rows_of(dy_far, wd, 512)
    h = (x.astype(F32) + scatter_near(near_mine, near_other, after(far, dhid_far))).astype(BF)
    b, b_scale = norm(h)
    b_near, b_far = gather(b)
    hid_near, dgate_near, dup_near = mlp(b_near, dhid_near, wg, wu)
    b_far = far_of(b_far, hid_near)
    hid_far, dgate_far, dup_far = mlp(b_far, dhid_far, wg, wu)
    both, far = scatter_far(*back([dgate_far, dup_far], [wg, wu], 512))
    near = back(later([dgate_near, dup_near], both), [wg, wu], 512)
    (d_wd,) = weight_grads(later([hid_near, hid_far], near[0]), [[*dy_near, *dy_far]], 640)
    db = scatter_near(*near, after(far, d_wd))
    dh = (dy.astype(F32) + norm_bwd(h, b_scale, db)).astype(BF)
    dh_near, dh_far = gather(dh)
    dheads_near = by_rows_of(dh_near, wo, 512)
    (d_wg,) = weight_grads(later([*b_near, *b_far], dheads_near), [[dgate_near, dgate_far]], 512)
    dh_far = far_of(dh_far, d_wg)
    dheads_far = by_rows_of(dh_far, wo, 512)
    dq, dk, dv = attend_bwd(me, q, k, v, jnp.concatenate([dheads_near, dheads_far]), heads, lse, cos, sin)
    both, far = scatter_far(*back([t[cut:] for t in (dq, dk, dv)], [wq, wk, wv], 512))
    near = back(later([t[:cut] for t in (dq, dk, dv)], both), [wq, wk, wv], 512)
    d_wq, d_wk, d_wv = weight_grads(later([*a_near, *a_far], near[0]), [[dq], [dk], [dv]], 512)
    (d_wo,) = weight_grads(later([heads], d_wq), [[*dh_near, *dh_far]], 512)
    (d_wu,) = weight_grads(later([*b_near, *b_far], d_wo), [[dup_near, dup_far]], 512)
    da = scatter_near(*near, after(far, d_wu))
    dx = (dh.astype(F32) + norm_bwd(x, a_scale, da)).astype(BF)
    return (dx[None], d_wq, d_wk, d_wv, d_wo, d_wg, d_wu, d_wd)


def solution(mesh):
    states, by_columns, by_rows = P("dp", "tp", None), P(None, "tp"), P("tp", None)
    weights = (by_columns, by_columns, by_columns, by_rows, by_columns, by_columns, by_rows)
    own = tuple(P("dp", "tp") if spec == by_columns else P(("dp", "tp"), None) for spec in weights)
    return jax.shard_map(layer, mesh=mesh, in_specs=(states, states, *weights), out_specs=(states, *own), check_vma=False)
```

```python
import jax
import jax.numpy as jnp
from jax import lax
from jax.experimental import pallas as pl
from jax.experimental.pallas import tpu as pltpu
from jax.sharding import PartitionSpec as P


HEAD = 128
THETA = 10000
LOG2E = 1.4426950408889634
NEG = -1e30
HIDDEN = 2 * NEG
SCALE = HEAD**-0.5
BF, F32 = jnp.bfloat16, jnp.float32
BLOCK = 256
STRIP = 512


def _dot(a, b, ca, cb):
    return lax.dot_general(a, b, (((ca,), (cb,)), ((), ())), preferred_element_type=F32)


def _rope(x, cos, sin):
    x = x.astype(F32)
    return x * cos + pltpu.roll(x, HEAD // 2, 1) * sin


def _unrope(x, cos, sin):
    return x * cos - pltpu.roll(x, HEAD // 2, 1) * sin


def _hidden(cols):
    key = lax.broadcasted_iota(jnp.int32, (BLOCK, cols), 0)
    return key > lax.rem(lax.broadcasted_iota(jnp.int32, (BLOCK, cols), 1), BLOCK)


def _attend(me_ref, qn_ref, qf_ref, kn_ref, kf_ref, vn_ref, vf_ref, cos_ref, sin_ref, o_ref, lse_ref, qr_ref, kr_ref, vt_s, q_s, top_s, mix_s):
    iq = pl.program_id(1)
    me = me_ref[0]
    n = kr_ref.shape[0] // BLOCK
    g = qr_ref.shape[1] // HEAD
    cols = g * BLOCK
    e = SCALE * LOG2E

    @pl.when(iq == 0)
    def _():
        for s in range(n):
            here = pl.ds((s ^ me) * BLOCK, BLOCK)
            rows, half = slice(s * BLOCK, (s + 1) * BLOCK), slice(s % 2 * BLOCK, (s % 2 + 1) * BLOCK)
            k, v = (kn_ref, vn_ref) if s < 2 else (kf_ref, vf_ref)
            kr_ref[rows, :] = _rope(k[half, :], cos_ref[here, :], sin_ref[here, :]).astype(BF)
            vt_s[s, :HEAD, :] = v[half, :].T
            vt_s[s, HEAD:, :] = jnp.ones((8, BLOCK), BF)

    here = pl.ds(iq * BLOCK, BLOCK)
    cos, sin = cos_ref[here, :], sin_ref[here, :]
    near = (iq ^ me) < 2

    def turn(q_ref):
        for h in range(g):
            turned = _rope(q_ref[:, h * HEAD : (h + 1) * HEAD], cos, sin).astype(BF)
            qr_ref[:, h * HEAD : (h + 1) * HEAD] = turned
            q_s[h * BLOCK : (h + 1) * BLOCK, :] = turned

    pl.when(near)(lambda: turn(qn_ref))
    pl.when(jnp.logical_not(near))(lambda: turn(qf_ref))
    top_s[...] = jnp.full((1, cols), NEG, F32)
    mix_s[...] = jnp.zeros((HEAD + 8, cols), F32)

    def block(j, masked):
        slot = j ^ me
        keys = kr_ref[pl.ds(slot * BLOCK, BLOCK), :]
        strips = range(0, cols, STRIP)
        scores = [_dot(keys, q_s[at : at + STRIP, :], 1, 1) for at in strips]
        weights, keeps = [], []
        for at, s in zip(strips, scores):
            if masked:
                s = jnp.where(_hidden(STRIP), HIDDEN, s)
            old = top_s[:, at : at + STRIP]
            top = jnp.maximum(old, s.max(axis=0, keepdims=True))
            top_s[:, at : at + STRIP] = top
            weights.append(jnp.exp2((s - top) * e).astype(BF))
            keeps.append(jnp.exp2((old - top) * e))
        for at, p, keep in zip(strips, weights, keeps):
            mix_s[:, at : at + STRIP] = mix_s[:, at : at + STRIP] * keep + _dot(vt_s[slot], p, 1, 0)

    lax.fori_loop(0, iq, lambda j, _: block(j, False), None)
    block(iq, True)
    total = mix_s[HEAD : HEAD + 1, :]
    out = (mix_s[:HEAD, :] * (1 / total)).T.astype(BF)
    for h in range(g):
        o_ref[:, h * HEAD : (h + 1) * HEAD] = out[h * BLOCK : (h + 1) * BLOCK, :]
    lse_ref[0] = top_s[...] * e + jnp.log2(total)


def _attend_bwd(me_ref, q_ref, k_ref, vn_ref, vf_ref, don_ref, dof_ref, o_ref, lse_ref, cos_ref, sin_ref, dq_ref, dk_ref, dv_ref,
                q_s, do_s, dq_s, dk_s, dv_s, kt_s, v_s, delta_s):
    iq = pl.program_id(1)
    me = me_ref[0]
    n = k_ref.shape[0] // BLOCK
    g = q_ref.shape[1] // HEAD
    cols = g * BLOCK
    e = SCALE * LOG2E

    @pl.when(iq == 0)
    def _():
        dk_s[...] = jnp.zeros_like(dk_s)
        dv_s[...] = jnp.zeros_like(dv_s)
        v_s[: 2 * BLOCK, :], v_s[2 * BLOCK :, :] = vn_ref[...], vf_ref[...]
        for s in range(n):
            kt_s[s] = k_ref[s * BLOCK : (s + 1) * BLOCK, :].T

    dq_s[...] = jnp.zeros_like(dq_s)
    near = (iq ^ me) < 2

    def take(do_ref):
        for h in range(g):
            lanes, rows = slice(h * HEAD, (h + 1) * HEAD), slice(h * BLOCK, (h + 1) * BLOCK)
            q_s[rows, :] = q_ref[:, lanes]
            do_s[rows, :] = do_ref[:, lanes]
            prod = do_ref[:, lanes].astype(F32) * o_ref[:, lanes].astype(F32)
            delta_s[:, rows] = prod.T.sum(axis=0, keepdims=True)

    pl.when(near)(lambda: take(don_ref))
    pl.when(jnp.logical_not(near))(lambda: take(dof_ref))

    def block(j, masked):
        slot = j ^ me
        here = pl.ds(slot * BLOCK, BLOCK)
        keys, values = k_ref[here, :], v_s[here, :]
        strips = range(0, cols, STRIP)
        scores = [_dot(keys, q_s[at : at + STRIP, :], 1, 1) for at in strips]
        dps = [_dot(values, do_s[at : at + STRIP, :], 1, 1) for at in strips]
        for at, s, dp in zip(strips, scores, dps):
            p = jnp.exp2(s * e - lse_ref[0, :, at : at + STRIP])
            if masked:
                p = jnp.where(_hidden(STRIP), 0.0, p)
            ds = (p * (dp - delta_s[:, at : at + STRIP])).astype(BF)
            dv_s[here, :] += _dot(p.astype(BF), do_s[at : at + STRIP, :], 1, 0)
            dk_s[here, :] += _dot(ds, q_s[at : at + STRIP, :], 1, 0)
            dq_s[:, at : at + STRIP] += _dot(kt_s[slot], ds, 1, 0)

    lax.fori_loop(0, iq, lambda j, _: block(j, False), None)
    block(iq, True)
    here = pl.ds(iq * BLOCK, BLOCK)
    cos, sin = cos_ref[here, :], sin_ref[here, :]
    dq = (dq_s[...] * SCALE).T
    for h in range(g):
        dq_ref[:, h * HEAD : (h + 1) * HEAD] = _unrope(dq[h * BLOCK : (h + 1) * BLOCK, :], cos, sin).astype(BF)

    @pl.when(iq == n - 1)
    def _():
        for s in range(n):
            here = pl.ds((s ^ me) * BLOCK, BLOCK)
            rows = slice(s * BLOCK, (s + 1) * BLOCK)
            dk_ref[rows, :] = _unrope(dk_s[rows, :] * SCALE, cos_ref[here, :], sin_ref[here, :]).astype(BF)
            dv_ref[rows, :] = dv_s[rows, :].astype(BF)


def _attn_specs(tokens, g):
    queries = pl.BlockSpec((BLOCK, g * HEAD), lambda h, i, me: (i ^ me[0], h))
    near = pl.BlockSpec((BLOCK, g * HEAD), lambda h, i, me: (jnp.minimum(i ^ me[0], 1), h))
    far = pl.BlockSpec((BLOCK, g * HEAD), lambda h, i, me: (jnp.maximum((i ^ me[0]) - 2, 0), h))
    keys = pl.BlockSpec((tokens, HEAD), lambda h, i, me: (0, h))
    half = pl.BlockSpec((tokens // 2, HEAD), lambda h, i, me: (0, h))
    table = pl.BlockSpec((tokens, HEAD), lambda h, i, me: (0, 0))
    stats = pl.BlockSpec((1, 1, g * BLOCK), lambda h, i, me: (h * (tokens // BLOCK) + i, 0, 0))
    return queries, near, far, keys, half, table, stats


def attend(me, qs, ks, vs, cos, sin):
    tokens, width, kv = 2 * ks[0].shape[0], qs[0].shape[1], ks[0].shape[1] // HEAD
    g = width // ks[0].shape[1]
    queries, near, far, keys, half, table, stats = _attn_specs(tokens, g)
    n = tokens // BLOCK
    return pl.pallas_call(
        _attend,
        grid_spec=pltpu.PrefetchScalarGridSpec(
            num_scalar_prefetch=1, grid=(kv, n), in_specs=[near, far, half, half, half, half, table, table],
            out_specs=[queries, stats, queries, keys],
            scratch_shapes=[pltpu.VMEM((n, HEAD + 8, BLOCK), BF), pltpu.VMEM((g * BLOCK, HEAD), BF), pltpu.VMEM((1, g * BLOCK), F32),
                            pltpu.VMEM((HEAD + 8, g * BLOCK), F32)]),
        out_shape=[jax.ShapeDtypeStruct((tokens, width), BF), jax.ShapeDtypeStruct((kv * n, 1, g * BLOCK), F32),
                   jax.ShapeDtypeStruct((tokens, width), BF), jax.ShapeDtypeStruct((tokens, kv * HEAD), BF)],
        compiler_params=pltpu.CompilerParams(dimension_semantics=("arbitrary", "arbitrary"), vmem_limit_bytes=24 * 2**20),
        cost_estimate=pl.CostEstimate(flops=12 * 10**9, transcendentals=0, bytes_accessed=8 * 2**20),
        name="attend",
    )(me, *qs, *ks, *vs, cos, sin)


def attend_bwd(me, q, k, vs, dos, o, lse, cos, sin):
    tokens, kv = k.shape[0], k.shape[1] // HEAD
    g = q.shape[1] // k.shape[1]
    queries, near, far, keys, half, table, stats = _attn_specs(tokens, g)
    n = tokens // BLOCK
    return pl.pallas_call(
        _attend_bwd,
        grid_spec=pltpu.PrefetchScalarGridSpec(
            num_scalar_prefetch=1, grid=(kv, n), in_specs=[queries, keys, half, half, near, far, queries, stats, table, table],
            out_specs=[queries, keys, keys],
            scratch_shapes=[pltpu.VMEM((g * BLOCK, HEAD), BF), pltpu.VMEM((g * BLOCK, HEAD), BF), pltpu.VMEM((HEAD, g * BLOCK), F32),
                            pltpu.VMEM((tokens, HEAD), F32), pltpu.VMEM((tokens, HEAD), F32), pltpu.VMEM((n, HEAD, BLOCK), BF),
                            pltpu.VMEM((tokens, HEAD), BF), pltpu.VMEM((1, g * BLOCK), F32)]),
        out_shape=[jax.ShapeDtypeStruct(q.shape, BF), jax.ShapeDtypeStruct(k.shape, BF), jax.ShapeDtypeStruct(k.shape, BF)],
        compiler_params=pltpu.CompilerParams(dimension_semantics=("arbitrary", "arbitrary"), vmem_limit_bytes=24 * 2**20),
        cost_estimate=pl.CostEstimate(flops=18 * 10**9, transcendentals=0, bytes_accessed=12 * 2**20),
        name="attend_bwd",
    )(me, q, k, *vs, *dos, o, lse, cos, sin)


ANY = pl.BlockSpec(memory_space=pltpu.HBM)


def _load(pieces, whole, sems):
    copies, at = [], 0
    for i, piece in enumerate(pieces):
        n = piece.shape[0]
        copies.append(pltpu.make_async_copy(piece, whole.at[pl.ds(at, n), :], sems.at[i]))
        at += n
    for c in copies:
        c.start()
    return copies


def _params(mib, steps=1):
    return pltpu.CompilerParams(dimension_semantics=("arbitrary",) * steps, vmem_limit_bytes=mib * 2**20)


def _price(flops, arrays):
    return pl.CostEstimate(flops=flops, transcendentals=0, bytes_accessed=sum(a.size * 2 for a in arrays))


def _rows(pieces):
    return sum(p.shape[0] for p in pieces)


def qkv(pieces, wq, wk, wv):
    n, (d, nq), nk = len(pieces), wq.shape, wk.shape[1]
    rows, cut = _rows(pieces), 512

    def kernel(*refs):
        xs, (wq_ref, wk_ref, wv_ref), (q_ref, k_ref, v_ref) = refs[:n], refs[n : n + 3], refs[n + 3 : n + 6]
        x_s, q_s, k_s, v_s, sems, wsems = refs[n + 6 :]
        copies = _load(xs, x_s, sems)
        todo = []
        for i, at in enumerate(range(0, nq, cut)):
            here = slice(at, at + cut)
            todo.append((pltpu.make_async_copy(wq_ref.at[:, here], q_s.at[:, here], wsems.at[i]), q_s.at[:, here], q_ref, here))
        for i, (w, w_s, o) in enumerate(((wk_ref, k_s, k_ref), (wv_ref, v_s, v_ref))):
            todo.append((pltpu.make_async_copy(w, w_s, wsems.at[nq // cut + i]), w_s, o, slice(0, nk)))
        todo[0][0].start()
        for c in copies:
            c.wait()
        for i, (c, w_s, o, here) in enumerate(todo):
            c.wait()
            if i + 1 < len(todo):
                todo[i + 1][0].start()
            o[:, here] = _dot(x_s[...], w_s[...], 1, 0).astype(BF)

    return pl.pallas_call(
        kernel, in_specs=[ANY] * (n + 3), out_specs=[pl.BlockSpec(memory_space=pltpu.VMEM)] * 3,
        out_shape=[jax.ShapeDtypeStruct((rows, m), BF) for m in (nq, nk, nk)],
        scratch_shapes=[pltpu.VMEM((rows, d), BF), pltpu.VMEM((d, nq), BF), pltpu.VMEM((d, nk), BF), pltpu.VMEM((d, nk), BF),
                        pltpu.SemaphoreType.DMA((n,)), pltpu.SemaphoreType.DMA((nq // cut + 2,))],
        compiler_params=pltpu.CompilerParams(vmem_limit_bytes=57 * 2**20),
        cost_estimate=_price(2 * rows * d * (nq + 2 * nk), [*pieces, wq, wk, wv]), name="qkv",
    )(*pieces, wq, wk, wv)


def by_rows_of(pieces, w, bn, mib=40):
    n, (cols, d) = len(pieces), w.shape
    rows = _rows(pieces)
    steps, rest = -(-cols // bn), cols % bn
    small = -(-rest // 256) * 256

    def kernel(*refs):
        xs, w_ref, o_ref, x_s, sems = refs[:n], refs[n], refs[n + 1], refs[n + 2], refs[n + 3]
        i = pl.program_id(0)

        @pl.when(i == 0)
        def _():
            for c in _load(xs, x_s, sems):
                c.wait()

        if rest == 0 or small == bn:
            o_ref[...] = _dot(x_s[...], w_ref[...], 1, 1).astype(BF)
            return

        @pl.when(i < steps - 1)
        def _():
            o_ref[...] = _dot(x_s[...], w_ref[...], 1, 1).astype(BF)

        @pl.when(i == steps - 1)
        def _():
            o_ref[:, :small] = _dot(x_s[...], w_ref[:small, :], 1, 1).astype(BF)

    return pl.pallas_call(
        kernel, grid=(steps,), in_specs=[ANY] * n + [pl.BlockSpec((bn, d), lambda i: (i, 0))],
        out_specs=pl.BlockSpec((rows, bn), lambda i: (0, i)), out_shape=jax.ShapeDtypeStruct((rows, cols), BF),
        scratch_shapes=[pltpu.VMEM((rows, d), BF), pltpu.SemaphoreType.DMA((n,))], compiler_params=_params(mib),
        cost_estimate=_price(2 * rows * d * cols, [*pieces, w]),
    )(*pieces, w)


def mlp(pieces, dhid, wg, wu, bn=256):
    n, (d, cols) = len(pieces), wg.shape
    rows = _rows(pieces)

    def kernel(*refs):
        xs, (dhid_ref, g_ref, u_ref), (hid_ref, dg_ref, du_ref), (x_s, sems) = refs[:n], refs[n : n + 3], refs[n + 3 : n + 6], refs[n + 6 :]

        @pl.when(pl.program_id(0) == 0)
        def _():
            for c in _load(xs, x_s, sems):
                c.wait()

        gate, up = _dot(x_s[...], g_ref[...], 1, 0), _dot(x_s[...], u_ref[...], 1, 0)
        dhid = dhid_ref[...].astype(F32)
        sig = jax.nn.sigmoid(gate)
        silu = gate * sig
        hid_ref[...] = (silu * up).astype(BF)
        du_ref[...] = (dhid * silu).astype(BF)
        dg_ref[...] = (dhid * up * (sig + silu * (1 - sig))).astype(BF)

    w, o = pl.BlockSpec((d, bn), lambda i: (0, i)), pl.BlockSpec((rows, bn), lambda i: (0, i))
    return pl.pallas_call(
        kernel, grid=(-(-cols // bn),), in_specs=[ANY] * n + [o, w, w], out_specs=[o, o, o],
        out_shape=[jax.ShapeDtypeStruct((rows, cols), BF)] * 3,
        scratch_shapes=[pltpu.VMEM((rows, d), BF), pltpu.SemaphoreType.DMA((n,))], compiler_params=_params(56),
        cost_estimate=_price(4 * rows * d * cols, [*pieces, wg, wu, dhid, dhid, dhid]), name="mlp",
    )(*pieces, dhid, wg, wu)


def back(xs, ws, bn, half=0):
    n, d = len(xs), ws[0].shape[0]
    rows = 2 * BLOCK

    def kernel(*refs):
        x, w, (a_ref, b_ref) = refs[:n], refs[n : 2 * n], refs[2 * n :]
        total = _dot(x[0][...], w[0][...], 1, 1)
        for i in range(1, n):
            total += _dot(x[i][...], w[i][...], 1, 1)
        total = total.astype(BF)
        a_ref[...], b_ref[...] = total[:BLOCK], total[BLOCK:]

    o = pl.BlockSpec((BLOCK, bn), lambda i: (0, i))
    return pl.pallas_call(
        kernel, grid=(d // bn,),
        in_specs=[pl.BlockSpec((rows, x.shape[1]), lambda i: (half, 0)) for x in xs] + [pl.BlockSpec((bn, w.shape[1]), lambda i: (i, 0)) for w in ws],
        out_specs=[o, o], out_shape=[jax.ShapeDtypeStruct((BLOCK, d), BF)] * 2, compiler_params=_params(48),
        cost_estimate=_price(sum(2 * rows * d * w.shape[1] for w in ws), [*xs, *ws]),
    )(*xs, *ws)


def weight_grads(lefts, rights, bm, mib=48):
    n, m, rows = len(lefts), lefts[0].shape[1], _rows(lefts)
    counts = [len(r) for r in rights]
    widths = [r[0].shape[1] for r in rights]

    def kernel(*refs):
        ls, refs = refs[:n], refs[n:]
        rs = []
        for c in counts:
            rs.append(refs[:c])
            refs = refs[c:]
        outs, wholes, sems = refs[: len(rights)], refs[len(rights) : 2 * len(rights)], refs[2 * len(rights) :]

        @pl.when(pl.program_id(0) == 0)
        def _():
            for c in [c for r, w, s in zip(rs, wholes, sems) for c in _load(r, w, s)]:
                c.wait()

        left = jnp.concatenate([l[...] for l in ls], axis=0).T
        for o, w in zip(outs, wholes):
            o[...] = _dot(left, w[...], 1, 0).astype(BF)

    return pl.pallas_call(
        kernel, grid=(m // bm,),
        in_specs=[pl.BlockSpec((l.shape[0], bm), lambda i: (0, i)) for l in lefts] + [ANY] * sum(counts),
        out_specs=[pl.BlockSpec((bm, w), lambda i: (i, 0)) for w in widths],
        out_shape=[jax.ShapeDtypeStruct((m, w), BF) for w in widths],
        scratch_shapes=[pltpu.VMEM((rows, w), BF) for w in widths] + [pltpu.SemaphoreType.DMA((c,)) for c in counts],
        compiler_params=_params(mib), cost_estimate=_price(2 * rows * m * sum(widths), [*lefts, *(p for r in rights for p in r)]),
    )(*lefts, *(p for r in rights for p in r))


CORE = [(0, 1), (1, 0), (2, 3), (3, 2)]
CROSS = [(0, 2), (2, 0), (1, 3), (3, 1)]


def core(v):
    return lax.ppermute(v, "tp", CORE)


def cross(v):
    return lax.ppermute(v, "tp", CROSS)


def after(v, *others):
    return lax.optimization_barrier((v, *others))[0]


def later(pieces, *others):
    return [after(pieces[0], *others), *pieces[1:]]


def gather(v):
    return [v, core(v)], cross(v)


def far_of(first, *others):
    first = after(first, *others)
    return [first, core(first)]


def scatter_far(mine, other):
    both = (mine.astype(F32) + core(other).astype(F32)).astype(BF)
    return both, cross(both)


def mm(a, b, ca, cb):
    return _dot(a, b, ca, cb).astype(BF)


def _scale(wide):
    return lax.rsqrt(jnp.mean(wide**2, -1, keepdims=True) + 1e-6)


def by_row(f, arrays, outs):
    rows, d = arrays[0].shape

    def kernel(*refs):
        got = f(*(r[...].astype(F32) for r in refs[: len(arrays)]))
        for ref, t in zip(refs[len(arrays) :], got, strict=True):
            ref[...] = t.astype(BF)

    spec = pl.BlockSpec((32, d), lambda i: (i, 0))
    return pl.pallas_call(
        kernel, grid=(rows // 32,), in_specs=[spec] * len(arrays), out_specs=[spec] * outs,
        out_shape=[jax.ShapeDtypeStruct((rows, d), BF)] * outs, compiler_params=_params(24),
        cost_estimate=_price(10 * rows * d, [*arrays, *arrays[:outs]]),
    )(*arrays)


def norm(h):
    return by_row(lambda wide: (wide * _scale(wide),), [h], 1)[0]


def add_norm(h, mine, other, far):
    def f(h, *terms):
        wide = (h + sum(terms)).astype(BF).astype(F32)
        return wide, wide * _scale(wide)

    return by_row(f, [h, mine, core(other), far], 2)


def norm_bwd(direct, h, mine, other, far):
    def f(direct, h, *terms):
        g, scale = sum(terms).astype(BF).astype(F32), _scale(h)
        return (direct + scale * g - h * (scale**3 * jnp.mean(g * h, -1, keepdims=True)),)

    return by_row(f, [direct, h, mine, core(other), far], 1)[0]


def layer(x, dy, wq, wk, wv, wo, wg, wu, wd):
    x, dy = x[0], dy[0]
    me = lax.axis_index("tp").astype(jnp.int32).reshape(1)
    tokens = 4 * x.shape[0]
    half = HEAD // 2
    angle = jnp.arange(tokens, dtype=F32)[:, None] * THETA ** (-jnp.arange(half, dtype=F32) / half)
    cos, sin = jnp.cos(angle), jnp.sin(angle)
    cos, sin = jnp.concatenate([cos, cos], 1), jnp.concatenate([-sin, sin], 1)

    a = norm(x)
    a_near, a_far = gather(a)
    dy_near = [dy, core(dy)]
    near_qkv = qkv(a_near, wq, wk, wv)
    dhid_near = by_rows_of(later(dy_near, near_qkv[0]), wd, 512)
    a_far = far_of(a_far, dhid_near)
    dy_far = cross(after(dy, a_far[0]))
    far_qkv = qkv(a_far, wq, wk, wv)
    qs, ks, vs = zip(near_qkv, far_qkv)
    heads, lse, q, k = attend(me, qs, ks, vs, cos, sin)
    cuts = [heads[at : at + BLOCK] for at in range(0, tokens, BLOCK)]
    other = mm(cuts[3], wo, 1, 0)
    mine = mm(after(cuts[2], other), wo, 1, 0)
    near_other = mm(after(cuts[1], mine), wo, 1, 0)
    near_mine = mm(after(cuts[0], near_other), wo, 1, 0)
    both, far = scatter_far(after(mine, near_other), other)
    dy_far = far_of(dy_far, both, near_mine)
    dhid_far = by_rows_of(dy_far, wd, 512)
    h, b = add_norm(x, near_mine, near_other, after(far, dhid_far))
    b_near, b_far = gather(b)
    hid_near, dgate_near, dup_near = mlp(b_near, dhid_near, wg, wu)
    b_far = far_of(b_far, hid_near)
    hid_far, dgate_far, dup_far = mlp(b_far, dhid_far, wg, wu)
    terms = back([dgate_far, dup_far], [wg, wu], 512)
    near = back(later([dgate_near, dup_near], terms[1]), [wg, wu], 512)
    both, far = scatter_far(after(terms[0], near[0]), terms[1])
    d_wg, d_wu = weight_grads(later([*b_near, *b_far], both), [[dgate_near, dgate_far], [dup_near, dup_far]], 512, 56)
    dh = norm_bwd(dy, h, *near, after(far, d_wg))
    dh_near, dh_far = gather(dh)
    dheads_near = by_rows_of(dh_near, wo, 512)
    (d_wd,) = weight_grads(later([hid_near, hid_far], dheads_near), [[*dy_near, *dy_far]], 640)
    dh_far = far_of(dh_far, d_wd)
    dheads_far = by_rows_of(dh_far, wo, 512, 57)
    dq, dk, dv = attend_bwd(me, q, k, vs, (dheads_near, dheads_far), heads, lse, cos, sin)
    both, far = scatter_far(*back([dq, dk, dv], [wq, wk, wv], 512, 1))
    near = back(later([dq, dk, dv], both), [wq, wk, wv], 512)
    d_wq, d_wk, d_wv = weight_grads(later([*a_near, *a_far], near[0]), [[dq], [dk], [dv]], 512)
    (d_wo,) = weight_grads(later([heads], d_wq), [[*dh_near, *dh_far]], 512)
    dx = norm_bwd(dh, x, *near, after(far, d_wo))
    return (dx[None], d_wq, d_wk, d_wv, d_wo, d_wg, d_wu, d_wd)


def solution(mesh):
    states, by_columns, by_rows = P("dp", "tp", None), P(None, "tp"), P("tp", None)
    weights = (by_columns, by_columns, by_columns, by_rows, by_columns, by_columns, by_rows)
    own = tuple(P("dp", "tp") if spec == by_columns else P(("dp", "tp"), None) for spec in weights)
    return jax.shard_map(layer, mesh=mesh, in_specs=(states, states, *weights), out_specs=(states, *own), check_vma=False)
```

```python
import jax
import jax.numpy as jnp
from jax import lax
from jax.experimental import pallas as pl
from jax.experimental.pallas import tpu as pltpu
from jax.sharding import PartitionSpec as P


HEAD = 128
THETA = 10000
LOG2E = 1.4426950408889634
NEG = -1e30
HIDDEN = 2 * NEG
SCALE = HEAD**-0.5
BF, F32 = jnp.bfloat16, jnp.float32
BLOCK = 256
STRIP = 512


def _dot(a, b, ca, cb):
    return lax.dot_general(a, b, (((ca,), (cb,)), ((), ())), preferred_element_type=F32)


def _rope(x, cos, sin):
    x = x.astype(F32)
    return x * cos + pltpu.roll(x, HEAD // 2, 1) * sin


def _unrope(x, cos, sin):
    return x * cos - pltpu.roll(x, HEAD // 2, 1) * sin


def _hidden(cols):
    key = lax.broadcasted_iota(jnp.int32, (BLOCK, cols), 0)
    return key > lax.rem(lax.broadcasted_iota(jnp.int32, (BLOCK, cols), 1), BLOCK)


def _attend(me_ref, qn_ref, qf_ref, kn_ref, kf_ref, vn_ref, vf_ref, cos_ref, sin_ref, o_ref, lse_ref, qr_ref, kr_ref, vt_s, q_s, top_s, mix_s):
    iq = pl.program_id(1)
    me = me_ref[0]
    n = kr_ref.shape[0] // BLOCK
    g = qr_ref.shape[1] // HEAD
    cols = g * BLOCK
    e = SCALE * LOG2E

    @pl.when(iq == 0)
    def _():
        for s in range(n):
            here = pl.ds((s ^ me) * BLOCK, BLOCK)
            rows, half = slice(s * BLOCK, (s + 1) * BLOCK), slice(s % 2 * BLOCK, (s % 2 + 1) * BLOCK)
            k, v = (kn_ref, vn_ref) if s < 2 else (kf_ref, vf_ref)
            kr_ref[rows, :] = _rope(k[half, :], cos_ref[here, :], sin_ref[here, :]).astype(BF)
            vt_s[s, :HEAD, :] = v[half, :].T
            vt_s[s, HEAD:, :] = jnp.ones((8, BLOCK), BF)

    here = pl.ds(iq * BLOCK, BLOCK)
    cos, sin = cos_ref[here, :], sin_ref[here, :]
    near = (iq ^ me) < 2

    def turn(q_ref):
        for h in range(g):
            turned = _rope(q_ref[:, h * HEAD : (h + 1) * HEAD], cos, sin).astype(BF)
            qr_ref[:, h * HEAD : (h + 1) * HEAD] = turned
            q_s[h * BLOCK : (h + 1) * BLOCK, :] = turned

    pl.when(near)(lambda: turn(qn_ref))
    pl.when(jnp.logical_not(near))(lambda: turn(qf_ref))
    top_s[...] = jnp.full((1, cols), NEG, F32)
    mix_s[...] = jnp.zeros((HEAD + 8, cols), F32)

    def block(j, masked):
        slot = j ^ me
        keys = kr_ref[pl.ds(slot * BLOCK, BLOCK), :]
        strips = range(0, cols, STRIP)
        scores = [_dot(keys, q_s[at : at + STRIP, :], 1, 1) for at in strips]
        weights, keeps = [], []
        for at, s in zip(strips, scores):
            if masked:
                s = jnp.where(_hidden(STRIP), HIDDEN, s)
            old = top_s[:, at : at + STRIP]
            top = jnp.maximum(old, s.max(axis=0, keepdims=True))
            top_s[:, at : at + STRIP] = top
            weights.append(jnp.exp2((s - top) * e).astype(BF))
            keeps.append(jnp.exp2((old - top) * e))
        for at, p, keep in zip(strips, weights, keeps):
            mix_s[:, at : at + STRIP] = mix_s[:, at : at + STRIP] * keep + _dot(vt_s[slot], p, 1, 0)

    lax.fori_loop(0, iq, lambda j, _: block(j, False), None)
    block(iq, True)
    total = mix_s[HEAD : HEAD + 1, :]
    out = (mix_s[:HEAD, :] * (1 / total)).T.astype(BF)
    for h in range(g):
        o_ref[:, h * HEAD : (h + 1) * HEAD] = out[h * BLOCK : (h + 1) * BLOCK, :]
    lse_ref[0] = top_s[...] * e + jnp.log2(total)


def _attend_bwd(me_ref, q_ref, k_ref, vn_ref, vf_ref, don_ref, dof_ref, o_ref, lse_ref, cos_ref, sin_ref, dq_ref, dk_ref, dv_ref,
                q_s, do_s, dq_s, dk_s, dv_s, kt_s, v_s, delta_s):
    iq = pl.program_id(1)
    me = me_ref[0]
    n = k_ref.shape[0] // BLOCK
    g = q_ref.shape[1] // HEAD
    cols = g * BLOCK
    e = SCALE * LOG2E

    @pl.when(iq == 0)
    def _():
        dk_s[...] = jnp.zeros_like(dk_s)
        dv_s[...] = jnp.zeros_like(dv_s)
        v_s[: 2 * BLOCK, :], v_s[2 * BLOCK :, :] = vn_ref[...], vf_ref[...]
        for s in range(n):
            kt_s[s] = k_ref[s * BLOCK : (s + 1) * BLOCK, :].T

    dq_s[...] = jnp.zeros_like(dq_s)
    near = (iq ^ me) < 2

    def take(do_ref):
        for h in range(g):
            lanes, rows = slice(h * HEAD, (h + 1) * HEAD), slice(h * BLOCK, (h + 1) * BLOCK)
            q_s[rows, :] = q_ref[:, lanes]
            do_s[rows, :] = do_ref[:, lanes]
            prod = do_ref[:, lanes].astype(F32) * o_ref[:, lanes].astype(F32)
            delta_s[:, rows] = prod.T.sum(axis=0, keepdims=True)

    pl.when(near)(lambda: take(don_ref))
    pl.when(jnp.logical_not(near))(lambda: take(dof_ref))

    def block(j, masked):
        slot = j ^ me
        here = pl.ds(slot * BLOCK, BLOCK)
        keys, values = k_ref[here, :], v_s[here, :]
        strips = range(0, cols, STRIP)
        scores = [_dot(keys, q_s[at : at + STRIP, :], 1, 1) for at in strips]
        dps = [_dot(values, do_s[at : at + STRIP, :], 1, 1) for at in strips]
        for at, s, dp in zip(strips, scores, dps):
            p = jnp.exp2(s * e - lse_ref[0, :, at : at + STRIP])
            if masked:
                p = jnp.where(_hidden(STRIP), 0.0, p)
            ds = (p * (dp - delta_s[:, at : at + STRIP])).astype(BF)
            dv_s[here, :] += _dot(p.astype(BF), do_s[at : at + STRIP, :], 1, 0)
            dk_s[here, :] += _dot(ds, q_s[at : at + STRIP, :], 1, 0)
            dq_s[:, at : at + STRIP] += _dot(kt_s[slot], ds, 1, 0)

    lax.fori_loop(0, iq, lambda j, _: block(j, False), None)
    block(iq, True)
    here = pl.ds(iq * BLOCK, BLOCK)
    cos, sin = cos_ref[here, :], sin_ref[here, :]
    dq = (dq_s[...] * SCALE).T
    for h in range(g):
        dq_ref[:, h * HEAD : (h + 1) * HEAD] = _unrope(dq[h * BLOCK : (h + 1) * BLOCK, :], cos, sin).astype(BF)

    @pl.when(iq == n - 1)
    def _():
        for s in range(n):
            here = pl.ds((s ^ me) * BLOCK, BLOCK)
            rows = slice(s * BLOCK, (s + 1) * BLOCK)
            dk_ref[rows, :] = _unrope(dk_s[rows, :] * SCALE, cos_ref[here, :], sin_ref[here, :]).astype(BF)
            dv_ref[rows, :] = dv_s[rows, :].astype(BF)


def _attn_specs(tokens, g):
    queries = pl.BlockSpec((BLOCK, g * HEAD), lambda h, i, me: (i ^ me[0], h))
    near = pl.BlockSpec((BLOCK, g * HEAD), lambda h, i, me: (jnp.minimum(i ^ me[0], 1), h))
    far = pl.BlockSpec((BLOCK, g * HEAD), lambda h, i, me: (jnp.maximum((i ^ me[0]) - 2, 0), h))
    keys = pl.BlockSpec((tokens, HEAD), lambda h, i, me: (0, h))
    half = pl.BlockSpec((tokens // 2, HEAD), lambda h, i, me: (0, h))
    table = pl.BlockSpec((tokens, HEAD), lambda h, i, me: (0, 0))
    stats = pl.BlockSpec((1, 1, g * BLOCK), lambda h, i, me: (h * (tokens // BLOCK) + i, 0, 0))
    return queries, near, far, keys, half, table, stats


def attend(me, qs, ks, vs, cos, sin):
    tokens, width, kv = 2 * ks[0].shape[0], qs[0].shape[1], ks[0].shape[1] // HEAD
    g = width // ks[0].shape[1]
    queries, near, far, keys, half, table, stats = _attn_specs(tokens, g)
    n = tokens // BLOCK
    return pl.pallas_call(
        _attend,
        grid_spec=pltpu.PrefetchScalarGridSpec(
            num_scalar_prefetch=1, grid=(kv, n), in_specs=[near, far, half, half, half, half, table, table],
            out_specs=[queries, stats, queries, keys],
            scratch_shapes=[pltpu.VMEM((n, HEAD + 8, BLOCK), BF), pltpu.VMEM((g * BLOCK, HEAD), BF), pltpu.VMEM((1, g * BLOCK), F32),
                            pltpu.VMEM((HEAD + 8, g * BLOCK), F32)]),
        out_shape=[jax.ShapeDtypeStruct((tokens, width), BF), jax.ShapeDtypeStruct((kv * n, 1, g * BLOCK), F32),
                   jax.ShapeDtypeStruct((tokens, width), BF), jax.ShapeDtypeStruct((tokens, kv * HEAD), BF)],
        compiler_params=pltpu.CompilerParams(dimension_semantics=("arbitrary", "arbitrary"), vmem_limit_bytes=60 * 2**20),
        cost_estimate=pl.CostEstimate(flops=12 * 10**9, transcendentals=0, bytes_accessed=8 * 2**20),
        name="attend",
    )(me, *qs, *ks, *vs, cos, sin)


def attend_bwd(me, q, k, vs, dos, o, lse, cos, sin):
    tokens, kv = k.shape[0], k.shape[1] // HEAD
    g = q.shape[1] // k.shape[1]
    queries, near, far, keys, half, table, stats = _attn_specs(tokens, g)
    n = tokens // BLOCK
    return pl.pallas_call(
        _attend_bwd,
        grid_spec=pltpu.PrefetchScalarGridSpec(
            num_scalar_prefetch=1, grid=(kv, n), in_specs=[queries, keys, half, half, near, far, queries, stats, table, table],
            out_specs=[queries, keys, keys],
            scratch_shapes=[pltpu.VMEM((g * BLOCK, HEAD), BF), pltpu.VMEM((g * BLOCK, HEAD), BF), pltpu.VMEM((HEAD, g * BLOCK), F32),
                            pltpu.VMEM((tokens, HEAD), F32), pltpu.VMEM((tokens, HEAD), F32), pltpu.VMEM((n, HEAD, BLOCK), BF),
                            pltpu.VMEM((tokens, HEAD), BF), pltpu.VMEM((1, g * BLOCK), F32)]),
        out_shape=[jax.ShapeDtypeStruct(q.shape, BF), jax.ShapeDtypeStruct(k.shape, BF), jax.ShapeDtypeStruct(k.shape, BF)],
        compiler_params=pltpu.CompilerParams(dimension_semantics=("arbitrary", "arbitrary"), vmem_limit_bytes=60 * 2**20),
        cost_estimate=pl.CostEstimate(flops=18 * 10**9, transcendentals=0, bytes_accessed=12 * 2**20),
        name="attend_bwd",
    )(me, q, k, *vs, *dos, o, lse, cos, sin)


ANY = pl.BlockSpec(memory_space=pltpu.HBM)


def _load(pieces, whole, sems):
    copies, at = [], 0
    for i, piece in enumerate(pieces):
        n = piece.shape[0]
        copies.append(pltpu.make_async_copy(piece, whole.at[pl.ds(at, n), :], sems.at[i]))
        at += n
    for c in copies:
        c.start()
    return copies


def _params(mib, steps=1):
    return pltpu.CompilerParams(dimension_semantics=("arbitrary",) * steps, vmem_limit_bytes=mib * 2**20)


def _price(flops, arrays):
    return pl.CostEstimate(flops=flops, transcendentals=0, bytes_accessed=sum(a.size * 2 for a in arrays))


def _rows(pieces):
    return sum(p.shape[0] for p in pieces)


def qkv(pieces, wq, wk, wv):
    n, (d, nq), nk = len(pieces), wq.shape, wk.shape[1]
    rows, cut = _rows(pieces), 512

    def kernel(*refs):
        xs, (wq_ref, wk_ref, wv_ref), (q_ref, k_ref, v_ref) = refs[:n], refs[n : n + 3], refs[n + 3 : n + 6]
        x_s, q_s, k_s, v_s, sems, wsems = refs[n + 6 :]
        copies = _load(xs, x_s, sems)
        todo = []
        for i, at in enumerate(range(0, nq, cut)):
            here = slice(at, at + cut)
            todo.append((pltpu.make_async_copy(wq_ref.at[:, here], q_s.at[:, here], wsems.at[i]), q_s.at[:, here], q_ref, here))
        for i, (w, w_s, o) in enumerate(((wk_ref, k_s, k_ref), (wv_ref, v_s, v_ref))):
            todo.append((pltpu.make_async_copy(w, w_s, wsems.at[nq // cut + i]), w_s, o, slice(0, nk)))
        todo[0][0].start()
        for c in copies:
            c.wait()
        for i, (c, w_s, o, here) in enumerate(todo):
            c.wait()
            if i + 1 < len(todo):
                todo[i + 1][0].start()
            o[:, here] = _dot(x_s[...], w_s[...], 1, 0).astype(BF)

    return pl.pallas_call(
        kernel, in_specs=[ANY] * (n + 3), out_specs=[pl.BlockSpec(memory_space=pltpu.VMEM)] * 3,
        out_shape=[jax.ShapeDtypeStruct((rows, m), BF) for m in (nq, nk, nk)],
        scratch_shapes=[pltpu.VMEM((rows, d), BF), pltpu.VMEM((d, nq), BF), pltpu.VMEM((d, nk), BF), pltpu.VMEM((d, nk), BF),
                        pltpu.SemaphoreType.DMA((n,)), pltpu.SemaphoreType.DMA((nq // cut + 2,))],
        compiler_params=pltpu.CompilerParams(vmem_limit_bytes=57 * 2**20),
        cost_estimate=_price(2 * rows * d * (nq + 2 * nk), [*pieces, wq, wk, wv]), name="qkv",
    )(*pieces, wq, wk, wv)


def by_rows_of(pieces, w, bn, mib=60):
    n, (cols, d) = len(pieces), w.shape
    rows = _rows(pieces)
    steps, rest = -(-cols // bn), cols % bn
    small = -(-rest // 256) * 256

    def kernel(*refs):
        xs, w_ref, o_ref, x_s, sems = refs[:n], refs[n], refs[n + 1], refs[n + 2], refs[n + 3]
        i = pl.program_id(0)

        @pl.when(i == 0)
        def _():
            for c in _load(xs, x_s, sems):
                c.wait()

        if rest == 0 or small == bn:
            o_ref[...] = _dot(x_s[...], w_ref[...], 1, 1).astype(BF)
            return

        @pl.when(i < steps - 1)
        def _():
            o_ref[...] = _dot(x_s[...], w_ref[...], 1, 1).astype(BF)

        @pl.when(i == steps - 1)
        def _():
            o_ref[:, :small] = _dot(x_s[...], w_ref[:small, :], 1, 1).astype(BF)

    return pl.pallas_call(
        kernel, grid=(steps,), in_specs=[ANY] * n + [pl.BlockSpec((bn, d), lambda i: (i, 0))],
        out_specs=pl.BlockSpec((rows, bn), lambda i: (0, i)), out_shape=jax.ShapeDtypeStruct((rows, cols), BF),
        scratch_shapes=[pltpu.VMEM((rows, d), BF), pltpu.SemaphoreType.DMA((n,))], compiler_params=_params(mib),
        cost_estimate=_price(2 * rows * d * cols, [*pieces, w]),
    )(*pieces, w)


def mlp(pieces, dhid, wg, wu, bn=256):
    n, (d, cols) = len(pieces), wg.shape
    rows = _rows(pieces)

    def kernel(*refs):
        xs, (dhid_ref, g_ref, u_ref), (hid_ref, dg_ref, du_ref), (x_s, sems) = refs[:n], refs[n : n + 3], refs[n + 3 : n + 6], refs[n + 6 :]

        @pl.when(pl.program_id(0) == 0)
        def _():
            for c in _load(xs, x_s, sems):
                c.wait()

        gate, up = _dot(x_s[...], g_ref[...], 1, 0), _dot(x_s[...], u_ref[...], 1, 0)
        dhid = dhid_ref[...].astype(F32)
        sig = jax.nn.sigmoid(gate)
        silu = gate * sig
        hid_ref[...] = (silu * up).astype(BF)
        du_ref[...] = (dhid * silu).astype(BF)
        dg_ref[...] = (dhid * up * (sig + silu * (1 - sig))).astype(BF)

    w, o = pl.BlockSpec((d, bn), lambda i: (0, i)), pl.BlockSpec((rows, bn), lambda i: (0, i))
    return pl.pallas_call(
        kernel, grid=(-(-cols // bn),), in_specs=[ANY] * n + [o, w, w], out_specs=[o, o, o],
        out_shape=[jax.ShapeDtypeStruct((rows, cols), BF)] * 3,
        scratch_shapes=[pltpu.VMEM((rows, d), BF), pltpu.SemaphoreType.DMA((n,))], compiler_params=_params(56),
        cost_estimate=_price(4 * rows * d * cols, [*pieces, wg, wu, dhid, dhid, dhid]), name="mlp",
    )(*pieces, dhid, wg, wu)


def back(xs, ws, bn, half=0):
    n, d = len(xs), ws[0].shape[0]
    rows = 2 * BLOCK

    def kernel(*refs):
        x, w, (a_ref, b_ref) = refs[:n], refs[n : 2 * n], refs[2 * n :]
        total = _dot(x[0][...], w[0][...], 1, 1)
        for i in range(1, n):
            total += _dot(x[i][...], w[i][...], 1, 1)
        total = total.astype(BF)
        a_ref[...], b_ref[...] = total[:BLOCK], total[BLOCK:]

    o = pl.BlockSpec((BLOCK, bn), lambda i: (0, i))
    return pl.pallas_call(
        kernel, grid=(d // bn,),
        in_specs=[pl.BlockSpec((rows, x.shape[1]), lambda i: (half, 0)) for x in xs] + [pl.BlockSpec((bn, w.shape[1]), lambda i: (i, 0)) for w in ws],
        out_specs=[o, o], out_shape=[jax.ShapeDtypeStruct((BLOCK, d), BF)] * 2, compiler_params=_params(48),
        cost_estimate=_price(sum(2 * rows * d * w.shape[1] for w in ws), [*xs, *ws]),
    )(*xs, *ws)


def forth(x, w, bn, half):
    (d, cols), rows = w.shape, 2 * BLOCK

    def kernel(x_ref, w_ref, a_ref, b_ref):
        total = _dot(x_ref[...], w_ref[...], 1, 0).astype(BF)
        a_ref[...], b_ref[...] = total[:BLOCK], total[BLOCK:]

    o = pl.BlockSpec((BLOCK, bn), lambda i: (0, i))
    return pl.pallas_call(
        kernel, grid=(cols // bn,), in_specs=[pl.BlockSpec((rows, d), lambda i: (half, 0)), pl.BlockSpec((d, bn), lambda i: (0, i))],
        out_specs=[o, o], out_shape=[jax.ShapeDtypeStruct((BLOCK, cols), BF)] * 2, compiler_params=_params(60),
        cost_estimate=_price(2 * rows * d * cols, [x, w]),
    )(x, w)


def weight_grads(lefts, rights, bm, mib=48):
    n, m, rows = len(lefts), lefts[0].shape[1], _rows(lefts)
    counts = [len(r) for r in rights]
    widths = [r[0].shape[1] for r in rights]

    def kernel(*refs):
        ls, refs = refs[:n], refs[n:]
        rs = []
        for c in counts:
            rs.append(refs[:c])
            refs = refs[c:]
        outs, wholes, sems = refs[: len(rights)], refs[len(rights) : 2 * len(rights)], refs[2 * len(rights) :]

        @pl.when(pl.program_id(0) == 0)
        def _():
            for c in [c for r, w, s in zip(rs, wholes, sems) for c in _load(r, w, s)]:
                c.wait()

        left = jnp.concatenate([l[...] for l in ls], axis=0).T
        for o, w in zip(outs, wholes):
            o[...] = _dot(left, w[...], 1, 0).astype(BF)

    return pl.pallas_call(
        kernel, grid=(m // bm,),
        in_specs=[pl.BlockSpec((l.shape[0], bm), lambda i: (0, i)) for l in lefts] + [ANY] * sum(counts),
        out_specs=[pl.BlockSpec((bm, w), lambda i: (i, 0)) for w in widths],
        out_shape=[jax.ShapeDtypeStruct((m, w), BF) for w in widths],
        scratch_shapes=[pltpu.VMEM((rows, w), BF) for w in widths] + [pltpu.SemaphoreType.DMA((c,)) for c in counts],
        compiler_params=_params(mib), cost_estimate=_price(2 * rows * m * sum(widths), [*lefts, *(p for r in rights for p in r)]),
    )(*lefts, *(p for r in rights for p in r))


CORE = [(0, 1), (1, 0), (2, 3), (3, 2)]
CROSS = [(0, 2), (2, 0), (1, 3), (3, 1)]


def core(v):
    return lax.ppermute(v, "tp", CORE)


def cross(v):
    return lax.ppermute(v, "tp", CROSS)


def after(v, *others):
    return lax.optimization_barrier((v, *others))[0]


def later(pieces, *others):
    return [after(pieces[0], *others), *pieces[1:]]


def gather(v):
    return [v, core(v)], cross(v)


def far_of(first, *others):
    first = after(first, *others)
    return [first, core(first)]


def scatter_far(mine, other):
    both = (mine.astype(F32) + core(other).astype(F32)).astype(BF)
    return both, cross(both)


def _scale(wide):
    return lax.rsqrt(jnp.mean(wide**2, -1, keepdims=True) + 1e-6)


def by_row(f, arrays, outs):
    rows, d = arrays[0].shape

    def kernel(*refs):
        got = f(*(r[...].astype(F32) for r in refs[: len(arrays)]))
        for ref, t in zip(refs[len(arrays) :], got, strict=True):
            ref[...] = t.astype(BF)

    spec = pl.BlockSpec((32, d), lambda i: (i, 0))
    return pl.pallas_call(
        kernel, grid=(rows // 32,), in_specs=[spec] * len(arrays), out_specs=[spec] * outs,
        out_shape=[jax.ShapeDtypeStruct((rows, d), BF)] * outs, compiler_params=_params(60),
        cost_estimate=_price(10 * rows * d, [*arrays, *arrays[:outs]]),
    )(*arrays)


def norm(h):
    return by_row(lambda wide: (wide * _scale(wide),), [h], 1)[0]


def add_norm(h, mine, other, far):
    def f(h, *terms):
        wide = (h + sum(terms)).astype(BF).astype(F32)
        return wide, wide * _scale(wide)

    return by_row(f, [h, mine, core(other), far], 2)


def norm_bwd(direct, h, mine, other, far):
    def f(direct, h, *terms):
        g, scale = sum(terms).astype(BF).astype(F32), _scale(h)
        return (direct + scale * g - h * (scale**3 * jnp.mean(g * h, -1, keepdims=True)),)

    return by_row(f, [direct, h, mine, core(other), far], 1)[0]


def layer(x, dy, wq, wk, wv, wo, wg, wu, wd):
    x, dy = x[0], dy[0]
    me = lax.axis_index("tp").astype(jnp.int32).reshape(1)
    tokens = 4 * x.shape[0]
    half = HEAD // 2
    angle = jnp.arange(tokens, dtype=F32)[:, None] * THETA ** (-jnp.arange(half, dtype=F32) / half)
    cos, sin = jnp.cos(angle), jnp.sin(angle)
    cos, sin = jnp.concatenate([cos, cos], 1), jnp.concatenate([-sin, sin], 1)

    a = norm(x)
    a_near, a_far = gather(a)
    dy_near = [dy, core(dy)]
    near_qkv = qkv(a_near, wq, wk, wv)
    dhid_near = by_rows_of(later(dy_near, near_qkv[0]), wd, 512)
    a_far = far_of(a_far, dhid_near, cos, sin)
    dy_far = cross(after(dy, a_far[0]))
    far_qkv = qkv(a_far, wq, wk, wv)
    qs, ks, vs = zip(near_qkv, far_qkv)
    heads, lse, q, k = attend(me, qs, ks, vs, cos, sin)
    terms = forth(heads, wo, 1024, 1)
    near = forth(after(heads, terms[1]), wo, 1024, 0)
    both, far = scatter_far(*terms)
    dy_far = far_of(dy_far, both, near[0])
    dhid_far = by_rows_of(dy_far, wd, 512)
    h, b = add_norm(x, *near, after(far, dhid_far))
    b_near, b_far = gather(b)
    hid_near, dgate_near, dup_near = mlp(b_near, dhid_near, wg, wu)
    b_far = far_of(b_far, hid_near)
    hid_far, dgate_far, dup_far = mlp(b_far, dhid_far, wg, wu)
    terms = back([dgate_far, dup_far], [wg, wu], 512)
    near = back(later([dgate_near, dup_near], terms[1]), [wg, wu], 512)
    both, far = scatter_far(after(terms[0], near[0]), terms[1])
    d_wg, d_wu = weight_grads(later([*b_near, *b_far], both), [[dgate_near, dgate_far], [dup_near, dup_far]], 512, 56)
    dh = norm_bwd(dy, h, *near, after(far, d_wg))
    dh_near, dh_far = gather(dh)
    (d_wd,) = weight_grads(later([hid_near, hid_far], dh), [[*dy_near, *dy_far]], 640)
    dheads_near = by_rows_of(later(dh_near, d_wd), wo, 512)
    dh_far = far_of(dh_far, dheads_near)
    dheads_far = by_rows_of(dh_far, wo, 512)
    dq, dk, dv = attend_bwd(me, q, k, vs, (dheads_near, dheads_far), heads, lse, cos, sin)
    both, far = scatter_far(*back([dq, dk, dv], [wq, wk, wv], 512, 1))
    near = back(later([dq, dk, dv], both), [wq, wk, wv], 512)
    d_wq, d_wk, d_wv = weight_grads(later([*a_near, *a_far], near[0]), [[dq], [dk], [dv]], 512)
    (d_wo,) = weight_grads(later([heads], d_wq), [[*dh_near, *dh_far]], 512)
    dx = norm_bwd(dh, x, *near, after(far, d_wo))
    return (dx[None], d_wq, d_wk, d_wv, d_wo, d_wg, d_wu, d_wd)


def solution(mesh):
    states, by_columns, by_rows = P("dp", "tp", None), P(None, "tp"), P("tp", None)
    weights = (by_columns, by_columns, by_columns, by_rows, by_columns, by_columns, by_rows)
    own = tuple(P("dp", "tp") if spec == by_columns else P(("dp", "tp"), None) for spec in weights)
    return jax.shard_map(layer, mesh=mesh, in_specs=(states, states, *weights), out_specs=(states, *own), check_vma=False)
```

```python
import functools

import jax
import jax.numpy as jnp
from jax import lax
from jax.experimental import pallas as pl
from jax.experimental.pallas import tpu as pltpu
from jax.sharding import PartitionSpec as P


HEAD = 128
THETA = 10000
LOG2E = 1.4426950408889634
HIDDEN = -2e30
SCALE = HEAD**-0.5
BF, F32 = jnp.bfloat16, jnp.float32
BLOCK = 256
STRIP = 512


def _dot(a, b, ca, cb):
    return lax.dot_general(a, b, (((ca,), (cb,)), ((), ())), preferred_element_type=F32)


def _rope(x, cos, sin):
    x = x.astype(F32)
    return x * cos + pltpu.roll(x, HEAD // 2, 1) * sin


def _unrope(x, cos, sin):
    return x * cos - pltpu.roll(x, HEAD // 2, 1) * sin


def _hidden(cols):
    key = lax.broadcasted_iota(jnp.int32, (BLOCK, cols), 0)
    return key > lax.rem(lax.broadcasted_iota(jnp.int32, (BLOCK, cols), 1), BLOCK)


def _attend(me_ref, qn_ref, qf_ref, kn_ref, kf_ref, vn_ref, vf_ref, cos_ref, sin_ref, o_ref, lse_ref, qr_ref, kr_ref, vt_s, q_s):
    iq = pl.program_id(1)
    me = me_ref[0]
    n = kr_ref.shape[0] // BLOCK
    g = qr_ref.shape[1] // HEAD
    cols = g * BLOCK
    e = SCALE * LOG2E

    @pl.when(iq == 0)
    def _():
        for s in range(n):
            here = pl.ds((s ^ me) * BLOCK, BLOCK)
            rows, half = slice(s * BLOCK, (s + 1) * BLOCK), slice(s % 2 * BLOCK, (s % 2 + 1) * BLOCK)
            k, v = (kn_ref, vn_ref) if s < 2 else (kf_ref, vf_ref)
            kr_ref[rows, :] = _rope(k[half, :], cos_ref[here, :], sin_ref[here, :]).astype(BF)
            vt_s[s, :HEAD, :] = v[half, :].T
            vt_s[s, HEAD:, :] = jnp.ones((8, BLOCK), BF)

    here = pl.ds(iq * BLOCK, BLOCK)
    cos, sin = cos_ref[here, :], sin_ref[here, :]
    near = (iq ^ me) < 2

    def turn(q_ref):
        for h in range(g):
            turned = _rope(q_ref[:, h * HEAD : (h + 1) * HEAD], cos, sin).astype(BF)
            qr_ref[:, h * HEAD : (h + 1) * HEAD] = turned
            q_s[h * BLOCK : (h + 1) * BLOCK, :] = turned

    pl.when(near)(lambda: turn(qn_ref))
    pl.when(jnp.logical_not(near))(lambda: turn(qf_ref))

    def queries(blocks):
        for at in range(0, cols, STRIP):
            lanes = slice(at, at + STRIP)
            slots = [j ^ me for j in range(blocks)]
            scores = [_dot(kr_ref[pl.ds(pl.multiple_of(j * BLOCK, BLOCK), BLOCK), :], q_s[lanes, :], 1, 1) for j in slots]
            scores[-1] = jnp.where(_hidden(STRIP), HIDDEN, scores[-1])
            top = functools.reduce(jnp.maximum, [s.max(axis=0, keepdims=True) for s in scores])
            mix = sum(_dot(vt_s[j], jnp.exp2((s - top) * e).astype(BF), 1, 0) for j, s in zip(slots, scores))
            total = mix[HEAD : HEAD + 1, :]
            out = (mix[:HEAD, :] * (1 / total)).T.astype(BF)
            for h in range(STRIP // BLOCK):
                to = at // BLOCK + h
                o_ref[:, to * HEAD : (to + 1) * HEAD] = out[h * BLOCK : (h + 1) * BLOCK, :]
            lse_ref[0, :, lanes] = top * e + jnp.log2(total)

    for i in range(n):
        pl.when(iq == i)(functools.partial(queries, i + 1))


def _attend_bwd(me_ref, q_ref, k_ref, vn_ref, vf_ref, don_ref, dof_ref, o_ref, lse_ref, cos_ref, sin_ref, dq_ref, dk_ref, dv_ref,
                q_s, do_s, dq_s, dk_s, dv_s, kt_s, v_s, delta_s):
    iq = pl.program_id(1)
    me = me_ref[0]
    n = k_ref.shape[0] // BLOCK
    g = q_ref.shape[1] // HEAD
    cols = g * BLOCK
    e = SCALE * LOG2E

    @pl.when(iq == 0)
    def _():
        dk_s[...] = jnp.zeros_like(dk_s)
        dv_s[...] = jnp.zeros_like(dv_s)
        v_s[: 2 * BLOCK, :], v_s[2 * BLOCK :, :] = vn_ref[...], vf_ref[...]
        for s in range(n):
            kt_s[s] = k_ref[s * BLOCK : (s + 1) * BLOCK, :].T

    dq_s[...] = jnp.zeros_like(dq_s)
    near = (iq ^ me) < 2

    def take(do_ref):
        for h in range(g):
            lanes, rows = slice(h * HEAD, (h + 1) * HEAD), slice(h * BLOCK, (h + 1) * BLOCK)
            q_s[rows, :] = q_ref[:, lanes]
            do_s[rows, :] = do_ref[:, lanes]
            prod = do_ref[:, lanes].astype(F32) * o_ref[:, lanes].astype(F32)
            delta_s[:, rows] = prod.T.sum(axis=0, keepdims=True)

    pl.when(near)(lambda: take(don_ref))
    pl.when(jnp.logical_not(near))(lambda: take(dof_ref))

    def block(j, masked):
        slot = j ^ me
        here = pl.ds(pl.multiple_of(slot * BLOCK, BLOCK), BLOCK)
        keys, values = k_ref[here, :], v_s[here, :]
        strips = range(0, cols, STRIP)
        scores = [_dot(keys, q_s[at : at + STRIP, :], 1, 1) for at in strips]
        dps = [_dot(values, do_s[at : at + STRIP, :], 1, 1) for at in strips]
        for at, s, dp in zip(strips, scores, dps):
            p = jnp.exp2(s * e - lse_ref[0, :, at : at + STRIP])
            if masked:
                p = jnp.where(_hidden(STRIP), 0.0, p)
            ds = (p * (dp - delta_s[:, at : at + STRIP])).astype(BF)
            dv_s[here, :] += _dot(p.astype(BF), do_s[at : at + STRIP, :], 1, 0)
            dk_s[here, :] += _dot(ds, q_s[at : at + STRIP, :], 1, 0)
            dq_s[:, at : at + STRIP] += _dot(kt_s[slot], ds, 1, 0)

    def queries(blocks):
        for j in range(blocks):
            block(j, j == blocks - 1)

    for i in range(n):
        pl.when(iq == i)(functools.partial(queries, i + 1))
    here = pl.ds(iq * BLOCK, BLOCK)
    cos, sin = cos_ref[here, :], sin_ref[here, :]
    dq = (dq_s[...] * SCALE).T
    for h in range(g):
        dq_ref[:, h * HEAD : (h + 1) * HEAD] = _unrope(dq[h * BLOCK : (h + 1) * BLOCK, :], cos, sin).astype(BF)

    @pl.when(iq == n - 1)
    def _():
        for s in range(n):
            here = pl.ds((s ^ me) * BLOCK, BLOCK)
            rows = slice(s * BLOCK, (s + 1) * BLOCK)
            dk_ref[rows, :] = _unrope(dk_s[rows, :] * SCALE, cos_ref[here, :], sin_ref[here, :]).astype(BF)
            dv_ref[rows, :] = dv_s[rows, :].astype(BF)


def _attn_specs(tokens, g):
    queries = pl.BlockSpec((BLOCK, g * HEAD), lambda h, i, me: (i ^ me[0], h))
    near = pl.BlockSpec((BLOCK, g * HEAD), lambda h, i, me: (jnp.minimum(i ^ me[0], 1), h))
    far = pl.BlockSpec((BLOCK, g * HEAD), lambda h, i, me: (jnp.maximum((i ^ me[0]) - 2, 0), h))
    keys = pl.BlockSpec((tokens, HEAD), lambda h, i, me: (0, h))
    half = pl.BlockSpec((tokens // 2, HEAD), lambda h, i, me: (0, h))
    table = pl.BlockSpec((tokens, HEAD), lambda h, i, me: (0, 0))
    stats = pl.BlockSpec((1, 1, g * BLOCK), lambda h, i, me: (h * (tokens // BLOCK) + i, 0, 0))
    return queries, near, far, keys, half, table, stats


def attend(me, qs, ks, vs, cos, sin):
    tokens, width, kv = 2 * ks[0].shape[0], qs[0].shape[1], ks[0].shape[1] // HEAD
    g = width // ks[0].shape[1]
    queries, near, far, keys, half, table, stats = _attn_specs(tokens, g)
    n = tokens // BLOCK
    return pl.pallas_call(
        _attend,
        grid_spec=pltpu.PrefetchScalarGridSpec(
            num_scalar_prefetch=1, grid=(kv, n), in_specs=[near, far, half, half, half, half, table, table],
            out_specs=[queries, stats, queries, keys],
            scratch_shapes=[pltpu.VMEM((n, HEAD + 8, BLOCK), BF), pltpu.VMEM((g * BLOCK, HEAD), BF)]),
        out_shape=[jax.ShapeDtypeStruct((tokens, width), BF), jax.ShapeDtypeStruct((kv * n, 1, g * BLOCK), F32),
                   jax.ShapeDtypeStruct((tokens, width), BF), jax.ShapeDtypeStruct((tokens, kv * HEAD), BF)],
        compiler_params=pltpu.CompilerParams(dimension_semantics=("arbitrary", "arbitrary"), vmem_limit_bytes=60 * 2**20),
        cost_estimate=pl.CostEstimate(flops=12 * 10**9, transcendentals=0, bytes_accessed=8 * 2**20),
        name="attend",
    )(me, *qs, *ks, *vs, cos, sin)


def attend_bwd(me, q, k, vs, dos, o, lse, cos, sin):
    tokens, kv = k.shape[0], k.shape[1] // HEAD
    g = q.shape[1] // k.shape[1]
    queries, near, far, keys, half, table, stats = _attn_specs(tokens, g)
    n = tokens // BLOCK
    return pl.pallas_call(
        _attend_bwd,
        grid_spec=pltpu.PrefetchScalarGridSpec(
            num_scalar_prefetch=1, grid=(kv, n), in_specs=[queries, keys, half, half, near, far, queries, stats, table, table],
            out_specs=[queries, keys, keys],
            scratch_shapes=[pltpu.VMEM((g * BLOCK, HEAD), BF), pltpu.VMEM((g * BLOCK, HEAD), BF), pltpu.VMEM((HEAD, g * BLOCK), F32),
                            pltpu.VMEM((tokens, HEAD), F32), pltpu.VMEM((tokens, HEAD), F32), pltpu.VMEM((n, HEAD, BLOCK), BF),
                            pltpu.VMEM((tokens, HEAD), BF), pltpu.VMEM((1, g * BLOCK), F32)]),
        out_shape=[jax.ShapeDtypeStruct(q.shape, BF), jax.ShapeDtypeStruct(k.shape, BF), jax.ShapeDtypeStruct(k.shape, BF)],
        compiler_params=pltpu.CompilerParams(dimension_semantics=("arbitrary", "arbitrary"), vmem_limit_bytes=60 * 2**20),
        cost_estimate=pl.CostEstimate(flops=18 * 10**9, transcendentals=0, bytes_accessed=12 * 2**20),
        name="attend_bwd",
    )(me, q, k, *vs, *dos, o, lse, cos, sin)


ANY = pl.BlockSpec(memory_space=pltpu.HBM)


def _load(pieces, whole, sems):
    copies, at = [], 0
    for i, piece in enumerate(pieces):
        n = piece.shape[0]
        copies.append(pltpu.make_async_copy(piece, whole.at[pl.ds(at, n), :], sems.at[i]))
        at += n
    for c in copies:
        c.start()
    return copies


def _params(mib, steps=1):
    return pltpu.CompilerParams(dimension_semantics=("arbitrary",) * steps, vmem_limit_bytes=mib * 2**20)


def _price(flops, arrays):
    return pl.CostEstimate(flops=flops, transcendentals=0, bytes_accessed=sum(a.size * 2 for a in arrays))


def _rows(pieces):
    return sum(p.shape[0] for p in pieces)


def qkv(pieces, wq, wk, wv):
    n, (d, nq), nk = len(pieces), wq.shape, wk.shape[1]
    rows, cut = _rows(pieces), 512

    def kernel(*refs):
        xs, (wq_ref, wk_ref, wv_ref), (q_ref, k_ref, v_ref) = refs[:n], refs[n : n + 3], refs[n + 3 : n + 6]
        x_s, q_s, k_s, v_s, sems, wsems = refs[n + 6 :]
        copies = _load(xs, x_s, sems)
        todo = []
        for i, at in enumerate(range(0, nq, cut)):
            here = slice(at, at + cut)
            todo.append((pltpu.make_async_copy(wq_ref.at[:, here], q_s.at[:, here], wsems.at[i]), q_s.at[:, here], q_ref, here))
        for i, (w, w_s, o) in enumerate(((wk_ref, k_s, k_ref), (wv_ref, v_s, v_ref))):
            todo.append((pltpu.make_async_copy(w, w_s, wsems.at[nq // cut + i]), w_s, o, slice(0, nk)))
        todo[0][0].start()
        for c in copies:
            c.wait()
        for i, (c, w_s, o, here) in enumerate(todo):
            c.wait()
            if i + 1 < len(todo):
                todo[i + 1][0].start()
            o[:, here] = _dot(x_s[...], w_s[...], 1, 0).astype(BF)

    return pl.pallas_call(
        kernel, in_specs=[ANY] * (n + 3), out_specs=[pl.BlockSpec(memory_space=pltpu.VMEM)] * 3,
        out_shape=[jax.ShapeDtypeStruct((rows, m), BF) for m in (nq, nk, nk)],
        scratch_shapes=[pltpu.VMEM((rows, d), BF), pltpu.VMEM((d, nq), BF), pltpu.VMEM((d, nk), BF), pltpu.VMEM((d, nk), BF),
                        pltpu.SemaphoreType.DMA((n,)), pltpu.SemaphoreType.DMA((nq // cut + 2,))],
        compiler_params=pltpu.CompilerParams(vmem_limit_bytes=57 * 2**20),
        cost_estimate=_price(2 * rows * d * (nq + 2 * nk), [*pieces, wq, wk, wv]), name="qkv",
    )(*pieces, wq, wk, wv)


def by_rows_of(pieces, w, bn, mib=40):
    n, (cols, d) = len(pieces), w.shape
    rows = _rows(pieces)
    steps, rest = -(-cols // bn), cols % bn
    small = -(-rest // 256) * 256

    def kernel(*refs):
        xs, w_ref, o_ref, x_s, sems = refs[:n], refs[n], refs[n + 1], refs[n + 2], refs[n + 3]
        i = pl.program_id(0)

        @pl.when(i == 0)
        def _():
            for c in _load(xs, x_s, sems):
                c.wait()

        if rest == 0 or small == bn:
            o_ref[...] = _dot(x_s[...], w_ref[...], 1, 1).astype(BF)
            return

        @pl.when(i < steps - 1)
        def _():
            o_ref[...] = _dot(x_s[...], w_ref[...], 1, 1).astype(BF)

        @pl.when(i == steps - 1)
        def _():
            o_ref[:, :small] = _dot(x_s[...], w_ref[:small, :], 1, 1).astype(BF)

    return pl.pallas_call(
        kernel, grid=(steps,), in_specs=[ANY] * n + [pl.BlockSpec((bn, d), lambda i: (i, 0))],
        out_specs=pl.BlockSpec((rows, bn), lambda i: (0, i)), out_shape=jax.ShapeDtypeStruct((rows, cols), BF),
        scratch_shapes=[pltpu.VMEM((rows, d), BF), pltpu.SemaphoreType.DMA((n,))], compiler_params=_params(mib),
        cost_estimate=_price(2 * rows * d * cols, [*pieces, w]),
    )(*pieces, w)


def mlp(pieces, dhid, wg, wu, bn=256):
    n, (d, cols) = len(pieces), wg.shape
    rows = _rows(pieces)

    def kernel(*refs):
        xs, (dhid_ref, g_ref, u_ref), (hid_ref, dg_ref, du_ref), x_s = refs[:n], refs[n : n + 3], refs[n + 3 : n + 6], refs[n + 6]

        @pl.when(pl.program_id(0) == 0)
        def _():
            at = 0
            for x in xs:
                x_s[at : at + x.shape[0], :] = x[...]
                at += x.shape[0]

        gate, up = _dot(x_s[...], g_ref[...], 1, 0), _dot(x_s[...], u_ref[...], 1, 0)
        dhid = dhid_ref[...].astype(F32)
        sig = jax.nn.sigmoid(gate)
        silu = gate * sig
        hid_ref[...] = (silu * up).astype(BF)
        du_ref[...] = (dhid * silu).astype(BF)
        dg_ref[...] = (dhid * up * (sig + silu * (1 - sig))).astype(BF)

    w, o = pl.BlockSpec((d, bn), lambda i: (0, i)), pl.BlockSpec((rows, bn), lambda i: (0, i))
    return pl.pallas_call(
        kernel, grid=(-(-cols // bn),), out_specs=[o, o, o],
        in_specs=[pl.BlockSpec(p.shape, lambda i: (0, 0), pipeline_mode=pl.Buffered(1)) for p in pieces] + [o, w, w],
        out_shape=[jax.ShapeDtypeStruct((rows, cols), BF)] * 3,
        scratch_shapes=[pltpu.VMEM((rows, d), BF)], compiler_params=_params(56),
        cost_estimate=_price(4 * rows * d * cols, [*pieces, wg, wu, dhid, dhid, dhid]), name="mlp",
    )(*pieces, dhid, wg, wu)


def back(xs, ws, bn, half=0):
    n, d = len(xs), ws[0].shape[0]
    rows = 2 * BLOCK

    def kernel(*refs):
        x, w, (a_ref, b_ref) = refs[:n], refs[n : 2 * n], refs[2 * n :]
        total = _dot(x[0][...], w[0][...], 1, 1)
        for i in range(1, n):
            total += _dot(x[i][...], w[i][...], 1, 1)
        total = total.astype(BF)
        a_ref[...], b_ref[...] = total[:BLOCK], total[BLOCK:]

    o = pl.BlockSpec((BLOCK, bn), lambda i: (0, i))
    return pl.pallas_call(
        kernel, grid=(d // bn,),
        in_specs=[pl.BlockSpec((rows, x.shape[1]), lambda i: (half, 0)) for x in xs] + [pl.BlockSpec((bn, w.shape[1]), lambda i: (i, 0)) for w in ws],
        out_specs=[o, o], out_shape=[jax.ShapeDtypeStruct((BLOCK, d), BF)] * 2, compiler_params=_params(48),
        cost_estimate=_price(sum(2 * rows * d * w.shape[1] for w in ws), [*xs, *ws]),
    )(*xs, *ws)


def forth(x, w, bn, half):
    (d, cols), rows = w.shape, 2 * BLOCK

    def kernel(x_ref, w_ref, a_ref, b_ref):
        total = _dot(x_ref[...], w_ref[...], 1, 0).astype(BF)
        a_ref[...], b_ref[...] = total[:BLOCK], total[BLOCK:]

    o = pl.BlockSpec((BLOCK, bn), lambda i: (0, i))
    return pl.pallas_call(
        kernel, grid=(cols // bn,), in_specs=[pl.BlockSpec((rows, d), lambda i: (half, 0)), pl.BlockSpec((d, bn), lambda i: (0, i))],
        out_specs=[o, o], out_shape=[jax.ShapeDtypeStruct((BLOCK, cols), BF)] * 2, compiler_params=_params(60),
        cost_estimate=_price(2 * rows * d * cols, [x, w]),
    )(x, w)


def weight_grads(lefts, rights, bm, mib=48):
    n, m, rows = len(lefts), lefts[0].shape[1], _rows(lefts)
    counts = [len(r) for r in rights]
    widths = [r[0].shape[1] for r in rights]

    def kernel(*refs):
        ls, refs = refs[:n], refs[n:]
        rs = []
        for c in counts:
            rs.append(refs[:c])
            refs = refs[c:]
        outs, wholes, sems = refs[: len(rights)], refs[len(rights) : 2 * len(rights)], refs[2 * len(rights) :]

        @pl.when(pl.program_id(0) == 0)
        def _():
            for c in [c for r, w, s in zip(rs, wholes, sems) for c in _load(r, w, s)]:
                c.wait()

        left = jnp.concatenate([l[...] for l in ls], axis=0).T
        for o, w in zip(outs, wholes):
            o[...] = _dot(left, w[...], 1, 0).astype(BF)

    return pl.pallas_call(
        kernel, grid=(m // bm,),
        in_specs=[pl.BlockSpec((l.shape[0], bm), lambda i: (0, i)) for l in lefts] + [ANY] * sum(counts),
        out_specs=[pl.BlockSpec((bm, w), lambda i: (i, 0)) for w in widths],
        out_shape=[jax.ShapeDtypeStruct((m, w), BF) for w in widths],
        scratch_shapes=[pltpu.VMEM((rows, w), BF) for w in widths] + [pltpu.SemaphoreType.DMA((c,)) for c in counts],
        compiler_params=_params(mib), cost_estimate=_price(2 * rows * m * sum(widths), [*lefts, *(p for r in rights for p in r)]),
    )(*lefts, *(p for r in rights for p in r))


CORE = [(0, 1), (1, 0), (2, 3), (3, 2)]
CROSS = [(0, 2), (2, 0), (1, 3), (3, 1)]


def core(v):
    return lax.ppermute(v, "tp", CORE)


def cross(v):
    return lax.ppermute(v, "tp", CROSS)


def after(v, *others):
    return lax.optimization_barrier((v, *others))[0]


def later(pieces, *others):
    return [after(pieces[0], *others), *pieces[1:]]


def gather(v):
    return [v, core(v)], cross(v)


def far_of(first, *others):
    first = after(first, *others)
    return [first, core(first)]


def scatter_far(mine, other):
    both = (mine.astype(F32) + core(other).astype(F32)).astype(BF)
    return both, cross(both)


def _scale(wide):
    return lax.rsqrt(jnp.mean(wide**2, -1, keepdims=True) + 1e-6)


def by_row(f, arrays, outs, block=128, mib=60):
    rows, d = arrays[0].shape

    def kernel(*refs):
        got = f(*(r[...].astype(F32) for r in refs[: len(arrays)]))
        for ref, t in zip(refs[len(arrays) :], got, strict=True):
            ref[...] = t.astype(BF)

    spec = pl.BlockSpec((block, d), lambda i: (i, 0))
    return pl.pallas_call(
        kernel, grid=(rows // block,), in_specs=[spec] * len(arrays), out_specs=[spec] * outs,
        out_shape=[jax.ShapeDtypeStruct((rows, d), BF)] * outs, compiler_params=_params(mib),
        cost_estimate=_price(10 * rows * d, [*arrays, *arrays[:outs]]),
    )(*arrays)


def norm(h):
    return by_row(lambda wide: (wide * _scale(wide),), [h], 1, 32, 24)[0]


def add_norm(h, mine, other, far):
    def f(h, *terms):
        wide = (h + sum(terms)).astype(BF).astype(F32)
        return wide, wide * _scale(wide)

    return by_row(f, [h, mine, core(other), far], 2, 32, 24)


def norm_bwd(direct, h, mine, other, far):
    def f(direct, h, *terms):
        g, scale = sum(terms).astype(BF).astype(F32), _scale(h)
        return (direct + scale * g - h * (scale**3 * jnp.mean(g * h, -1, keepdims=True)),)

    return by_row(f, [direct, h, mine, core(other), far], 1)[0]


def layer(x, dy, wq, wk, wv, wo, wg, wu, wd):
    x, dy = x[0], dy[0]
    me = lax.axis_index("tp").astype(jnp.int32).reshape(1)
    tokens = 4 * x.shape[0]
    half = HEAD // 2
    angle = jnp.arange(tokens, dtype=F32)[:, None] * THETA ** (-jnp.arange(half, dtype=F32) / half)
    cos, sin = jnp.cos(angle), jnp.sin(angle)
    cos, sin = jnp.concatenate([cos, cos], 1), jnp.concatenate([-sin, sin], 1)

    a = norm(x)
    a_near, a_far = gather(a)
    dy_near = [dy, core(dy)]
    near_qkv = qkv(a_near, wq, wk, wv)
    dhid_near = by_rows_of(later(dy_near, near_qkv[0]), wd, 512)
    a_far = far_of(a_far, dhid_near, cos, sin)
    dy_far = cross(after(dy, a_far[0]))
    far_qkv = qkv(a_far, wq, wk, wv)
    qs, ks, vs = zip(near_qkv, far_qkv)
    heads, lse, q, k = attend(me, qs, ks, vs, cos, sin)
    terms = forth(heads, wo, 1024, 1)
    both, far = scatter_far(*terms)
    near = forth(after(heads, both), wo, 1024, 0)
    dy_far = far_of(dy_far, both, near[0])
    dhid_far = by_rows_of(dy_far, wd, 512)
    h, b = add_norm(x, *near, after(far, dhid_far))
    b_near, b_far = gather(b)
    hid_near, dgate_near, dup_near = mlp(b_near, dhid_near, wg, wu)
    b_far = far_of(b_far, hid_near)
    hid_far, dgate_far, dup_far = mlp(b_far, dhid_far, wg, wu)
    terms = back([dgate_far, dup_far], [wg, wu], 512)
    near = back(later([dgate_near, dup_near], terms[1]), [wg, wu], 512)
    both, far = scatter_far(after(terms[0], near[0]), terms[1])
    d_wg, d_wu = weight_grads(later([*b_near, *b_far], both), [[dgate_near, dgate_far], [dup_near, dup_far]], 512, 56)
    dh = norm_bwd(dy, h, *near, after(far, d_wg))
    dh_near, dh_far = gather(dh)
    (d_wd,) = weight_grads(later([hid_near, hid_far], dh), [[*dy_near, *dy_far]], 640)
    dheads_near = by_rows_of(later(dh_near, d_wd), wo, 512, 60)
    dh_far = far_of(dh_far, dheads_near)
    dheads_far = by_rows_of(dh_far, wo, 512, 60)
    dq, dk, dv = attend_bwd(me, q, k, vs, (dheads_near, dheads_far), heads, lse, cos, sin)
    both, far = scatter_far(*back([dq, dk, dv], [wq, wk, wv], 512, 1))
    near = back(later([dq, dk, dv], both), [wq, wk, wv], 512)
    d_wq, d_wk, d_wv = weight_grads(later([*a_near, *a_far], near[0]), [[dq], [dk], [dv]], 512)
    (d_wo,) = weight_grads(later([heads], d_wq), [[*dh_near, *dh_far]], 512)
    dx = norm_bwd(dh, x, *near, after(far, d_wo))
    return (dx[None], d_wq, d_wk, d_wv, d_wo, d_wg, d_wu, d_wd)


def solution(mesh):
    states, by_columns, by_rows = P("dp", "tp", None), P(None, "tp"), P("tp", None)
    weights = (by_columns, by_columns, by_columns, by_rows, by_columns, by_columns, by_rows)
    own = tuple(P("dp", "tp") if spec == by_columns else P(("dp", "tp"), None) for spec in weights)
    return jax.shard_map(layer, mesh=mesh, in_specs=(states, states, *weights), out_specs=(states, *own), check_vma=False)
```

```python
import functools

import jax
import jax.numpy as jnp
from jax import lax
from jax.experimental import pallas as pl
from jax.experimental.pallas import tpu as pltpu
from jax.sharding import PartitionSpec as P


HEAD = 128
THETA = 10000
LOG2E = 1.4426950408889634
HIDDEN = -2e30
SCALE = HEAD**-0.5
BF, F32 = jnp.bfloat16, jnp.float32
BLOCK = 256
STRIP, STRIP_BWD = 1024, 512


def _dot(a, b, ca, cb):
    return lax.dot_general(a, b, (((ca,), (cb,)), ((), ())), preferred_element_type=F32)


def _rope(x, cos, sin):
    x = x.astype(F32)
    return x * cos + pltpu.roll(x, HEAD // 2, 1) * sin


def _unrope(x, cos, sin):
    return x * cos - pltpu.roll(x, HEAD // 2, 1) * sin


def _hidden(cols):
    key = lax.broadcasted_iota(jnp.int32, (BLOCK, cols), 0)
    return key > lax.rem(lax.broadcasted_iota(jnp.int32, (BLOCK, cols), 1), BLOCK)


def _attend(me_ref, qn_ref, qf_ref, kn_ref, kf_ref, vn_ref, vf_ref, cos_ref, sin_ref, o_ref, lse_ref, qr_ref, kr_ref, vt_s, q_s):
    iq = pl.program_id(1)
    me = me_ref[0]
    n = kr_ref.shape[0] // BLOCK
    g = qr_ref.shape[1] // HEAD
    cols = g * BLOCK
    e = SCALE * LOG2E

    @pl.when(iq == 0)
    def _():
        for s in range(n):
            here = pl.ds(pl.multiple_of((s ^ me) * BLOCK, BLOCK), BLOCK)
            half = slice(s % 2 * BLOCK, (s % 2 + 1) * BLOCK)
            k, v = (kn_ref, vn_ref) if s < 2 else (kf_ref, vf_ref)
            kr_ref[here, :] = _rope(k[half, :], cos_ref[here, :], sin_ref[here, :]).astype(BF)
            vt_s[s ^ me, :HEAD, :] = v[half, :].T
            vt_s[s, HEAD:, :] = jnp.ones((8, BLOCK), BF)

    here = pl.ds(iq * BLOCK, BLOCK)
    cos, sin = cos_ref[here, :], sin_ref[here, :]
    near = (iq ^ me) < 2

    def turn(q_ref):
        for h in range(g):
            turned = _rope(q_ref[:, h * HEAD : (h + 1) * HEAD], cos, sin).astype(BF)
            qr_ref[:, h * HEAD : (h + 1) * HEAD] = turned
            q_s[h * BLOCK : (h + 1) * BLOCK, :] = turned

    pl.when(near)(lambda: turn(qn_ref))
    pl.when(jnp.logical_not(near))(lambda: turn(qf_ref))

    def queries(blocks):
        for at in range(0, cols, STRIP):
            lanes = slice(at, at + STRIP)
            scores = [_dot(kr_ref[j * BLOCK : (j + 1) * BLOCK, :], q_s[lanes, :], 1, 1) for j in range(blocks)]
            scores[-1] = jnp.where(_hidden(STRIP), HIDDEN, scores[-1])
            top = functools.reduce(jnp.maximum, [s.max(axis=0, keepdims=True) for s in scores])
            mix = sum(_dot(vt_s[j], jnp.exp2((s - top) * e).astype(BF), 1, 0) for j, s in enumerate(scores))
            total = mix[HEAD : HEAD + 1, :]
            out = (mix[:HEAD, :] * (1 / total)).T.astype(BF)
            for h in range(STRIP // BLOCK):
                to = at // BLOCK + h
                o_ref[:, to * HEAD : (to + 1) * HEAD] = out[h * BLOCK : (h + 1) * BLOCK, :]
            lse_ref[0, :, lanes] = top * e + jnp.log2(total)

    for i in range(n):
        pl.when(iq == i)(functools.partial(queries, i + 1))


def _attend_bwd(me_ref, q_ref, k_ref, vn_ref, vf_ref, don_ref, dof_ref, o_ref, lse_ref, cos_ref, sin_ref, dq_ref, dk_ref, dv_ref,
                q_s, do_s, dk_s, dv_s, kt_s, v_s, delta_s):
    iq = pl.program_id(1)
    me = me_ref[0]
    n = k_ref.shape[0] // BLOCK
    g = q_ref.shape[1] // HEAD
    cols = g * BLOCK
    e = SCALE * LOG2E
    block = lambda i: pl.ds(pl.multiple_of(i * BLOCK, BLOCK), BLOCK)

    @pl.when(iq == 0)
    def _():
        dk_s[...] = jnp.zeros_like(dk_s)
        dv_s[...] = jnp.zeros_like(dv_s)
        for s in range(n):
            v_s[block(s ^ me), :] = (vn_ref if s < 2 else vf_ref)[s % 2 * BLOCK : (s % 2 + 1) * BLOCK, :]
            kt_s[:, s * BLOCK : (s + 1) * BLOCK] = k_ref[s * BLOCK : (s + 1) * BLOCK, :].T

    near = (iq ^ me) < 2

    def take(do_ref):
        for h in range(g):
            lanes, rows = slice(h * HEAD, (h + 1) * HEAD), slice(h * BLOCK, (h + 1) * BLOCK)
            q_s[rows, :] = q_ref[:, lanes]
            do_s[rows, :] = do_ref[:, lanes]
            prod = do_ref[:, lanes].astype(F32) * o_ref[:, lanes].astype(F32)
            delta_s[:, rows] = prod.T.sum(axis=0, keepdims=True)

    pl.when(near)(lambda: take(don_ref))
    pl.when(jnp.logical_not(near))(lambda: take(dof_ref))
    cos, sin = cos_ref[block(iq), :], sin_ref[block(iq), :]

    def queries(blocks):
        m = blocks * BLOCK
        for at in range(0, cols, STRIP_BWD):
            lanes = slice(at, at + STRIP_BWD)
            q, do = q_s[lanes, :], do_s[lanes, :]
            p = jnp.exp2(_dot(k_ref[:m, :], q, 1, 1) * e - lse_ref[0, :, lanes])
            last = jnp.where(_hidden(STRIP_BWD), 0.0, p[m - BLOCK :])
            p = last if blocks == 1 else jnp.concatenate([p[: m - BLOCK], last], axis=0)
            ds = (p * (_dot(v_s[:m, :], do, 1, 1) - delta_s[:, lanes])).astype(BF)
            dv_s[:m, :] += _dot(p.astype(BF), do, 1, 0)
            dk_s[:m, :] += _dot(ds, q, 1, 0)
            dq = (_dot(kt_s[:, :m], ds, 1, 0) * SCALE).T
            for h in range(STRIP_BWD // BLOCK):
                to = at // BLOCK + h
                dq_ref[:, to * HEAD : (to + 1) * HEAD] = _unrope(dq[h * BLOCK : (h + 1) * BLOCK, :], cos, sin).astype(BF)

    for i in range(n):
        pl.when(iq == i)(functools.partial(queries, i + 1))

    @pl.when(iq == n - 1)
    def _():
        for s in range(n):
            here, rows = block(s ^ me), slice(s * BLOCK, (s + 1) * BLOCK)
            dk_ref[rows, :] = _unrope(dk_s[here, :] * SCALE, cos_ref[here, :], sin_ref[here, :]).astype(BF)
            dv_ref[rows, :] = dv_s[here, :].astype(BF)


def _attn_specs(tokens, g):
    queries = pl.BlockSpec((BLOCK, g * HEAD), lambda h, i, me: (i ^ me[0], h))
    near = pl.BlockSpec((BLOCK, g * HEAD), lambda h, i, me: (jnp.minimum(i ^ me[0], 1), h))
    far = pl.BlockSpec((BLOCK, g * HEAD), lambda h, i, me: (jnp.maximum((i ^ me[0]) - 2, 0), h))
    keys = pl.BlockSpec((tokens, HEAD), lambda h, i, me: (0, h))
    half = pl.BlockSpec((tokens // 2, HEAD), lambda h, i, me: (0, h))
    table = pl.BlockSpec((tokens, HEAD), lambda h, i, me: (0, 0))
    stats = pl.BlockSpec((1, 1, g * BLOCK), lambda h, i, me: (h * (tokens // BLOCK) + i, 0, 0))
    return queries, near, far, keys, half, table, stats


def attend(me, qs, ks, vs, cos, sin):
    tokens, width, kv = 2 * ks[0].shape[0], qs[0].shape[1], ks[0].shape[1] // HEAD
    g = width // ks[0].shape[1]
    queries, near, far, keys, half, table, stats = _attn_specs(tokens, g)
    n = tokens // BLOCK
    return pl.pallas_call(
        _attend,
        grid_spec=pltpu.PrefetchScalarGridSpec(
            num_scalar_prefetch=1, grid=(kv, n), in_specs=[near, far, half, half, half, half, table, table],
            out_specs=[queries, stats, queries, keys],
            scratch_shapes=[pltpu.VMEM((n, HEAD + 8, BLOCK), BF), pltpu.VMEM((g * BLOCK, HEAD), BF)]),
        out_shape=[jax.ShapeDtypeStruct((tokens, width), BF), jax.ShapeDtypeStruct((kv * n, 1, g * BLOCK), F32),
                   jax.ShapeDtypeStruct((tokens, width), BF), jax.ShapeDtypeStruct((tokens, kv * HEAD), BF)],
        compiler_params=pltpu.CompilerParams(dimension_semantics=("arbitrary", "arbitrary"), vmem_limit_bytes=60 * 2**20),
        cost_estimate=pl.CostEstimate(flops=12 * 10**9, transcendentals=0, bytes_accessed=8 * 2**20),
        name="attend",
    )(me, *qs, *ks, *vs, cos, sin)


def attend_bwd(me, q, k, vs, dos, o, lse, cos, sin):
    tokens, kv = k.shape[0], k.shape[1] // HEAD
    g = q.shape[1] // k.shape[1]
    queries, near, far, keys, half, table, stats = _attn_specs(tokens, g)
    n = tokens // BLOCK
    return pl.pallas_call(
        _attend_bwd,
        grid_spec=pltpu.PrefetchScalarGridSpec(
            num_scalar_prefetch=1, grid=(kv, n), in_specs=[queries, keys, half, half, near, far, queries, stats, table, table],
            out_specs=[queries, keys, keys],
            scratch_shapes=[pltpu.VMEM((g * BLOCK, HEAD), BF), pltpu.VMEM((g * BLOCK, HEAD), BF),
                            pltpu.VMEM((tokens, HEAD), F32), pltpu.VMEM((tokens, HEAD), F32), pltpu.VMEM((HEAD, tokens), BF),
                            pltpu.VMEM((tokens, HEAD), BF), pltpu.VMEM((1, g * BLOCK), F32)]),
        out_shape=[jax.ShapeDtypeStruct(q.shape, BF), jax.ShapeDtypeStruct(k.shape, BF), jax.ShapeDtypeStruct(k.shape, BF)],
        compiler_params=pltpu.CompilerParams(dimension_semantics=("arbitrary", "arbitrary"), vmem_limit_bytes=60 * 2**20),
        cost_estimate=pl.CostEstimate(flops=18 * 10**9, transcendentals=0, bytes_accessed=12 * 2**20),
        name="attend_bwd",
    )(me, q, k, *vs, *dos, o, lse, cos, sin)


ANY = pl.BlockSpec(memory_space=pltpu.HBM)


def _load(pieces, whole, sems):
    copies, at = [], 0
    for i, piece in enumerate(pieces):
        n = piece.shape[0]
        copies.append(pltpu.make_async_copy(piece, whole.at[pl.ds(at, n), :], sems.at[i]))
        at += n
    for c in copies:
        c.start()
    return copies


def _params(mib, steps=1):
    return pltpu.CompilerParams(dimension_semantics=("arbitrary",) * steps, vmem_limit_bytes=mib * 2**20)


def _price(flops, arrays):
    return pl.CostEstimate(flops=flops, transcendentals=0, bytes_accessed=sum(a.size * 2 for a in arrays))


def _rows(pieces):
    return sum(p.shape[0] for p in pieces)


def qkv(pieces, wq, wk, wv):
    n, (d, nq), nk = len(pieces), wq.shape, wk.shape[1]
    rows, cut = _rows(pieces), 512

    def kernel(*refs):
        xs, (wq_ref, wk_ref, wv_ref), (q_ref, k_ref, v_ref) = refs[:n], refs[n : n + 3], refs[n + 3 : n + 6]
        x_s, q_s, k_s, v_s, sems, wsems = refs[n + 6 :]
        copies = _load(xs, x_s, sems)
        todo = []
        for i, at in enumerate(range(0, nq, cut)):
            here = slice(at, at + cut)
            todo.append((pltpu.make_async_copy(wq_ref.at[:, here], q_s.at[:, here], wsems.at[i]), q_s.at[:, here], q_ref, here))
        for i, (w, w_s, o) in enumerate(((wk_ref, k_s, k_ref), (wv_ref, v_s, v_ref))):
            todo.append((pltpu.make_async_copy(w, w_s, wsems.at[nq // cut + i]), w_s, o, slice(0, nk)))
        todo[0][0].start()
        for c in copies:
            c.wait()
        for i, (c, w_s, o, here) in enumerate(todo):
            c.wait()
            if i + 1 < len(todo):
                todo[i + 1][0].start()
            o[:, here] = _dot(x_s[...], w_s[...], 1, 0).astype(BF)

    return pl.pallas_call(
        kernel, in_specs=[ANY] * (n + 3), out_specs=[pl.BlockSpec(memory_space=pltpu.VMEM)] * 3,
        out_shape=[jax.ShapeDtypeStruct((rows, m), BF) for m in (nq, nk, nk)],
        scratch_shapes=[pltpu.VMEM((rows, d), BF), pltpu.VMEM((d, nq), BF), pltpu.VMEM((d, nk), BF), pltpu.VMEM((d, nk), BF),
                        pltpu.SemaphoreType.DMA((n,)), pltpu.SemaphoreType.DMA((nq // cut + 2,))],
        compiler_params=pltpu.CompilerParams(vmem_limit_bytes=57 * 2**20),
        cost_estimate=_price(2 * rows * d * (nq + 2 * nk), [*pieces, wq, wk, wv]), name="qkv",
    )(*pieces, wq, wk, wv)


def by_rows_of(pieces, w, bn, mib=40):
    n, (cols, d) = len(pieces), w.shape
    rows = _rows(pieces)
    steps, rest = -(-cols // bn), cols % bn
    small = -(-rest // 256) * 256

    def kernel(*refs):
        xs, w_ref, o_ref, x_s, sems = refs[:n], refs[n], refs[n + 1], refs[n + 2], refs[n + 3]
        i = pl.program_id(0)

        @pl.when(i == 0)
        def _():
            for c in _load(xs, x_s, sems):
                c.wait()

        if rest == 0 or small == bn:
            o_ref[...] = _dot(x_s[...], w_ref[...], 1, 1).astype(BF)
            return

        @pl.when(i < steps - 1)
        def _():
            o_ref[...] = _dot(x_s[...], w_ref[...], 1, 1).astype(BF)

        @pl.when(i == steps - 1)
        def _():
            o_ref[:, :small] = _dot(x_s[...], w_ref[:small, :], 1, 1).astype(BF)

    return pl.pallas_call(
        kernel, grid=(steps,), in_specs=[ANY] * n + [pl.BlockSpec((bn, d), lambda i: (i, 0))],
        out_specs=pl.BlockSpec((rows, bn), lambda i: (0, i)), out_shape=jax.ShapeDtypeStruct((rows, cols), BF),
        scratch_shapes=[pltpu.VMEM((rows, d), BF), pltpu.SemaphoreType.DMA((n,))], compiler_params=_params(mib),
        cost_estimate=_price(2 * rows * d * cols, [*pieces, w]),
    )(*pieces, w)


def mlp(pieces, dhid, wg, wu, bn=256):
    n, (d, cols) = len(pieces), wg.shape
    rows = _rows(pieces)

    def kernel(*refs):
        xs, (dhid_ref, g_ref, u_ref), (hid_ref, dg_ref, du_ref), x_s = refs[:n], refs[n : n + 3], refs[n + 3 : n + 6], refs[n + 6]

        @pl.when(pl.program_id(0) == 0)
        def _():
            at = 0
            for x in xs:
                x_s[at : at + x.shape[0], :] = x[...]
                at += x.shape[0]

        gate, up = _dot(x_s[...], g_ref[...], 1, 0), _dot(x_s[...], u_ref[...], 1, 0)
        dhid = dhid_ref[...].astype(F32)
        sig = jax.nn.sigmoid(gate)
        silu = gate * sig
        hid_ref[...] = (silu * up).astype(BF)
        du_ref[...] = (dhid * silu).astype(BF)
        dg_ref[...] = (dhid * up * (sig + silu * (1 - sig))).astype(BF)

    w, o = pl.BlockSpec((d, bn), lambda i: (0, i)), pl.BlockSpec((rows, bn), lambda i: (0, i))
    return pl.pallas_call(
        kernel, grid=(-(-cols // bn),), out_specs=[o, o, o],
        in_specs=[pl.BlockSpec(p.shape, lambda i: (0, 0), pipeline_mode=pl.Buffered(1)) for p in pieces] + [o, w, w],
        out_shape=[jax.ShapeDtypeStruct((rows, cols), BF)] * 3,
        scratch_shapes=[pltpu.VMEM((rows, d), BF)], compiler_params=_params(40),
        cost_estimate=_price(4 * rows * d * cols, [*pieces, wg, wu, dhid, dhid, dhid]), name="mlp",
    )(*pieces, dhid, wg, wu)


def back(xs, ws, bn, half=0):
    n, d = len(xs), ws[0].shape[0]
    rows = 2 * BLOCK

    def kernel(*refs):
        x, w, (a_ref, b_ref), later_s, sems = refs[:n], refs[n : 2 * n], refs[2 * n : 2 * n + 2], refs[2 * n + 2 : -1], refs[-1]
        first = pl.program_id(0) == 0
        copies = [pltpu.make_async_copy(t.at[pl.ds(half * rows, rows), :], t_s, sems.at[i]) for i, (t, t_s) in enumerate(zip(x[1:], later_s))]

        @pl.when(first)
        def _():
            for c in copies:
                c.start()

        total = _dot(x[0][...], w[0][...], 1, 1)
        for t, w_ref, c in zip(later_s, w[1:], copies):
            pl.when(first)(c.wait)
            total += _dot(t[...], w_ref[...], 1, 1)
        total = total.astype(BF)
        a_ref[...], b_ref[...] = total[:BLOCK], total[BLOCK:]

    o = pl.BlockSpec((BLOCK, bn), lambda i: (0, i))
    return pl.pallas_call(
        kernel, grid=(d // bn,),
        in_specs=[pl.BlockSpec((rows, xs[0].shape[1]), lambda i: (half, 0))] + [ANY] * (n - 1)
        + [pl.BlockSpec((bn, w.shape[1]), lambda i: (i, 0)) for w in ws],
        out_specs=[o, o], out_shape=[jax.ShapeDtypeStruct((BLOCK, d), BF)] * 2, compiler_params=_params(48),
        scratch_shapes=[pltpu.VMEM((rows, x.shape[1]), BF) for x in xs[1:]] + [pltpu.SemaphoreType.DMA((n - 1,))],
        cost_estimate=_price(sum(2 * rows * d * w.shape[1] for w in ws), [*xs, *ws]),
    )(*xs, *ws)


def forth(x, w, bn, half):
    (d, cols), rows = w.shape, 2 * BLOCK

    def kernel(x_ref, w_ref, a_ref, b_ref):
        total = _dot(x_ref[...], w_ref[...], 1, 0).astype(BF)
        a_ref[...], b_ref[...] = total[:BLOCK], total[BLOCK:]

    o = pl.BlockSpec((BLOCK, bn), lambda i: (0, i))
    return pl.pallas_call(
        kernel, grid=(cols // bn,), in_specs=[pl.BlockSpec((rows, d), lambda i: (half, 0)), pl.BlockSpec((d, bn), lambda i: (0, i))],
        out_specs=[o, o], out_shape=[jax.ShapeDtypeStruct((BLOCK, cols), BF)] * 2, compiler_params=_params(60),
        cost_estimate=_price(2 * rows * d * cols, [x, w]),
    )(x, w)


def _parts(width):
    cut = width // 512 * 256
    return [(0, width)] if width < 2048 else [(0, cut), (cut, width - cut)]


def weight_grads(lefts, rights, bm, mib=48):
    n, m, rows = len(lefts), lefts[0].shape[1], _rows(lefts)
    counts = [len(r) for r in rights]
    widths = [r[0].shape[1] for r in rights]

    def kernel(*refs):
        ls, refs = refs[:n], refs[n:]
        rs = []
        for c in counts:
            rs.append(refs[:c])
            refs = refs[c:]
        outs, wholes, sems = refs[: len(rights)], refs[len(rights) : 2 * len(rights)], refs[2 * len(rights) :]
        jobs = [(r, w, o, sem, part, pl.ds(at, size)) for r, w, o, sem in zip(rs, wholes, outs, sems)
                for part, (at, size) in enumerate(_parts(w.shape[1]))]

        def copies(r, w, o, sem, part, cols):
            at = 0
            for i, piece in enumerate(r):
                yield pltpu.make_async_copy(piece.at[:, cols], w.at[pl.ds(at, piece.shape[0]), cols], sem.at[part, i])
                at += piece.shape[0]

        def begin(job):
            for c in copies(*job):
                c.start()

        first = pl.program_id(0) == 0
        pl.when(first)(lambda: begin(jobs[0]))
        left = jnp.concatenate([l[...] for l in ls], axis=0).T
        for n_job, job in enumerate(jobs):

            @pl.when(first)
            def _():
                for c in copies(*job):
                    c.wait()
                if n_job + 1 < len(jobs):
                    begin(jobs[n_job + 1])

            _, w, o, _, _, cols = job
            o[:, cols] = _dot(left, w[:, cols], 1, 0).astype(BF)

    return pl.pallas_call(
        kernel, grid=(m // bm,),
        in_specs=[pl.BlockSpec((l.shape[0], bm), lambda i: (0, i)) for l in lefts] + [ANY] * sum(counts),
        out_specs=[pl.BlockSpec((bm, w), lambda i: (i, 0)) for w in widths],
        out_shape=[jax.ShapeDtypeStruct((m, w), BF) for w in widths],
        scratch_shapes=[pltpu.VMEM((rows, w), BF) for w in widths] + [pltpu.SemaphoreType.DMA((len(_parts(w)), c)) for c, w in zip(counts, widths)],
        compiler_params=_params(mib), cost_estimate=_price(2 * rows * m * sum(widths), [*lefts, *(p for r in rights for p in r)]),
    )(*lefts, *(p for r in rights for p in r))


CORE = [(0, 1), (1, 0), (2, 3), (3, 2)]
CROSS = [(0, 2), (2, 0), (1, 3), (3, 1)]


def core(v):
    return lax.ppermute(v, "tp", CORE)


def cross(v):
    return lax.ppermute(v, "tp", CROSS)


def after(v, *others):
    return lax.optimization_barrier((v, *others))[0]


def later(pieces, *others):
    return [after(pieces[0], *others), *pieces[1:]]


def gather(v):
    return [v, core(v)], cross(v)


def far_of(first, *others):
    first = after(first, *others)
    return [first, core(first)]


def scatter_far(mine, other):
    both = (mine.astype(F32) + core(other).astype(F32)).astype(BF)
    return both, cross(both)


def _scale(wide):
    return lax.rsqrt(jnp.mean(wide**2, -1, keepdims=True) + 1e-6)


def by_row(f, arrays, outs, block=128, mib=60):
    rows, d = arrays[0].shape

    def kernel(*refs):
        got = f(*(r[...].astype(F32) for r in refs[: len(arrays)]))
        for ref, t in zip(refs[len(arrays) :], got, strict=True):
            ref[...] = t.astype(BF)

    spec = pl.BlockSpec((block, d), lambda i: (i, 0))
    return pl.pallas_call(
        kernel, grid=(rows // block,), in_specs=[spec] * len(arrays), out_specs=[spec] * outs,
        out_shape=[jax.ShapeDtypeStruct((rows, d), BF)] * outs, compiler_params=_params(mib),
        cost_estimate=_price(10 * rows * d, [*arrays, *arrays[:outs]]),
    )(*arrays)


def norm(h):
    return by_row(lambda wide: (wide * _scale(wide),), [h], 1, 32, 24)[0]


def add_norm(h, mine, other, far):
    def f(h, *terms):
        wide = (h + sum(terms)).astype(BF).astype(F32)
        return wide, wide * _scale(wide)

    return by_row(f, [h, mine, core(other), far], 2, 32, 24)


def norm_bwd(direct, h, mine, other, far, block=128, mib=60):
    def f(direct, h, *terms):
        g, scale = sum(terms).astype(BF).astype(F32), _scale(h)
        return (direct + scale * g - h * (scale**3 * jnp.mean(g * h, -1, keepdims=True)),)

    return by_row(f, [direct, h, mine, core(other), far], 1, block, mib)[0]


def layer(x, dy, wq, wk, wv, wo, wg, wu, wd):
    x, dy = x[0], dy[0]
    me = lax.axis_index("tp").astype(jnp.int32).reshape(1)
    tokens = 4 * x.shape[0]
    half = HEAD // 2
    angle = jnp.arange(tokens, dtype=F32)[:, None] * THETA ** (-jnp.arange(half, dtype=F32) / half)
    cos, sin = jnp.cos(angle), jnp.sin(angle)
    cos, sin = jnp.concatenate([cos, cos], 1), jnp.concatenate([-sin, sin], 1)

    a = norm(x)
    a_near, a_far = gather(a)
    dy_near = [dy, core(dy)]
    near_qkv = qkv(a_near, wq, wk, wv)
    dhid_near = by_rows_of(later(dy_near, near_qkv[0]), wd, 512)
    a_far = far_of(a_far, dhid_near, cos, sin)
    dy_far = cross(after(dy, a_far[0]))
    far_qkv = qkv(a_far, wq, wk, wv)
    qs, ks, vs = zip(near_qkv, far_qkv)
    heads, lse, q, k = attend(me, qs, ks, vs, cos, sin)
    terms = forth(heads, wo, 1024, 1)
    both, far = scatter_far(*terms)
    near = forth(after(heads, both), wo, 1024, 0)
    dy_far = far_of(dy_far, both, near[0])
    dhid_far = by_rows_of(dy_far, wd, 512)
    h, b = add_norm(x, *near, after(far, dhid_far))
    b_near, b_far = gather(b)
    hid_near, dgate_near, dup_near = mlp(b_near, dhid_near, wg, wu)
    b_far = far_of(b_far, hid_near)
    hid_far, dgate_far, dup_far = mlp(b_far, dhid_far, wg, wu)
    terms = back([dgate_far, dup_far], [wg, wu], 512)
    near = back(later([dgate_near, dup_near], terms[1]), [wg, wu], 512)
    both, far = scatter_far(after(terms[0], near[0]), terms[1])
    d_wg, d_wu = weight_grads(later([*b_near, *b_far], both), [[dgate_near, dgate_far], [dup_near, dup_far]], 512, 56)
    dh = norm_bwd(dy, h, *near, after(far, d_wg))
    dh_near, dh_far = gather(dh)
    (d_wd,) = weight_grads(later([hid_near, hid_far], dh), [[*dy_near, *dy_far]], 640)
    dheads_near = by_rows_of(later(dh_near, d_wd), wo, 512, 40)
    dh_far = far_of(dh_far, dheads_near)
    dheads_far = by_rows_of(dh_far, wo, 512, 40)
    dq, dk, dv = attend_bwd(me, q, k, vs, (dheads_near, dheads_far), heads, lse, cos, sin)
    both, far = scatter_far(*back([dq, dk, dv], [wq, wk, wv], 1024, 1))
    near = back(later([dq, dk, dv], both), [wq, wk, wv], 1024)
    d_wq, d_wk, d_wv = weight_grads(later([*a_near, *a_far], near[0]), [[dq], [dk], [dv]], 1024)
    (d_wo,) = weight_grads(later([heads], d_wq), [[*dh_near, *dh_far]], 512)
    dx = norm_bwd(dh, x, *near, after(far, d_wo), 32, 24)
    return (dx[None], d_wq, d_wk, d_wv, d_wo, d_wg, d_wu, d_wd)


def solution(mesh):
    states, by_columns, by_rows = P("dp", "tp", None), P(None, "tp"), P("tp", None)
    weights = (by_columns, by_columns, by_columns, by_rows, by_columns, by_columns, by_rows)
    own = tuple(P("dp", "tp") if spec == by_columns else P(("dp", "tp"), None) for spec in weights)
    return jax.shard_map(layer, mesh=mesh, in_specs=(states, states, *weights), out_specs=(states, *own), check_vma=False)
```

```python
import functools

import jax
import jax.numpy as jnp
from jax import lax
from jax.experimental import pallas as pl
from jax.experimental.pallas import tpu as pltpu
from jax.sharding import PartitionSpec as P


HEAD = 128
THETA = 10000
LOG2E = 1.4426950408889634
HIDDEN = -2e30
SCALE = HEAD**-0.5
BF, F32 = jnp.bfloat16, jnp.float32
BLOCK = 256
STRIP, STRIP_BWD = 1024, 512


def _dot(a, b, ca, cb):
    return lax.dot_general(a, b, (((ca,), (cb,)), ((), ())), preferred_element_type=F32)


def _rope(x, cos, sin):
    x = x.astype(F32)
    return x * cos + pltpu.roll(x, HEAD // 2, 1) * sin


def _unrope(x, cos, sin):
    return x * cos - pltpu.roll(x, HEAD // 2, 1) * sin


def _hidden(cols):
    key = lax.broadcasted_iota(jnp.int32, (BLOCK, cols), 0)
    return key > lax.rem(lax.broadcasted_iota(jnp.int32, (BLOCK, cols), 1), BLOCK)


def _attend(me_ref, qn_ref, qf_ref, kn_ref, kf_ref, vn_ref, vf_ref, cos_ref, sin_ref, o_ref, lse_ref, qr_ref, kr_ref, vt_s, q_s):
    iq = pl.program_id(1)
    me = me_ref[0]
    n = kr_ref.shape[0] // BLOCK
    g = qr_ref.shape[1] // HEAD
    cols = g * BLOCK
    e = SCALE * LOG2E

    @pl.when(iq == 0)
    def _():
        for s in range(n):
            here = pl.ds(pl.multiple_of((s ^ me) * BLOCK, BLOCK), BLOCK)
            half = slice(s % 2 * BLOCK, (s % 2 + 1) * BLOCK)
            k, v = (kn_ref, vn_ref) if s < 2 else (kf_ref, vf_ref)
            kr_ref[here, :] = _rope(k[half, :], cos_ref[here, :], sin_ref[here, :]).astype(BF)
            vt_s[s ^ me, :HEAD, :] = v[half, :].T
            vt_s[s, HEAD:, :] = jnp.ones((8, BLOCK), BF)

    here = pl.ds(iq * BLOCK, BLOCK)
    cos, sin = cos_ref[here, :], sin_ref[here, :]
    near = (iq ^ me) < 2

    def turn(q_ref):
        for h in range(g):
            turned = _rope(q_ref[:, h * HEAD : (h + 1) * HEAD], cos, sin).astype(BF)
            qr_ref[:, h * HEAD : (h + 1) * HEAD] = turned
            q_s[h * BLOCK : (h + 1) * BLOCK, :] = turned

    pl.when(near)(lambda: turn(qn_ref))
    pl.when(jnp.logical_not(near))(lambda: turn(qf_ref))

    def queries(blocks):
        for at in range(0, cols, STRIP):
            lanes = slice(at, at + STRIP)
            scores = [_dot(kr_ref[j * BLOCK : (j + 1) * BLOCK, :], q_s[lanes, :], 1, 1) for j in range(blocks)]
            scores[-1] = jnp.where(_hidden(STRIP), HIDDEN, scores[-1])
            top = functools.reduce(jnp.maximum, [s.max(axis=0, keepdims=True) for s in scores])
            mix = sum(_dot(vt_s[j], jnp.exp2((s - top) * e).astype(BF), 1, 0) for j, s in enumerate(scores))
            total = mix[HEAD : HEAD + 1, :]
            out = (mix[:HEAD, :] * (1 / total)).T.astype(BF)
            for h in range(STRIP // BLOCK):
                to = at // BLOCK + h
                o_ref[:, to * HEAD : (to + 1) * HEAD] = out[h * BLOCK : (h + 1) * BLOCK, :]
            lse_ref[0, :, lanes] = top * e + jnp.log2(total)

    for i in range(n):
        pl.when(iq == i)(functools.partial(queries, i + 1))


def _attend_bwd(me_ref, q_ref, k_ref, vn_ref, vf_ref, don_ref, dof_ref, o_ref, lse_ref, cos_ref, sin_ref, dq_ref, dk_ref, dv_ref,
                q_s, do_s, dk_s, dv_s, kt_s, v_s, delta_s):
    iq = pl.program_id(1)
    me = me_ref[0]
    n = k_ref.shape[0] // BLOCK
    g = q_ref.shape[1] // HEAD
    cols = g * BLOCK
    e = SCALE * LOG2E
    block = lambda i: pl.ds(pl.multiple_of(i * BLOCK, BLOCK), BLOCK)

    @pl.when(iq == 0)
    def _():
        dk_s[...] = jnp.zeros_like(dk_s)
        dv_s[...] = jnp.zeros_like(dv_s)
        for s in range(n):
            v_s[block(s ^ me), :] = (vn_ref if s < 2 else vf_ref)[s % 2 * BLOCK : (s % 2 + 1) * BLOCK, :]
            kt_s[:, s * BLOCK : (s + 1) * BLOCK] = k_ref[s * BLOCK : (s + 1) * BLOCK, :].T

    near = (iq ^ me) < 2

    def take(do_ref):
        for h in range(g):
            lanes, rows = slice(h * HEAD, (h + 1) * HEAD), slice(h * BLOCK, (h + 1) * BLOCK)
            q_s[rows, :] = q_ref[:, lanes]
            do_s[rows, :] = do_ref[:, lanes]
            prod = do_ref[:, lanes].astype(F32) * o_ref[:, lanes].astype(F32)
            delta_s[:, rows] = prod.T.sum(axis=0, keepdims=True)

    pl.when(near)(lambda: take(don_ref))
    pl.when(jnp.logical_not(near))(lambda: take(dof_ref))
    cos, sin = cos_ref[block(iq), :], sin_ref[block(iq), :]

    def queries(blocks):
        m = blocks * BLOCK
        for at in range(0, cols, STRIP_BWD):
            lanes = slice(at, at + STRIP_BWD)
            q, do = q_s[lanes, :], do_s[lanes, :]
            p = jnp.exp2(_dot(k_ref[:m, :], q, 1, 1) * e - lse_ref[0, :, lanes])
            last = jnp.where(_hidden(STRIP_BWD), 0.0, p[m - BLOCK :])
            p = last if blocks == 1 else jnp.concatenate([p[: m - BLOCK], last], axis=0)
            ds = (p * (_dot(v_s[:m, :], do, 1, 1) - delta_s[:, lanes])).astype(BF)
            dv_s[:m, :] += _dot(p.astype(BF), do, 1, 0)
            dk_s[:m, :] += _dot(ds, q, 1, 0)
            dq = (_dot(kt_s[:, :m], ds, 1, 0) * SCALE).T
            for h in range(STRIP_BWD // BLOCK):
                to = at // BLOCK + h
                dq_ref[:, to * HEAD : (to + 1) * HEAD] = _unrope(dq[h * BLOCK : (h + 1) * BLOCK, :], cos, sin).astype(BF)

    for i in range(n):
        pl.when(iq == i)(functools.partial(queries, i + 1))

    @pl.when(iq == n - 1)
    def _():
        for s in range(n):
            here, rows = block(s ^ me), slice(s * BLOCK, (s + 1) * BLOCK)
            dk_ref[rows, :] = _unrope(dk_s[here, :] * SCALE, cos_ref[here, :], sin_ref[here, :]).astype(BF)
            dv_ref[rows, :] = dv_s[here, :].astype(BF)


def _attn_specs(tokens, g):
    queries = pl.BlockSpec((BLOCK, g * HEAD), lambda h, i, me: (i ^ me[0], h))
    near = pl.BlockSpec((BLOCK, g * HEAD), lambda h, i, me: (jnp.minimum(i ^ me[0], 1), h))
    far = pl.BlockSpec((BLOCK, g * HEAD), lambda h, i, me: (jnp.maximum((i ^ me[0]) - 2, 0), h))
    keys = pl.BlockSpec((tokens, HEAD), lambda h, i, me: (0, h))
    half = pl.BlockSpec((tokens // 2, HEAD), lambda h, i, me: (0, h))
    table = pl.BlockSpec((tokens, HEAD), lambda h, i, me: (0, 0))
    stats = pl.BlockSpec((1, 1, g * BLOCK), lambda h, i, me: (h * (tokens // BLOCK) + i, 0, 0))
    return queries, near, far, keys, half, table, stats


def attend(me, qs, ks, vs, cos, sin):
    tokens, width, kv = 2 * ks[0].shape[0], qs[0].shape[1], ks[0].shape[1] // HEAD
    g = width // ks[0].shape[1]
    queries, near, far, keys, half, table, stats = _attn_specs(tokens, g)
    n = tokens // BLOCK
    return pl.pallas_call(
        _attend,
        grid_spec=pltpu.PrefetchScalarGridSpec(
            num_scalar_prefetch=1, grid=(kv, n), in_specs=[near, far, half, half, half, half, table, table],
            out_specs=[queries, stats, queries, keys],
            scratch_shapes=[pltpu.VMEM((n, HEAD + 8, BLOCK), BF), pltpu.VMEM((g * BLOCK, HEAD), BF)]),
        out_shape=[jax.ShapeDtypeStruct((tokens, width), BF), jax.ShapeDtypeStruct((kv * n, 1, g * BLOCK), F32),
                   jax.ShapeDtypeStruct((tokens, width), BF), jax.ShapeDtypeStruct((tokens, kv * HEAD), BF)],
        compiler_params=pltpu.CompilerParams(dimension_semantics=("arbitrary", "arbitrary"), vmem_limit_bytes=60 * 2**20),
        cost_estimate=pl.CostEstimate(flops=12 * 10**9, transcendentals=0, bytes_accessed=8 * 2**20),
        name="attend",
    )(me, *qs, *ks, *vs, cos, sin)


def attend_bwd(me, q, k, vs, dos, o, lse, cos, sin):
    tokens, kv = k.shape[0], k.shape[1] // HEAD
    g = q.shape[1] // k.shape[1]
    queries, near, far, keys, half, table, stats = _attn_specs(tokens, g)
    n = tokens // BLOCK
    return pl.pallas_call(
        _attend_bwd,
        grid_spec=pltpu.PrefetchScalarGridSpec(
            num_scalar_prefetch=1, grid=(kv, n), in_specs=[queries, keys, half, half, near, far, queries, stats, table, table],
            out_specs=[queries, keys, keys],
            scratch_shapes=[pltpu.VMEM((g * BLOCK, HEAD), BF), pltpu.VMEM((g * BLOCK, HEAD), BF),
                            pltpu.VMEM((tokens, HEAD), F32), pltpu.VMEM((tokens, HEAD), F32), pltpu.VMEM((HEAD, tokens), BF),
                            pltpu.VMEM((tokens, HEAD), BF), pltpu.VMEM((1, g * BLOCK), F32)]),
        out_shape=[jax.ShapeDtypeStruct(q.shape, BF), jax.ShapeDtypeStruct(k.shape, BF), jax.ShapeDtypeStruct(k.shape, BF)],
        compiler_params=pltpu.CompilerParams(dimension_semantics=("arbitrary", "arbitrary"), vmem_limit_bytes=60 * 2**20),
        cost_estimate=pl.CostEstimate(flops=18 * 10**9, transcendentals=0, bytes_accessed=12 * 2**20),
        name="attend_bwd",
    )(me, q, k, *vs, *dos, o, lse, cos, sin)


ANY = pl.BlockSpec(memory_space=pltpu.HBM)


def _load(pieces, whole, sems):
    copies, at = [], 0
    for i, piece in enumerate(pieces):
        n = piece.shape[0]
        copies.append(pltpu.make_async_copy(piece, whole.at[pl.ds(at, n), :], sems.at[i]))
        at += n
    for c in copies:
        c.start()
    return copies


def _params(mib, steps=1):
    return pltpu.CompilerParams(dimension_semantics=("arbitrary",) * steps, vmem_limit_bytes=mib * 2**20)


def _price(flops, arrays):
    return pl.CostEstimate(flops=flops, transcendentals=0, bytes_accessed=sum(a.size * 2 for a in arrays))


def _rows(pieces):
    return sum(p.shape[0] for p in pieces)


def qkv(pieces, wq, wk, wv):
    n, (d, nq), nk = len(pieces), wq.shape, wk.shape[1]
    rows, cut = _rows(pieces), 512

    def kernel(*refs):
        xs, (wq_ref, wk_ref, wv_ref), (q_ref, k_ref, v_ref) = refs[:n], refs[n : n + 3], refs[n + 3 : n + 6]
        x_s, q_s, k_s, v_s, sems, wsems = refs[n + 6 :]
        copies = _load(xs, x_s, sems)
        todo = []
        for i, at in enumerate(range(0, nq, cut)):
            here = slice(at, at + cut)
            todo.append((pltpu.make_async_copy(wq_ref.at[:, here], q_s.at[:, here], wsems.at[i]), q_s.at[:, here], q_ref, here))
        for i, (w, w_s, o) in enumerate(((wk_ref, k_s, k_ref), (wv_ref, v_s, v_ref))):
            todo.append((pltpu.make_async_copy(w, w_s, wsems.at[nq // cut + i]), w_s, o, slice(0, nk)))
        todo[0][0].start()
        for c in copies:
            c.wait()
        for i, (c, w_s, o, here) in enumerate(todo):
            c.wait()
            if i + 1 < len(todo):
                todo[i + 1][0].start()
            o[:, here] = _dot(x_s[...], w_s[...], 1, 0).astype(BF)

    return pl.pallas_call(
        kernel, in_specs=[ANY] * (n + 3), out_specs=[pl.BlockSpec(memory_space=pltpu.VMEM)] * 3,
        out_shape=[jax.ShapeDtypeStruct((rows, m), BF) for m in (nq, nk, nk)],
        scratch_shapes=[pltpu.VMEM((rows, d), BF), pltpu.VMEM((d, nq), BF), pltpu.VMEM((d, nk), BF), pltpu.VMEM((d, nk), BF),
                        pltpu.SemaphoreType.DMA((n,)), pltpu.SemaphoreType.DMA((nq // cut + 2,))],
        compiler_params=pltpu.CompilerParams(vmem_limit_bytes=57 * 2**20),
        cost_estimate=_price(2 * rows * d * (nq + 2 * nk), [*pieces, wq, wk, wv]), name="qkv",
    )(*pieces, wq, wk, wv)


def by_rows_of(pieces, w, bn, mib=40):
    n, (cols, d) = len(pieces), w.shape
    rows = _rows(pieces)
    steps, rest = -(-cols // bn), cols % bn
    small = -(-rest // 256) * 256

    def kernel(*refs):
        xs, w_ref, o_ref, x_s, sems = refs[:n], refs[n], refs[n + 1], refs[n + 2], refs[n + 3]
        i = pl.program_id(0)

        @pl.when(i == 0)
        def _():
            for c in _load(xs, x_s, sems):
                c.wait()

        if rest == 0 or small == bn:
            o_ref[...] = _dot(x_s[...], w_ref[...], 1, 1).astype(BF)
            return

        @pl.when(i < steps - 1)
        def _():
            o_ref[...] = _dot(x_s[...], w_ref[...], 1, 1).astype(BF)

        @pl.when(i == steps - 1)
        def _():
            o_ref[:, :small] = _dot(x_s[...], w_ref[:small, :], 1, 1).astype(BF)

    return pl.pallas_call(
        kernel, grid=(steps,), in_specs=[ANY] * n + [pl.BlockSpec((bn, d), lambda i: (i, 0))],
        out_specs=pl.BlockSpec((rows, bn), lambda i: (0, i)), out_shape=jax.ShapeDtypeStruct((rows, cols), BF),
        scratch_shapes=[pltpu.VMEM((rows, d), BF), pltpu.SemaphoreType.DMA((n,))], compiler_params=_params(mib),
        cost_estimate=_price(2 * rows * d * cols, [*pieces, w]),
    )(*pieces, w)


def mlp(pieces, dhid, wg, wu, bn=256):
    n, (d, cols) = len(pieces), wg.shape
    rows = _rows(pieces)

    def kernel(*refs):
        xs, (dhid_ref, g_ref, u_ref), (hid_ref, dg_ref, du_ref), x_s = refs[:n], refs[n : n + 3], refs[n + 3 : n + 6], refs[n + 6]

        @pl.when(pl.program_id(0) == 0)
        def _():
            at = 0
            for x in xs:
                x_s[at : at + x.shape[0], :] = x[...]
                at += x.shape[0]

        gate, up = _dot(x_s[...], g_ref[...], 1, 0), _dot(x_s[...], u_ref[...], 1, 0)
        dhid = dhid_ref[...].astype(F32)
        sig = jax.nn.sigmoid(gate)
        silu = gate * sig
        hid_ref[...] = (silu * up).astype(BF)
        du_ref[...] = (dhid * silu).astype(BF)
        dg_ref[...] = (dhid * up * (sig + silu * (1 - sig))).astype(BF)

    w, o = pl.BlockSpec((d, bn), lambda i: (0, i)), pl.BlockSpec((rows, bn), lambda i: (0, i))
    return pl.pallas_call(
        kernel, grid=(-(-cols // bn),), out_specs=[o, o, o],
        in_specs=[pl.BlockSpec(p.shape, lambda i: (0, 0), pipeline_mode=pl.Buffered(1)) for p in pieces] + [o, w, w],
        out_shape=[jax.ShapeDtypeStruct((rows, cols), BF)] * 3,
        scratch_shapes=[pltpu.VMEM((rows, d), BF)], compiler_params=_params(56),
        cost_estimate=_price(4 * rows * d * cols, [*pieces, wg, wu, dhid, dhid, dhid]), name="mlp",
    )(*pieces, dhid, wg, wu)


def back(xs, ws, bn, half=0):
    n, d = len(xs), ws[0].shape[0]
    rows = 2 * BLOCK

    def kernel(*refs):
        x, w, (a_ref, b_ref) = refs[:n], refs[n : 2 * n], refs[2 * n :]
        total = _dot(x[0][...], w[0][...], 1, 1)
        for i in range(1, n):
            total += _dot(x[i][...], w[i][...], 1, 1)
        total = total.astype(BF)
        a_ref[...], b_ref[...] = total[:BLOCK], total[BLOCK:]

    o = pl.BlockSpec((BLOCK, bn), lambda i: (0, i))
    return pl.pallas_call(
        kernel, grid=(d // bn,),
        in_specs=[pl.BlockSpec((rows, x.shape[1]), lambda i: (half, 0)) for x in xs] + [pl.BlockSpec((bn, w.shape[1]), lambda i: (i, 0)) for w in ws],
        out_specs=[o, o], out_shape=[jax.ShapeDtypeStruct((BLOCK, d), BF)] * 2, compiler_params=_params(48),
        cost_estimate=_price(sum(2 * rows * d * w.shape[1] for w in ws), [*xs, *ws]),
    )(*xs, *ws)


def forth(x, w, bn, half):
    (d, cols), rows = w.shape, 2 * BLOCK

    def kernel(x_ref, w_ref, a_ref, b_ref):
        total = _dot(x_ref[...], w_ref[...], 1, 0).astype(BF)
        a_ref[...], b_ref[...] = total[:BLOCK], total[BLOCK:]

    o = pl.BlockSpec((BLOCK, bn), lambda i: (0, i))
    return pl.pallas_call(
        kernel, grid=(cols // bn,), in_specs=[pl.BlockSpec((rows, d), lambda i: (half, 0)), pl.BlockSpec((d, bn), lambda i: (0, i))],
        out_specs=[o, o], out_shape=[jax.ShapeDtypeStruct((BLOCK, cols), BF)] * 2, compiler_params=_params(60),
        cost_estimate=_price(2 * rows * d * cols, [x, w]),
    )(x, w)


def weight_grads(lefts, rights, bm, mib=48):
    n, m, rows = len(lefts), lefts[0].shape[1], _rows(lefts)
    counts = [len(r) for r in rights]
    widths = [r[0].shape[1] for r in rights]

    def kernel(*refs):
        ls, refs = refs[:n], refs[n:]
        rs = []
        for c in counts:
            rs.append(refs[:c])
            refs = refs[c:]
        outs, wholes, sems = refs[: len(rights)], refs[len(rights) : 2 * len(rights)], refs[2 * len(rights) :]

        @pl.when(pl.program_id(0) == 0)
        def _():
            for c in [c for r, w, s in zip(rs, wholes, sems) for c in _load(r, w, s)]:
                c.wait()

        left = jnp.concatenate([l[...] for l in ls], axis=0).T
        for o, w in zip(outs, wholes):
            o[...] = _dot(left, w[...], 1, 0).astype(BF)

    return pl.pallas_call(
        kernel, grid=(m // bm,),
        in_specs=[pl.BlockSpec((l.shape[0], bm), lambda i: (0, i)) for l in lefts] + [ANY] * sum(counts),
        out_specs=[pl.BlockSpec((bm, w), lambda i: (i, 0)) for w in widths],
        out_shape=[jax.ShapeDtypeStruct((m, w), BF) for w in widths],
        scratch_shapes=[pltpu.VMEM((rows, w), BF) for w in widths] + [pltpu.SemaphoreType.DMA((c,)) for c in counts],
        compiler_params=_params(mib), cost_estimate=_price(2 * rows * m * sum(widths), [*lefts, *(p for r in rights for p in r)]),
    )(*lefts, *(p for r in rights for p in r))


CORE = [(0, 1), (1, 0), (2, 3), (3, 2)]
CROSS = [(0, 2), (2, 0), (1, 3), (3, 1)]


def core(v):
    return lax.ppermute(v, "tp", CORE)


def cross(v):
    return lax.ppermute(v, "tp", CROSS)


def after(v, *others):
    return lax.optimization_barrier((v, *others))[0]


def later(pieces, *others):
    return [after(pieces[0], *others), *pieces[1:]]


def gather(v):
    return [v, core(v)], cross(v)


def far_of(first, *others):
    first = after(first, *others)
    return [first, core(first)]


def scatter_far(mine, other):
    both = (mine.astype(F32) + core(other).astype(F32)).astype(BF)
    return both, cross(both)


def _scale(wide):
    return lax.rsqrt(jnp.mean(wide**2, -1, keepdims=True) + 1e-6)


def by_row(f, arrays, outs, block=128, mib=60):
    rows, d = arrays[0].shape

    def kernel(*refs):
        got = f(*(r[...].astype(F32) for r in refs[: len(arrays)]))
        for ref, t in zip(refs[len(arrays) :], got, strict=True):
            ref[...] = t.astype(BF)

    spec = pl.BlockSpec((block, d), lambda i: (i, 0))
    return pl.pallas_call(
        kernel, grid=(rows // block,), in_specs=[spec] * len(arrays), out_specs=[spec] * outs,
        out_shape=[jax.ShapeDtypeStruct((rows, d), BF)] * outs, compiler_params=_params(mib),
        cost_estimate=_price(10 * rows * d, [*arrays, *arrays[:outs]]),
    )(*arrays)


def norm(h):
    return by_row(lambda wide: (wide * _scale(wide),), [h], 1, 32, 24)[0]


def add_norm(h, mine, other, far):
    def f(h, *terms):
        wide = (h + sum(terms)).astype(BF).astype(F32)
        return wide, wide * _scale(wide)

    return by_row(f, [h, mine, core(other), far], 2, 32, 24)


def norm_bwd(direct, h, mine, other, far, block=128, mib=60):
    def f(direct, h, *terms):
        g, scale = sum(terms).astype(BF).astype(F32), _scale(h)
        return (direct + scale * g - h * (scale**3 * jnp.mean(g * h, -1, keepdims=True)),)

    return by_row(f, [direct, h, mine, core(other), far], 1, block, mib)[0]


def layer(x, dy, wq, wk, wv, wo, wg, wu, wd):
    x, dy = x[0], dy[0]
    me = lax.axis_index("tp").astype(jnp.int32).reshape(1)
    tokens = 4 * x.shape[0]
    half = HEAD // 2
    angle = jnp.arange(tokens, dtype=F32)[:, None] * THETA ** (-jnp.arange(half, dtype=F32) / half)
    cos, sin = jnp.cos(angle), jnp.sin(angle)
    cos, sin = jnp.concatenate([cos, cos], 1), jnp.concatenate([-sin, sin], 1)

    a = norm(x)
    a_near, a_far = gather(a)
    dy_near = [dy, core(dy)]
    near_qkv = qkv(a_near, wq, wk, wv)
    dhid_near = by_rows_of(later(dy_near, near_qkv[0]), wd, 512)
    a_far = far_of(a_far, dhid_near, cos, sin)
    dy_far = cross(after(dy, a_far[0]))
    far_qkv = qkv(a_far, wq, wk, wv)
    qs, ks, vs = zip(near_qkv, far_qkv)
    heads, lse, q, k = attend(me, qs, ks, vs, cos, sin)
    terms = forth(heads, wo, 1024, 1)
    both, far = scatter_far(*terms)
    near = forth(after(heads, both), wo, 1024, 0)
    dy_far = far_of(dy_far, both, near[0])
    dhid_far = by_rows_of(dy_far, wd, 512)
    h, b = add_norm(x, *near, after(far, dhid_far))
    b_near, b_far = gather(b)
    hid_near, dgate_near, dup_near = mlp(b_near, dhid_near, wg, wu)
    b_far = far_of(b_far, hid_near)
    hid_far, dgate_far, dup_far = mlp(b_far, dhid_far, wg, wu)
    terms = back([dgate_far, dup_far], [wg, wu], 512)
    near = back(later([dgate_near, dup_near], terms[1]), [wg, wu], 512)
    both, far = scatter_far(after(terms[0], near[0]), terms[1])
    d_wg, d_wu = weight_grads(later([*b_near, *b_far], both), [[dgate_near, dgate_far], [dup_near, dup_far]], 512, 56)
    dh = norm_bwd(dy, h, *near, after(far, d_wg))
    dh_near, dh_far = gather(dh)
    (d_wd,) = weight_grads(later([hid_near, hid_far], dh), [[*dy_near, *dy_far]], 640)
    dheads_near = by_rows_of(later(dh_near, d_wd), wo, 512, 40)
    dh_far = far_of(dh_far, dheads_near)
    dheads_far = by_rows_of(dh_far, wo, 512, 40)
    dq, dk, dv = attend_bwd(me, q, k, vs, (dheads_near, dheads_far), heads, lse, cos, sin)
    both, far = scatter_far(*back([dq, dk, dv], [wq, wk, wv], 1024, 1))
    near = back(later([dq, dk, dv], both), [wq, wk, wv], 1024)
    d_wq, d_wk, d_wv = weight_grads(later([*a_near, *a_far], near[0]), [[dq], [dk], [dv]], 1024)
    (d_wo,) = weight_grads(later([heads], d_wq), [[*dh_near, *dh_far]], 512)
    dx = norm_bwd(dh, x, *near, after(far, d_wo), 32, 24)
    return (dx[None], d_wq, d_wk, d_wv, d_wo, d_wg, d_wu, d_wd)


def solution(mesh):
    states, by_columns, by_rows = P("dp", "tp", None), P(None, "tp"), P("tp", None)
    weights = (by_columns, by_columns, by_columns, by_rows, by_columns, by_columns, by_rows)
    own = tuple(P("dp", "tp") if spec == by_columns else P(("dp", "tp"), None) for spec in weights)
    return jax.shard_map(layer, mesh=mesh, in_specs=(states, states, *weights), out_specs=(states, *own), check_vma=False)
```
